128 devices in a mesh: groups: 4 (over y, x), row: 16 (over z), col: 2 (over core).
Axes of the slice: x: 2, y: 2, z: 16, core: 2. Of those that a mesh axis runs over, the one named last changes fastest.
The devices are a block of a 8x8x16 slice.
Arguments:
- cell_index: int32 [4096, 128], P(('groups', 'row', 'col')), parts along dimension 0, may hold values from 0 to 262143
- weights: bfloat16 [4096, 512], P(('groups', 'row', 'col')), parts along dimension 0, may hold values from -6 to 6
- block_tile: int32 [4096], P(('groups', 'row', 'col')), parts along dimension 0, may hold values from 0 to 31, as said below
- spread: float32 [2, 4], replicated, may hold values from 3 to 8
Outputs:
- density: float32 [4, 16384, 2048], P(None, ('groups', 'row'), 'col'), parts along dimension 1
The draws below stay inside these ranges and needn't reach their ends.
There are 4 independent parts, one for each index of `groups`. The reference program is written for one: setup_inputs(seed, part) draws one part's arguments, and reference() takes and returns one part's arrays. A program takes and returns all parts, laid end to end along the dimension named above; an argument that names none is the same for every part. Nothing has to cross between parts.
Inputs may be any that keep to these rules, and one draw needn't show every extreme that they name: `block_tile`: among the 32 blocks of one device no tile is named more than 3 times; in every draw some tile is named exactly 3 times by the blocks of every device.
All inputs are finite; a program needn't handle non-finite values.
Results may differ from the reference program's by a relative error of at most 0.0003.
Values may be sent and summed in bfloat16 or wider, within the bound.
A program may use at most 64 MiB of HBM per device.

```python
import math
import jax
import jax.numpy as jnp

CHANNELS = 4
BLOCK_PTS = 128
REACH = 16
TILE_ROWS = 256
TILE_COLS = 1024
BLOCKS = 32
CAPACITY = 3
TILES = 32
GRID_ROWS = 4096
GRID_COLS = 2048
N_COL = 2


def draw_block_tile(key, part):
    hottest = jax.random.randint(jax.random.fold_in(key, 1), (), 0, TILES)
    favour = jax.random.randint(jax.random.fold_in(key, 2), (TILES,), 0, 1 << 21)
    slot_tile = jnp.arange(TILES * CAPACITY, dtype=jnp.int32) // CAPACITY

    def one_device(device):
        subkey = jax.random.fold_in(key, 100 + device)
        scores = jax.random.randint(subkey, (TILES * CAPACITY,), 0, 1 << 20)
        scores = scores + favour[slot_tile] + jnp.where(slot_tile == hottest, 1 << 23, 0)
        ordering = jnp.argsort(-scores, stable=True)
        chosen = slot_tile[ordering[:BLOCKS]]
        shuffle = jax.random.permutation(jax.random.fold_in(subkey, 7), BLOCKS)
        return chosen[shuffle]
    result = jax.vmap(one_device)(jnp.arange(TILES, dtype=jnp.int32))
    return result.reshape(-1).astype(jnp.int32)


def place_ends(array, key, low, high):
    extent = array.shape
    spot = [jax.random.randint(jax.random.fold_in(key, axis), (), 0, extent[axis]) for axis in range(len(extent))]
    array = array.at[tuple(spot)].set(low)
    longest = extent.index(max(extent))
    spot[longest] = (spot[longest] + 1) % extent[longest]
    return array.at[tuple(spot)].set(high)


def shard_levels(own_key, dims, split, low, top_value):
    def one(axis_at, shards_of):
        heights = jax.random.uniform(jax.random.fold_in(jax.random.fold_in(own_key, 6), axis_at), (shards_of,), jnp.float32, low / len(split), top_value / len(split))
        return jnp.repeat(jnp.exp(heights), dims[axis_at] // shards_of).reshape((-1,) + (1,) * (len(dims) - axis_at - 1))

    factor_of = one(*split[0])
    for cut in split[1:]:
        factor_of = factor_of * one(*cut)
    return factor_of


def scatter_about(own_key, extent, scale, limit, pieces=(), kind=jnp.bfloat16):
    entries = scale * jax.random.normal(own_key, extent, jnp.float32)
    if pieces:
        entries = entries * shard_levels(own_key, extent, pieces, -0.22, 0.18)
    return jnp.clip(entries, -limit, limit).astype(kind)


def setup_inputs(seed: int = 0, part: int = 0) -> dict:
    seeds = jax.random.split(jax.random.key(seed), 5)
    part_keys = jax.random.split(jax.random.fold_in(seeds[4], part), 5)
    cell_index = place_ends(jax.random.randint(part_keys[0], (TILES * BLOCKS, BLOCK_PTS), 0, TILE_ROWS * TILE_COLS), jax.random.fold_in(part_keys[0], 1), 0, (TILE_ROWS * TILE_COLS) - 1).astype(jnp.int32)
    weights = scatter_about(part_keys[1], (TILES * BLOCKS, CHANNELS * BLOCK_PTS), 1.0, 6.0, ((0, 32),))
    block_tile = draw_block_tile(jax.random.fold_in(jax.random.fold_in(seeds[4], part), 71), part)
    spread = jnp.clip(jnp.exp(jax.random.uniform(seeds[3], (2, CHANNELS), jnp.float32, math.log(3.0), math.log(8.0))), 3.0, 8.0)
    return {"cell_index": cell_index, "weights": weights, "block_tile": block_tile, "spread": spread}


def kernel_taps(width):
    offsets = jnp.arange(-REACH, REACH + 1).astype(jnp.float32)
    return jnp.exp(-(offsets[None, :] * offsets[None, :]) / (2.0 * width[:, None] * width[:, None]))


def reference(cell_index, weights, block_tile, spread):
    tile_row = block_tile // N_COL
    tile_col = block_tile % N_COL
    point_row = tile_row[:, None] * TILE_ROWS + cell_index // TILE_COLS
    point_col = tile_col[:, None] * TILE_COLS + cell_index % TILE_COLS
    values = weights.astype(jnp.float32).reshape(-1, CHANNELS, BLOCK_PTS)
    channel = jnp.arange(CHANNELS).astype(jnp.int32)[None, :, None]
    density_raw = jnp.zeros((CHANNELS, GRID_ROWS, GRID_COLS), jnp.float32)
    density_raw = density_raw.at[channel, point_row[:, None, :], point_col[:, None, :]].add(values)
    col_taps = kernel_taps(spread[1])
    row_taps = kernel_taps(spread[0])
    padded = jnp.pad(density_raw, ((0, 0), (0, 0), (REACH, REACH)))
    smoothed = jnp.zeros((CHANNELS, GRID_ROWS, GRID_COLS), jnp.float32)
    for offset in range(2 * REACH + 1):
        smoothed = smoothed + col_taps[:, offset, None, None] * padded[:, :, offset:offset + GRID_COLS]
    padded = jnp.pad(smoothed, ((0, 0), (REACH, REACH), (0, 0)))
    density = jnp.zeros((CHANNELS, GRID_ROWS, GRID_COLS), jnp.float32)
    for offset in range(2 * REACH + 1):
        density = density + row_taps[:, offset, None, None] * padded[:, offset:offset + GRID_ROWS, :]
    return density
```

```python
import functools

import jax
import jax.numpy as jnp
from jax import lax
from jax.experimental import pallas as pl
from jax.experimental.pallas import tpu as pltpu
from jax.sharding import PartitionSpec as P

REACH = 16
TILE_ROWS = 256
TILE_COLS = 1024
CAPACITY = 3
LANES = 128
WINDOW = 88
MESH = pl.DeviceIdType.MESH
F32 = jnp.float32
BF16 = jnp.bfloat16


def iota(shape, dim):
    return lax.broadcasted_iota(jnp.int32, shape, dim)


def exchange_kernel(
    rows_n, cols_n, cell_ref, weight_ref, tile_ref, cells_out, weights_out,
    ranks, values, sorted_points, send_cells, send_weights, send_sem, recv_sem, local_sem
):
    blocks, points = cell_ref.shape
    channels = weight_ref.shape[1] // points
    peers = rows_n * cols_n
    my_row, my_col = lax.axis_index("row"), lax.axis_index("col")
    me = my_row * cols_n + my_col

    offsets = []
    for distance in range(rows_n // 2, 0, -1):
        for step in (distance, rows_n - distance):
            if step not in [o[0] for o in offsets]:
                offsets += [(step, c) for c in range(cols_n)]
    offsets += [(0, c) for c in range(1, cols_n)]

    barrier = pltpu.get_barrier_semaphore()
    targets = []
    for step, turn in offsets:
        row = lax.rem(my_row + step, rows_n)
        col = lax.rem(my_col + turn, cols_n)
        targets.append((row, col))
        pl.semaphore_signal(
            barrier, inc=1, device_id={"row": row, "col": col}, device_id_type=MESH
        )

    cells = cell_ref[...]
    point_row = cells // TILE_COLS
    col = cells % TILE_COLS
    key = (point_row * points + iota(cells.shape, 1)).astype(F32)
    pad = jnp.zeros((points - blocks, points), F32)
    key_t = jnp.transpose(jnp.concatenate([key, pad], axis=0))
    weights = weight_ref[...].astype(F32)
    values[0] = point_row.astype(F32)
    values[1] = (col // LANES).astype(F32)
    values[2] = (col % LANES).astype(F32)
    for c in range(channels):
        values[3 + c] = weights[:, c * points : (c + 1) * points]
    quarter = points // 4
    position = iota((points, points), 0)
    for b in range(blocks):
        less = (key_t[:, b : b + 1] < key[b : b + 1, :]).astype(F32)
        rank = jnp.sum(less, axis=0, keepdims=True).astype(jnp.int32)
        lane = (rank % 4) * quarter + rank // 4
        hot = (position == lane).astype(BF16)
        piece = jnp.concatenate(
            [values[v, b : b + 1, :] for v in range(3 + channels)]
            + [jnp.zeros((1, points), F32)],
            axis=0,
        ).astype(BF16)
        sorted_points[b] = lax.dot_general(
            piece, hot, (((1,), (1,)), ((), ())), preferred_element_type=F32
        )

    tile = tile_ref[...]
    tile_down = jnp.sum(
        jnp.where(iota((blocks, blocks), 0) == iota((blocks, blocks), 1), tile, 0),
        axis=1,
        keepdims=True,
    )
    earlier = (tile_down == tile) & (iota((blocks, blocks), 0) < iota((blocks, blocks), 1))
    turn_of = jnp.sum(earlier.astype(jnp.int32), axis=0, keepdims=True)
    for k in range(CAPACITY):
        place = (
            (iota((peers, blocks), 0) == tile) & (turn_of == k)
        ).astype(BF16)
        placed = [
            lax.dot_general(
                place,
                sorted_points[:, v, :].astype(BF16),
                (((1,), (0,)), ((), ())),
                preferred_element_type=F32,
            )
            for v in range(3 + channels)
        ]
        cell = placed[0] * TILE_COLS + placed[1] * LANES + placed[2]
        send_cells[:, k, :] = cell.astype(jnp.int32)
        for c in range(channels):
            send_weights[:, k * channels + c, :] = placed[3 + c].astype(BF16)

    own = [
        pltpu.make_async_copy(send_cells.at[me], cells_out.at[me], local_sem.at[0]),
        pltpu.make_async_copy(send_weights.at[me], weights_out.at[me], local_sem.at[1]),
    ]
    pl.semaphore_wait(barrier, peers - 1)
    copies = []
    for i, (row, col) in enumerate(targets):
        peer = row * cols_n + col
        for a, (source, out) in enumerate(
            ((send_cells, cells_out), (send_weights, weights_out))
        ):
            copy = pltpu.make_async_remote_copy(
                src_ref=source.at[peer],
                dst_ref=out.at[me],
                send_sem=send_sem.at[a, i],
                recv_sem=recv_sem.at[a, i],
                device_id={"row": row, "col": col},
                device_id_type=MESH,
            )
            copy.start()
            copies.append(copy)
    for copy in own:
        copy.start()
    for copy in own:
        copy.wait()
    for copy in copies:
        copy.wait_recv()
    for copy in copies:
        copy.wait_send()


def exchange(cell_index, weights, block_tile, rows_n, cols_n):
    blocks, points = cell_index.shape
    channels = weights.shape[1] // points
    peers = rows_n * cols_n
    vmem = pl.BlockSpec(memory_space=pltpu.VMEM)
    return pl.pallas_call(
        functools.partial(exchange_kernel, rows_n, cols_n),
        name="exchange",
        out_shape=(
            jax.ShapeDtypeStruct((peers, CAPACITY, points), jnp.int32),
            jax.ShapeDtypeStruct((peers, CAPACITY * channels, points), BF16),
        ),
        in_specs=[vmem] * 3,
        out_specs=(vmem, vmem),
        scratch_shapes=[
            pltpu.VMEM((blocks, points), F32),
            pltpu.VMEM((3 + channels, blocks, points), F32),
            pltpu.VMEM((blocks, 8, points), F32),
            pltpu.VMEM((peers, CAPACITY, points), jnp.int32),
            pltpu.VMEM((peers, CAPACITY * channels, points), BF16),
            pltpu.SemaphoreType.DMA((2, peers - 1)),
            pltpu.SemaphoreType.DMA((2, peers - 1)),
            pltpu.SemaphoreType.DMA((2,)),
        ],
        compiler_params=pltpu.CompilerParams(collective_id=0, has_side_effects=True),
    )(cell_index, weights, block_tile.reshape(1, -1))


def turned(slots, quarter):
    wide = jnp.concatenate(
        [
            jnp.concatenate([s[:, v * quarter : (v + 1) * quarter] for v in range(4)], axis=0)
            for s in slots
        ]
        + [jnp.zeros((LANES, LANES - len(slots) * quarter), F32)],
        axis=1,
    )
    return jnp.transpose(wide)


def scatter_kernel(cells_ref, weights_ref, raw_ref, rows_s, cols_s, weights_s, wide_s):
    senders, slots, points = cells_ref.shape
    channels = weights_ref.shape[1] // slots
    quarter = points // 4
    raw_ref[...] = jnp.zeros_like(raw_ref)
    wide_s[...] = weights_ref[...].astype(F32)
    cells = turned([cells_ref[:, k, :].astype(F32) for k in range(slots)], quarter).astype(jnp.int32)
    rows_s[...] = cells // TILE_COLS
    cols_s[...] = cells % TILE_COLS
    for c in range(channels):
        weights_s[c] = turned([wide_s[:, k * channels + c, :] for k in range(slots)], quarter)
    chunk_rows = 2
    chunks = quarter // chunk_rows
    span = 256

    def chunk(j, carry):
        def take(ref):
            return jnp.concatenate(
                [
                    ref[pl.ds(quarter * k + chunk_rows * j + i, 1), :]
                    for k in range(slots)
                    for i in range(chunk_rows)
                ],
                axis=1,
            )

        row = take(rows_s)
        col = take(cols_s)
        weight = [take(weights_s.at[c]) for c in range(channels)]
        first = jnp.min(row) // 8 * 8
        last = jnp.max(row)
        count = row.shape[1]

        def window(low):
            base = pl.multiple_of(jnp.minimum(low, TILE_ROWS - WINDOW), 8)
            offset = jnp.where(row >= low, row - base, -1)
            hot = iota((WINDOW, count), 0) == offset
            left = jnp.concatenate(
                [jnp.where(hot, weight[c], 0.0).astype(BF16) for c in range(channels)], axis=0
            )
            for g in range(TILE_COLS // span):
                right = (iota((span, count), 0) == col - g * span).astype(F32).astype(BF16)
                layer = lax.dot_general(
                    left, right, (((1,), (1,)), ((), ())), preferred_element_type=F32
                )
                for c in range(channels):
                    raw_ref[c, pl.ds(base, WINDOW), g * span : (g + 1) * span] += layer[
                        c * WINDOW : (c + 1) * WINDOW
                    ]
            return low + WINDOW

        lax.while_loop(lambda low: low <= last, window, first)
        return carry

    lax.fori_loop(0, chunks, chunk, 0)


def scatter(cells, weights):
    senders, slots, points = cells.shape
    channels = weights.shape[1] // slots
    vmem = pl.BlockSpec(memory_space=pltpu.VMEM)
    return pl.pallas_call(
        scatter_kernel,
        name="scatter",
        out_shape=jax.ShapeDtypeStruct((channels, TILE_ROWS, TILE_COLS), F32),
        in_specs=[vmem] * 2,
        out_specs=vmem,
        scratch_shapes=[
            pltpu.VMEM((LANES, LANES), jnp.int32),
            pltpu.VMEM((LANES, LANES), jnp.int32),
            pltpu.VMEM((channels, LANES, LANES), F32),
            pltpu.VMEM((senders, slots * channels, points), F32),
        ],
        cost_estimate=pl.CostEstimate(
            flops=2 * channels * WINDOW * TILE_COLS * senders * slots * points,
            bytes_accessed=4 * channels * TILE_ROWS * TILE_COLS,
            transcendentals=0,
        ),
    )(cells, weights)


def split(value):
    high = value.astype(BF16)
    return high, (value - high.astype(F32)).astype(BF16)


def tap(offset, width):
    near = jnp.abs(offset) <= REACH
    far = offset.astype(F32)
    return jnp.where(near, jnp.exp(-(far * far) / (2.0 * width * width)), 0.0)


def dot(a, b):
    return lax.dot_general(a, b, (((1,), (0,)), ((), ())), preferred_element_type=F32)


def smooth_kernel(spread_ref, raw_ref, up_ref, down_ref, side_ref, out_ref, tall, rows_done):
    c = pl.program_id(0)
    half = TILE_ROWS // 2
    tall_rows = TILE_ROWS + 2 * REACH
    wide = TILE_COLS + LANES
    tall[0:REACH, :TILE_COLS] = up_ref[0]
    tall[REACH : REACH + TILE_ROWS, :TILE_COLS] = raw_ref[0]
    tall[REACH + TILE_ROWS :, :TILE_COLS] = down_ref[0]
    tall[:, TILE_COLS:] = side_ref[0]
    row_width = spread_ref[0, c]
    col_width = spread_ref[1, c]
    for h in range(2):
        top = h * 2 * REACH
        depth = TILE_ROWS
        target = iota((half, depth), 0) + h * half
        source = iota((half, depth), 1) + top - REACH
        band_high, band_low = split(tap(source - target, row_width))
        x_high, x_low = split(tall[top : top + depth, :])
        both = dot(jnp.concatenate([band_high, band_low], axis=0), x_high)
        rows_done[h * half : (h + 1) * half, :] = (
            both[:half] + both[half:] + dot(band_high, x_low)
        )
    source = iota((2 * LANES, LANES), 0)
    target = iota((2 * LANES, LANES), 1)
    source = jnp.where(
        source < LANES + LANES // 2, source, source - 2 * LANES
    )
    band_high, band_low = split(tap(source - target, col_width))
    band = jnp.concatenate([band_high, band_low], axis=1)
    lanes = iota((TILE_ROWS, LANES), 1)
    count = TILE_COLS // LANES
    for n in range(count):
        before = n - 1 if n else count
        after = n + 1 if n + 1 < count else count
        own = rows_done[:, n * LANES : (n + 1) * LANES]
        edge = jnp.where(
            lanes < LANES // 2,
            rows_done[:, after * LANES : (after + 1) * LANES],
            rows_done[:, before * LANES : (before + 1) * LANES],
        )
        x_high, x_low = split(jnp.concatenate([own, edge], axis=1))
        both = dot(x_high, band)
        out_ref[0, :, n * LANES : (n + 1) * LANES] = (
            both[:, :LANES] + both[:, LANES:] + dot(x_low, band_high)
        )


def smooth(spread, raw, up, down, side):
    channels = raw.shape[0]
    tall = TILE_ROWS + 2 * REACH

    def block(rows, cols):
        return pl.BlockSpec((1, rows, cols), lambda c: (c, 0, 0))

    return pl.pallas_call(
        smooth_kernel,
        name="smooth",
        grid=(channels,),
        out_shape=jax.ShapeDtypeStruct((channels, TILE_ROWS, TILE_COLS), F32),
        in_specs=[
            pl.BlockSpec(memory_space=pltpu.SMEM),
            block(TILE_ROWS, TILE_COLS),
            block(REACH, TILE_COLS),
            block(REACH, TILE_COLS),
            block(tall, LANES),
        ],
        out_specs=block(TILE_ROWS, TILE_COLS),
        scratch_shapes=[
            pltpu.VMEM((tall, TILE_COLS + LANES), F32),
            pltpu.VMEM((TILE_ROWS, TILE_COLS + LANES), F32),
        ],
    )(spread, raw, up, down, side)


def neighbours(value, axis, dim, width):
    count, length = lax.axis_size(axis), value.shape[dim]
    up = [(i, i + 1) for i in range(count - 1)]
    down = [(j, i) for i, j in up]
    last = lax.slice_in_dim(value, length - width, length, axis=dim)
    first = lax.slice_in_dim(value, 0, width, axis=dim)
    return lax.ppermute(last, axis, up), lax.ppermute(first, axis, down)


def shards(cell_index, weights, block_tile, spread):
    rows_n, cols_n = lax.axis_size("row"), lax.axis_size("col")
    cells, points = exchange(cell_index, weights, block_tile, rows_n, cols_n)
    raw = scatter(cells, points)
    up, down = neighbours(raw, "row", 1, REACH)
    edges = jnp.concatenate(
        [
            jnp.concatenate([a[:, :, :REACH], a[:, :, -REACH:]], axis=2)
            for a in (up, raw, down)
        ],
        axis=1,
    )
    left, right = neighbours(edges, "col", 2, REACH)
    middle = jnp.zeros(edges.shape[:2] + (LANES - 2 * REACH,), F32)
    side = jnp.concatenate([right, middle, left], axis=2)
    return smooth(spread, raw, up, down, side)


def solution(mesh):
    return jax.shard_map(
        shards,
        mesh=mesh,
        in_specs=(
            P(("groups", "row", "col"), None),
            P(("groups", "row", "col"), None),
            P(("groups", "row", "col")),
            P(),
        ),
        out_specs=P(None, ("groups", "row"), "col"),
        check_vma=False,
    )
```

```python
import functools

import jax
import jax.numpy as jnp
from jax import lax
from jax.experimental import pallas as pl
from jax.experimental.pallas import tpu as pltpu
from jax.sharding import PartitionSpec as P

REACH = 16
TILE_ROWS = 256
TILE_COLS = 1024
CAPACITY = 3
LANES = 128
WINDOW = 80
MESH = pl.DeviceIdType.MESH
F32 = jnp.float32
BF16 = jnp.bfloat16


def iota(shape, dim):
    return lax.broadcasted_iota(jnp.int32, shape, dim)


def exchange_kernel(
    rows_n, cols_n, cell_ref, weight_ref, tile_ref, cells_out, weights_out,
    ranks, values, sorted_points, send_cells, send_weights, send_sem, recv_sem, local_sem
):
    blocks, points = cell_ref.shape
    channels = weight_ref.shape[1] // points
    peers = rows_n * cols_n
    my_row, my_col = lax.axis_index("row"), lax.axis_index("col")
    me = my_row * cols_n + my_col

    offsets = []
    for distance in range(rows_n // 2, 0, -1):
        for step in (distance, rows_n - distance):
            if step not in [o[0] for o in offsets]:
                offsets += [(step, c) for c in range(cols_n)]
    offsets += [(0, c) for c in range(1, cols_n)]

    barrier = pltpu.get_barrier_semaphore()
    targets = []
    for step, turn in offsets:
        row = lax.rem(my_row + step, rows_n)
        col = lax.rem(my_col + turn, cols_n)
        targets.append((row, col))
        pl.semaphore_signal(
            barrier, inc=1, device_id={"row": row, "col": col}, device_id_type=MESH
        )

    cells = cell_ref[...]
    point_row = cells // TILE_COLS
    col = cells % TILE_COLS
    key = (point_row * points + iota(cells.shape, 1)).astype(F32)
    pad = jnp.zeros((points - blocks, points), F32)
    key_t = jnp.transpose(jnp.concatenate([key, pad], axis=0))
    weights = weight_ref[...].astype(F32)
    values[0] = point_row.astype(F32)
    values[1] = (col // LANES).astype(F32)
    values[2] = (col % LANES).astype(F32)
    for c in range(channels):
        values[3 + c] = weights[:, c * points : (c + 1) * points]
    quarter = points // 4
    position = iota((points, points), 0)
    for b in range(blocks):
        less = (key_t[:, b : b + 1] < key[b : b + 1, :]).astype(F32)
        rank = jnp.sum(less, axis=0, keepdims=True).astype(jnp.int32)
        lane = (rank % 4) * quarter + rank // 4
        hot = (position == lane).astype(BF16)
        piece = jnp.concatenate(
            [values[v, b : b + 1, :] for v in range(3 + channels)]
            + [jnp.zeros((1, points), F32)],
            axis=0,
        ).astype(BF16)
        sorted_points[b] = lax.dot_general(
            piece, hot, (((1,), (1,)), ((), ())), preferred_element_type=F32
        )

    tile = tile_ref[...]
    tile_down = jnp.sum(
        jnp.where(iota((blocks, blocks), 0) == iota((blocks, blocks), 1), tile, 0),
        axis=1,
        keepdims=True,
    )
    earlier = (tile_down == tile) & (iota((blocks, blocks), 0) < iota((blocks, blocks), 1))
    turn_of = jnp.sum(earlier.astype(jnp.int32), axis=0, keepdims=True)
    lane = iota((1, points), 1)
    ramp = ((lane % quarter) * 4 + lane // quarter) * (TILE_ROWS // points) * TILE_COLS
    for k in range(CAPACITY):
        chosen = ((iota((peers, blocks), 0) == tile) & (turn_of == k)).astype(F32)
        empty = jnp.sum(chosen, axis=1, keepdims=True) < 0.5
        place = chosen.astype(BF16)
        placed = [
            lax.dot_general(
                place,
                sorted_points[:, v, :].astype(BF16),
                (((1,), (0,)), ((), ())),
                preferred_element_type=F32,
            )
            for v in range(3 + channels)
        ]
        cell = placed[0] * TILE_COLS + placed[1] * LANES + placed[2]
        send_cells[:, k, :] = jnp.where(empty, ramp, cell.astype(jnp.int32))
        for c in range(channels):
            send_weights[:, k * channels + c, :] = placed[3 + c].astype(BF16)

    own = [
        pltpu.make_async_copy(send_cells.at[me], cells_out.at[me], local_sem.at[0]),
        pltpu.make_async_copy(send_weights.at[me], weights_out.at[me], local_sem.at[1]),
    ]
    pl.semaphore_wait(barrier, peers - 1)
    copies = []
    for i, (row, col) in enumerate(targets):
        peer = row * cols_n + col
        for a, (source, out) in enumerate(
            ((send_cells, cells_out), (send_weights, weights_out))
        ):
            copy = pltpu.make_async_remote_copy(
                src_ref=source.at[peer],
                dst_ref=out.at[me],
                send_sem=send_sem.at[a, i],
                recv_sem=recv_sem.at[a, i],
                device_id={"row": row, "col": col},
                device_id_type=MESH,
            )
            copy.start()
            copies.append(copy)
    for copy in own:
        copy.start()
    for copy in own:
        copy.wait()
    for copy in copies:
        copy.wait_recv()
    for copy in copies:
        copy.wait_send()


def exchange(cell_index, weights, block_tile, rows_n, cols_n):
    blocks, points = cell_index.shape
    channels = weights.shape[1] // points
    peers = rows_n * cols_n
    vmem = pl.BlockSpec(memory_space=pltpu.VMEM)
    return pl.pallas_call(
        functools.partial(exchange_kernel, rows_n, cols_n),
        name="exchange",
        out_shape=(
            jax.ShapeDtypeStruct((peers, CAPACITY, points), jnp.int32),
            jax.ShapeDtypeStruct((peers, CAPACITY * channels, points), BF16),
        ),
        in_specs=[vmem] * 3,
        out_specs=(vmem, vmem),
        scratch_shapes=[
            pltpu.VMEM((blocks, points), F32),
            pltpu.VMEM((3 + channels, blocks, points), F32),
            pltpu.VMEM((blocks, 8, points), F32),
            pltpu.VMEM((peers, CAPACITY, points), jnp.int32),
            pltpu.VMEM((peers, CAPACITY * channels, points), BF16),
            pltpu.SemaphoreType.DMA((2, peers - 1)),
            pltpu.SemaphoreType.DMA((2, peers - 1)),
            pltpu.SemaphoreType.DMA((2,)),
        ],
        compiler_params=pltpu.CompilerParams(collective_id=0, has_side_effects=True, vmem_limit_bytes=8 << 20),
    )(cell_index, weights, block_tile.reshape(1, -1))


def turned(slots, quarter):
    wide = jnp.concatenate(
        [
            jnp.concatenate([s[:, v * quarter : (v + 1) * quarter] for v in range(4)], axis=0)
            for s in slots
        ]
        + [jnp.zeros((LANES, LANES - len(slots) * quarter), F32)],
        axis=1,
    )
    return jnp.transpose(wide)


def scatter_kernel(cells_ref, weights_ref, raw_ref, rows_s, cols_s, weights_s, wide_s):
    senders, slots, points = cells_ref.shape
    channels = weights_ref.shape[1] // slots
    quarter = points // 4
    raw_ref[...] = jnp.zeros_like(raw_ref)
    wide_s[...] = weights_ref[...].astype(F32)
    cells = turned([cells_ref[:, k, :].astype(F32) for k in range(slots)], quarter).astype(jnp.int32)
    rows_s[...] = cells // TILE_COLS
    cols_s[...] = cells % TILE_COLS
    for c in range(channels):
        weights_s[c] = turned([wide_s[:, k * channels + c, :] for k in range(slots)], quarter)
    chunk_rows = 2
    chunks = quarter // chunk_rows
    span = 256

    def chunk(j, carry):
        def take(ref):
            return jnp.concatenate(
                [
                    ref[pl.ds(quarter * k + chunk_rows * j + i, 1), :]
                    for k in range(slots)
                    for i in range(chunk_rows)
                ],
                axis=1,
            )

        row = take(rows_s)
        col = take(cols_s)
        weight = [take(weights_s.at[c]) for c in range(channels)]
        first = jnp.min(row) // 8 * 8
        last = jnp.max(row)
        count = row.shape[1]

        def window(low):
            base = pl.multiple_of(jnp.minimum(low, TILE_ROWS - WINDOW), 8)
            offset = jnp.where(row >= low, row - base, -1)
            hot = iota((WINDOW, count), 0) == offset
            left = jnp.concatenate(
                [jnp.where(hot, weight[c], 0.0).astype(BF16) for c in range(channels)], axis=0
            )
            for g in range(TILE_COLS // span):
                right = (iota((span, count), 0) == col - g * span).astype(F32).astype(BF16)
                layer = lax.dot_general(
                    left, right, (((1,), (1,)), ((), ())), preferred_element_type=F32
                )
                for c in range(channels):
                    raw_ref[c, pl.ds(base, WINDOW), g * span : (g + 1) * span] += layer[
                        c * WINDOW : (c + 1) * WINDOW
                    ]
            return low + WINDOW

        lax.while_loop(lambda low: low <= last, window, first)
        return carry

    lax.fori_loop(0, chunks, chunk, 0)


def scatter(cells, weights):
    senders, slots, points = cells.shape
    channels = weights.shape[1] // slots
    vmem = pl.BlockSpec(memory_space=pltpu.VMEM)
    return pl.pallas_call(
        scatter_kernel,
        name="scatter",
        out_shape=jax.ShapeDtypeStruct((channels, TILE_ROWS, TILE_COLS), F32),
        in_specs=[vmem] * 2,
        out_specs=vmem,
        scratch_shapes=[
            pltpu.VMEM((LANES, LANES), jnp.int32),
            pltpu.VMEM((LANES, LANES), jnp.int32),
            pltpu.VMEM((channels, LANES, LANES), F32),
            pltpu.VMEM((senders, slots * channels, points), F32),
        ],
        compiler_params=pltpu.CompilerParams(vmem_limit_bytes=16 << 20),
        cost_estimate=pl.CostEstimate(
            flops=2 * channels * WINDOW * TILE_COLS * senders * slots * points,
            bytes_accessed=4 * channels * TILE_ROWS * TILE_COLS,
            transcendentals=0,
        ),
    )(cells, weights)


def split(value):
    high = value.astype(BF16)
    return high, (value - high.astype(F32)).astype(BF16)


def tap(offset, width):
    near = jnp.abs(offset) <= REACH
    far = offset.astype(F32)
    return jnp.where(near, jnp.exp(-(far * far) / (2.0 * width * width)), 0.0)


def dot(a, b):
    return lax.dot_general(a, b, (((1,), (0,)), ((), ())), preferred_element_type=F32)


def smooth_kernel(
    rows_n, cols_n, spread_ref, raw_ref, out_ref, tall, side, above, below, send_sem, recv_sem
):
    channels, height, width = raw_ref.shape
    my_row, my_col = lax.axis_index("row"), lax.axis_index("col")
    other = lax.rem(my_col + 1, cols_n)
    prev = lax.rem(my_row + rows_n - 1, rows_n)
    following = lax.rem(my_row + 1, rows_n)

    def at(row, col):
        return {"row": row, "col": col}

    barrier = pltpu.get_barrier_semaphore()
    peers = [at(prev, my_col), at(following, my_col), at(prev, other), at(following, other), at(my_row, other)]
    for peer in peers:
        pl.semaphore_signal(barrier, inc=1, device_id=peer, device_id_type=MESH)
    pl.semaphore_wait(barrier, len(peers))
    near = pl.ds(pl.multiple_of((1 - my_col) * (width - LANES), LANES), LANES)
    main = pl.ds(0, width)
    beyond = pl.ds(width, LANES)
    top, bottom = pl.ds(0, REACH), pl.ds(height - REACH, REACH)

    def copies(c, only=slice(0, 5)):
        plan = [
            (raw_ref.at[c, :, near], side.at[c], peers[4]),
            (raw_ref.at[c, bottom, near], above.at[c, :, beyond], peers[3]),
            (raw_ref.at[c, top, near], below.at[c, :, beyond], peers[2]),
            (raw_ref.at[c, bottom, main], above.at[c, :, main], peers[1]),
            (raw_ref.at[c, top, main], below.at[c, :, main], peers[0]),
        ]
        return [
            pltpu.make_async_remote_copy(
                src_ref=source, dst_ref=target, send_sem=send_sem.at[i, c], recv_sem=recv_sem.at[i, c],
                device_id=peer, device_id_type=MESH,
            )
            for i, (source, target, peer) in list(enumerate(plan))[only]
        ]

    for c in range(channels):
        for copy in copies(c):
            copy.start()

    def row_band(c):
        return split(tap(iota((height, height), 1) - iota((height, height), 0), spread_ref[0, c]))

    def along_rows(c, high, low, x):
        x_high, x_low = split(x)
        both = dot(jnp.concatenate([high, low], axis=0), x_high)
        return both[:height] + both[height:] + dot(high, x_low)

    step = 2 * LANES

    def own_rows(c, carry):
        high, low = row_band(c)
        for g in range(width // step):
            cols = slice(g * step, (g + 1) * step)
            tall[c, :, cols] = along_rows(c, high, low, raw_ref[c, :, cols])
        return carry

    lax.fori_loop(0, channels, own_rows, 0)

    lane = iota((height, LANES), 1)
    count = width // LANES

    def along_cols(c, rows):
        size = rows.stop - rows.start
        source = iota((2 * LANES, LANES), 0)
        source = jnp.where(source < LANES + LANES // 2, source, source - 2 * LANES)
        high, low = split(tap(source - iota((2 * LANES, LANES), 1), spread_ref[1, c]))
        band = jnp.concatenate([high, low], axis=1)
        outer = tall[c, rows, width:]
        for n in range(count):
            if n:
                before = tall[c, rows, (n - 1) * LANES : n * LANES]
            else:
                before = jnp.where(my_col > 0, outer, 0.0)
            if n + 1 < count:
                after = tall[c, rows, (n + 1) * LANES : (n + 2) * LANES]
            else:
                after = jnp.where(my_col + 1 < cols_n, outer, 0.0)
            edge = jnp.where(lane[:size] < LANES // 2, after, before)
            own = tall[c, rows, n * LANES : (n + 1) * LANES]
            x_high, x_low = split(jnp.concatenate([own, edge], axis=1))
            both = dot(x_high, band)
            out_ref[c, rows, n * LANES : (n + 1) * LANES] = (
                both[:, :LANES] + both[:, LANES:] + dot(x_low, high)
            )

    def inner(c, carry):
        for copy in copies(c, slice(0, 1)):
            copy.wait_recv()
        high, low = row_band(c)
        tall[c, :, width:] = along_rows(c, high, low, side[c])
        along_cols(c, slice(REACH, height - REACH))
        return carry

    lax.fori_loop(0, channels, inner, 0)

    def outer_rows(c, carry):
        for copy in copies(c, slice(1, 5)):
            copy.wait_recv()
        part = iota((REACH, 3 * REACH), 1)
        offset = part % REACH - iota((REACH, 3 * REACH), 0)
        for halo, rows, shift, real in (
            (above, slice(0, REACH), -REACH, my_row > 0),
            (below, slice(height - REACH, height), REACH, my_row + 1 < rows_n),
        ):
            taps = tap(offset + shift, spread_ref[0, c])
            taps = jnp.where(real, taps, 0.0)
            high = taps.astype(BF16).astype(F32)
            taps = jnp.where(part // REACH == 1, taps - high, high).astype(BF16)
            x_high, x_low = split(halo[c])
            tall[c, rows, :] += dot(taps, jnp.concatenate([x_high, x_high, x_low], axis=0))
            along_cols(c, rows)
        return carry

    lax.fori_loop(0, channels, outer_rows, 0)
    for c in range(channels):
        for copy in copies(c):
            copy.wait_send()


def smooth(spread, raw, rows_n, cols_n):
    channels, height, width = raw.shape
    vmem = pl.BlockSpec(memory_space=pltpu.VMEM)
    return pl.pallas_call(
        functools.partial(smooth_kernel, rows_n, cols_n),
        name="smooth",
        out_shape=jax.ShapeDtypeStruct(raw.shape, F32),
        in_specs=[pl.BlockSpec(memory_space=pltpu.SMEM), vmem],
        out_specs=vmem,
        scratch_shapes=[
            pltpu.VMEM((channels, height, width + LANES), F32),
            pltpu.VMEM((channels, height, LANES), F32),
            pltpu.VMEM((channels, REACH, width + LANES), F32),
            pltpu.VMEM((channels, REACH, width + LANES), F32),
            pltpu.SemaphoreType.DMA((5, channels)),
            pltpu.SemaphoreType.DMA((5, channels)),
        ],
        compiler_params=pltpu.CompilerParams(
            collective_id=1, has_side_effects=True, vmem_limit_bytes=24 << 20
        ),
    )(spread, raw)


def shards(cell_index, weights, block_tile, spread):
    rows_n, cols_n = lax.axis_size("row"), lax.axis_size("col")
    cells, points = exchange(cell_index, weights, block_tile, rows_n, cols_n)
    raw = scatter(cells, points)
    return smooth(spread, raw, rows_n, cols_n)


def solution(mesh):
    return jax.shard_map(
        shards,
        mesh=mesh,
        in_specs=(
            P(("groups", "row", "col"), None),
            P(("groups", "row", "col"), None),
            P(("groups", "row", "col")),
            P(),
        ),
        out_specs=P(None, ("groups", "row"), "col"),
        check_vma=False,
    )
```

```python
import functools

import jax
import jax.numpy as jnp
from jax import lax
from jax.experimental import pallas as pl
from jax.experimental.pallas import tpu as pltpu
from jax.sharding import PartitionSpec as P

REACH = 16
TILE_ROWS = 256
TILE_COLS = 1024
CAPACITY = 3
LANES = 128
WINDOW = 80
UNROLL = 4
MESH = pl.DeviceIdType.MESH
F32 = jnp.float32
BF16 = jnp.bfloat16


def iota(shape, dim):
    return lax.broadcasted_iota(jnp.int32, shape, dim)


def exchange_kernel(
    rows_n, cols_n, cell_hbm, weight_hbm, tile_hbm, cells_out, weights_out,
    cell_ref, weight_ref, tile_ref, values, sorted_points, send_cells, send_weights,
    send_sem, recv_sem, local_sem
):
    loads = [
        pltpu.make_async_copy(source, target, local_sem.at[2 + i])
        for i, (source, target) in enumerate(
            ((cell_hbm, cell_ref), (weight_hbm, weight_ref), (tile_hbm, tile_ref))
        )
    ]
    for load in loads:
        load.start()
    blocks, points = cell_ref.shape
    channels = weight_ref.shape[1] // points
    peers = rows_n * cols_n
    my_row, my_col = lax.axis_index("row"), lax.axis_index("col")
    me = my_row * cols_n + my_col

    offsets = []
    for distance in range(rows_n // 2, 0, -1):
        for step in (distance, rows_n - distance):
            if step not in [o[0] for o in offsets]:
                offsets += [(step, c) for c in range(cols_n)]
    offsets += [(0, c) for c in range(1, cols_n)]

    barrier = pltpu.get_barrier_semaphore()
    targets = []
    for step, turn in offsets:
        row = lax.rem(my_row + step, rows_n)
        col = lax.rem(my_col + turn, cols_n)
        targets.append((row, col))
        pl.semaphore_signal(
            barrier, inc=1, device_id={"row": row, "col": col}, device_id_type=MESH
        )

    for load in loads:
        load.wait()
    cells = cell_ref[...]
    point_row = cells // TILE_COLS
    col = cells % TILE_COLS
    key = (point_row * points + iota(cells.shape, 1)).astype(F32)
    pad = jnp.zeros((points - blocks, points), F32)
    key_t = jnp.transpose(jnp.concatenate([key, pad], axis=0))
    weights = weight_ref[...].astype(F32)
    values[0] = point_row.astype(F32)
    values[1] = (col // LANES).astype(F32)
    values[2] = (col % LANES).astype(F32)
    for c in range(channels):
        values[3 + c] = weights[:, c * points : (c + 1) * points]
    quarter = points // 4
    position = iota((points, points), 0)
    for b in range(blocks):
        less = (key_t[:, b : b + 1] < key[b : b + 1, :]).astype(F32)
        rank = jnp.sum(less, axis=0, keepdims=True).astype(jnp.int32)
        lane = (rank % 4) * quarter + rank // 4
        hot = (position == lane).astype(BF16)
        piece = jnp.concatenate(
            [values[v, b : b + 1, :] for v in range(3 + channels)]
            + [jnp.zeros((1, points), F32)],
            axis=0,
        ).astype(BF16)
        sorted_points[b] = lax.dot_general(
            piece, hot, (((1,), (1,)), ((), ())), preferred_element_type=F32
        )

    tile = tile_ref[...]
    tile_down = jnp.sum(
        jnp.where(iota((blocks, blocks), 0) == iota((blocks, blocks), 1), tile, 0),
        axis=1,
        keepdims=True,
    )
    earlier = (tile_down == tile) & (iota((blocks, blocks), 0) < iota((blocks, blocks), 1))
    turn_of = jnp.sum(earlier.astype(jnp.int32), axis=0, keepdims=True)
    lane = iota((1, points), 1)
    ramp = ((lane % quarter) * 4 + lane // quarter) * (TILE_ROWS // points) * TILE_COLS
    for k in range(CAPACITY):
        chosen = ((iota((peers, blocks), 0) == tile) & (turn_of == k)).astype(F32)
        empty = jnp.sum(chosen, axis=1, keepdims=True) < 0.5
        place = chosen.astype(BF16)
        placed = [
            lax.dot_general(
                place,
                sorted_points[:, v, :].astype(BF16),
                (((1,), (0,)), ((), ())),
                preferred_element_type=F32,
            )
            for v in range(3 + channels)
        ]
        cell = placed[0] * TILE_COLS + placed[1] * LANES + placed[2]
        send_cells[:, k, :] = jnp.where(empty, ramp, cell.astype(jnp.int32))
        for c in range(channels):
            send_weights[:, k * channels + c, :] = placed[3 + c].astype(BF16)

    own = [
        pltpu.make_async_copy(send_cells.at[me], cells_out.at[me], local_sem.at[0]),
        pltpu.make_async_copy(send_weights.at[me], weights_out.at[me], local_sem.at[1]),
    ]
    pl.semaphore_wait(barrier, peers - 1)
    copies = []
    for i, (row, col) in enumerate(targets):
        peer = row * cols_n + col
        for a, (source, out) in enumerate(
            ((send_cells, cells_out), (send_weights, weights_out))
        ):
            copy = pltpu.make_async_remote_copy(
                src_ref=source.at[peer],
                dst_ref=out.at[me],
                send_sem=send_sem.at[a, i],
                recv_sem=recv_sem.at[a, i],
                device_id={"row": row, "col": col},
                device_id_type=MESH,
            )
            copy.start()
            copies.append(copy)
    for copy in own:
        copy.start()
    for copy in own:
        copy.wait()
    for copy in copies:
        copy.wait_recv()
    for copy in copies:
        copy.wait_send()


def exchange(cell_index, weights, block_tile, rows_n, cols_n):
    blocks, points = cell_index.shape
    channels = weights.shape[1] // points
    peers = rows_n * cols_n
    vmem = pl.BlockSpec(memory_space=pltpu.VMEM)
    return pl.pallas_call(
        functools.partial(exchange_kernel, rows_n, cols_n),
        name="exchange",
        out_shape=(
            jax.ShapeDtypeStruct((peers, CAPACITY, points), jnp.int32),
            jax.ShapeDtypeStruct((peers, CAPACITY * channels, points), BF16),
        ),
        in_specs=[pl.BlockSpec(memory_space=pltpu.MemorySpace.HBM)] * 3,
        out_specs=(vmem, vmem),
        scratch_shapes=[
            pltpu.VMEM(cell_index.shape, jnp.int32),
            pltpu.VMEM(weights.shape, BF16),
            pltpu.VMEM((1, blocks), jnp.int32),
            pltpu.VMEM((3 + channels, blocks, points), F32),
            pltpu.VMEM((blocks, 8, points), F32),
            pltpu.VMEM((peers, CAPACITY, points), jnp.int32),
            pltpu.VMEM((peers, CAPACITY * channels, points), BF16),
            pltpu.SemaphoreType.DMA((2, peers - 1)),
            pltpu.SemaphoreType.DMA((2, peers - 1)),
            pltpu.SemaphoreType.DMA((5,)),
        ],
        compiler_params=pltpu.CompilerParams(collective_id=0, has_side_effects=True, vmem_limit_bytes=8 << 20),
    )(cell_index, weights, block_tile.reshape(1, -1))


def turned(slots, quarter):
    wide = jnp.concatenate(
        [
            jnp.concatenate([s[:, v * quarter : (v + 1) * quarter] for v in range(4)], axis=0)
            for s in slots
        ]
        + [jnp.zeros((LANES, LANES - len(slots) * quarter), F32)],
        axis=1,
    )
    return jnp.transpose(wide)


def scatter_kernel(cells_ref, weights_ref, raw_ref, rows_s, cols_s, weights_s, wide_s, first_s, last_s):
    senders, slots, points = cells_ref.shape
    channels = weights_ref.shape[1] // slots
    quarter = points // 4
    chunk_rows = 2
    chunks = quarter // chunk_rows
    span = 256
    wide_s[...] = weights_ref[...].astype(F32)
    cells = turned([cells_ref[:, k, :].astype(F32) for k in range(slots)], quarter).astype(jnp.int32)
    rows = cells >> (TILE_COLS.bit_length() - 1)
    rows_s[...] = rows
    cols_s[...] = cells & (TILE_COLS - 1)
    for c in range(channels):
        weights_s[c] = turned([wide_s[:, k * channels + c, :] for k in range(slots)], quarter)
    low, high = rows[:quarter], rows[:quarter]
    for k in range(1, slots):
        low = jnp.minimum(low, rows[quarter * k : quarter * (k + 1)])
        high = jnp.maximum(high, rows[quarter * k : quarter * (k + 1)])
    low = jnp.min(low, axis=1, keepdims=True)
    high = jnp.max(high, axis=1, keepdims=True)
    for j in range(chunks):
        lows = [low[chunk_rows * j + i, 0] for i in range(chunk_rows)]
        highs = [high[chunk_rows * j + i, 0] for i in range(chunk_rows)]
        first_s[j] = (functools.reduce(jnp.minimum, lows) >> 3) << 3
        last_s[j] = functools.reduce(jnp.maximum, highs)
    raw_ref[...] = jnp.zeros_like(raw_ref)

    def window(j, low):
        def take(ref):
            return jnp.concatenate(
                [
                    ref[pl.ds(quarter * k + chunk_rows * j + i, 1), :]
                    for k in range(slots)
                    for i in range(chunk_rows)
                ],
                axis=1,
            )

        row = take(rows_s)
        col = take(cols_s)
        count = row.shape[1]
        base = pl.multiple_of(jnp.minimum(low, TILE_ROWS - WINDOW), 8)
        offset = jnp.where(row >= low, row - base, -1)
        hot = iota((WINDOW, count), 0) == offset
        left = jnp.concatenate(
            [jnp.where(hot, take(weights_s.at[c]), 0.0).astype(BF16) for c in range(channels)],
            axis=0,
        )
        for g in range(TILE_COLS // span):
            right = (iota((span, count), 0) == col - g * span).astype(F32).astype(BF16)
            layer = lax.dot_general(
                left, right, (((1,), (1,)), ((), ())), preferred_element_type=F32
            )
            for c in range(channels):
                raw_ref[c, pl.ds(base, WINDOW), g * span : (g + 1) * span] += layer[
                    c * WINDOW : (c + 1) * WINDOW
                ]

    def common(j, carry):
        window(j, first_s[j])
        return carry

    lax.fori_loop(0, chunks, common, 0, unroll=UNROLL)

    def rest(j, carry):
        def more(low):
            window(j, low)
            return low + WINDOW

        lax.while_loop(lambda low: low <= last_s[j], more, first_s[j] + WINDOW)
        return carry

    lax.fori_loop(0, chunks, rest, 0)


def scatter(cells, weights):
    senders, slots, points = cells.shape
    channels = weights.shape[1] // slots
    vmem = pl.BlockSpec(memory_space=pltpu.VMEM)
    return pl.pallas_call(
        scatter_kernel,
        name="scatter",
        out_shape=jax.ShapeDtypeStruct((channels, TILE_ROWS, TILE_COLS), F32),
        in_specs=[vmem] * 2,
        out_specs=vmem,
        scratch_shapes=[
            pltpu.VMEM((LANES, LANES), jnp.int32),
            pltpu.VMEM((LANES, LANES), jnp.int32),
            pltpu.VMEM((channels, LANES, LANES), F32),
            pltpu.VMEM((senders, slots * channels, points), F32),
            pltpu.SMEM((points // 8,), jnp.int32),
            pltpu.SMEM((points // 8,), jnp.int32),
        ],
        compiler_params=pltpu.CompilerParams(vmem_limit_bytes=16 << 20),
        cost_estimate=pl.CostEstimate(
            flops=2 * channels * WINDOW * TILE_COLS * senders * slots * points,
            bytes_accessed=4 * channels * TILE_ROWS * TILE_COLS,
            transcendentals=0,
        ),
    )(cells, weights)


def split(value):
    high = value.astype(BF16)
    return high, (value - high.astype(F32)).astype(BF16)


def tap(offset, width):
    near = jnp.abs(offset) <= REACH
    far = offset.astype(F32)
    return jnp.where(near, jnp.exp(-(far * far) / (2.0 * width * width)), 0.0)


def dot(a, b):
    return lax.dot_general(a, b, (((1,), (0,)), ((), ())), preferred_element_type=F32)


def smooth_kernel(
    rows_n, cols_n, spread_ref, raw_ref, out_ref, tall, side, above, below, send_sem, recv_sem
):
    channels, height, width = raw_ref.shape
    my_row, my_col = lax.axis_index("row"), lax.axis_index("col")
    other = lax.rem(my_col + 1, cols_n)
    prev = lax.rem(my_row + rows_n - 1, rows_n)
    following = lax.rem(my_row + 1, rows_n)

    def at(row, col):
        return {"row": row, "col": col}

    barrier = pltpu.get_barrier_semaphore()
    peers = [at(prev, my_col), at(following, my_col), at(prev, other), at(following, other), at(my_row, other)]
    for peer in peers:
        pl.semaphore_signal(barrier, inc=1, device_id=peer, device_id_type=MESH)
    pl.semaphore_wait(barrier, len(peers))
    near = pl.ds(pl.multiple_of((1 - my_col) * (width - LANES), LANES), LANES)
    main = pl.ds(0, width)
    beyond = pl.ds(width, LANES)
    top, bottom = pl.ds(0, REACH), pl.ds(height - REACH, REACH)

    def copies(c, only=slice(0, 5)):
        plan = [
            (raw_ref.at[c, :, near], side.at[c], peers[4]),
            (raw_ref.at[c, bottom, near], above.at[c, :, beyond], peers[3]),
            (raw_ref.at[c, top, near], below.at[c, :, beyond], peers[2]),
            (raw_ref.at[c, bottom, main], above.at[c, :, main], peers[1]),
            (raw_ref.at[c, top, main], below.at[c, :, main], peers[0]),
        ]
        return [
            pltpu.make_async_remote_copy(
                src_ref=source, dst_ref=target, send_sem=send_sem.at[i, c], recv_sem=recv_sem.at[i, c],
                device_id=peer, device_id_type=MESH,
            )
            for i, (source, target, peer) in list(enumerate(plan))[only]
        ]

    for c in range(channels):
        for copy in copies(c):
            copy.start()

    def row_band(c):
        return split(tap(iota((height, height), 1) - iota((height, height), 0), spread_ref[0, c]))

    def along_rows(c, high, low, x):
        x_high, x_low = split(x)
        both = dot(jnp.concatenate([high, low], axis=0), x_high)
        return both[:height] + both[height:] + dot(high, x_low)

    step = 2 * LANES

    def own_rows(c, carry):
        high, low = row_band(c)
        for g in range(width // step):
            cols = slice(g * step, (g + 1) * step)
            tall[c, :, cols] = along_rows(c, high, low, raw_ref[c, :, cols])
        return carry

    lax.fori_loop(0, channels, own_rows, 0)

    lane = iota((height, LANES), 1)
    count = width // LANES

    def along_cols(c, rows):
        size = rows.stop - rows.start
        source = iota((2 * LANES, LANES), 0)
        source = jnp.where(source < LANES + LANES // 2, source, source - 2 * LANES)
        high, low = split(tap(source - iota((2 * LANES, LANES), 1), spread_ref[1, c]))
        band = jnp.concatenate([high, low], axis=1)
        outer = tall[c, rows, width:]
        for n in range(count):
            if n:
                before = tall[c, rows, (n - 1) * LANES : n * LANES]
            else:
                before = jnp.where(my_col > 0, outer, 0.0)
            if n + 1 < count:
                after = tall[c, rows, (n + 1) * LANES : (n + 2) * LANES]
            else:
                after = jnp.where(my_col + 1 < cols_n, outer, 0.0)
            edge = jnp.where(lane[:size] < LANES // 2, after, before)
            own = tall[c, rows, n * LANES : (n + 1) * LANES]
            x_high, x_low = split(jnp.concatenate([own, edge], axis=1))
            both = dot(x_high, band)
            out_ref[c, rows, n * LANES : (n + 1) * LANES] = (
                both[:, :LANES] + both[:, LANES:] + dot(x_low, high)
            )

    def inner(c, carry):
        for copy in copies(c, slice(0, 1)):
            copy.wait_recv()
        high, low = row_band(c)
        tall[c, :, width:] = along_rows(c, high, low, side[c])
        along_cols(c, slice(REACH, height - REACH))
        return carry

    lax.fori_loop(0, channels, inner, 0)

    def outer_rows(c, carry):
        for copy in copies(c, slice(1, 5)):
            copy.wait_recv()
        part = iota((REACH, 3 * REACH), 1)
        offset = part % REACH - iota((REACH, 3 * REACH), 0)
        for halo, rows, shift, real in (
            (above, slice(0, REACH), -REACH, my_row > 0),
            (below, slice(height - REACH, height), REACH, my_row + 1 < rows_n),
        ):
            taps = tap(offset + shift, spread_ref[0, c])
            taps = jnp.where(real, taps, 0.0)
            high = taps.astype(BF16).astype(F32)
            taps = jnp.where(part // REACH == 1, taps - high, high).astype(BF16)
            x_high, x_low = split(halo[c])
            tall[c, rows, :] += dot(taps, jnp.concatenate([x_high, x_high, x_low], axis=0))
            along_cols(c, rows)
        return carry

    lax.fori_loop(0, channels, outer_rows, 0)
    for c in range(channels):
        for copy in copies(c):
            copy.wait_send()


def smooth(spread, raw, rows_n, cols_n):
    channels, height, width = raw.shape
    vmem = pl.BlockSpec(memory_space=pltpu.VMEM)
    return pl.pallas_call(
        functools.partial(smooth_kernel, rows_n, cols_n),
        name="smooth",
        out_shape=jax.ShapeDtypeStruct(raw.shape, F32),
        in_specs=[pl.BlockSpec(memory_space=pltpu.SMEM), vmem],
        out_specs=vmem,
        scratch_shapes=[
            pltpu.VMEM((channels, height, width + LANES), F32),
            pltpu.VMEM((channels, height, LANES), F32),
            pltpu.VMEM((channels, REACH, width + LANES), F32),
            pltpu.VMEM((channels, REACH, width + LANES), F32),
            pltpu.SemaphoreType.DMA((5, channels)),
            pltpu.SemaphoreType.DMA((5, channels)),
        ],
        compiler_params=pltpu.CompilerParams(
            collective_id=1, has_side_effects=True, vmem_limit_bytes=24 << 20
        ),
    )(spread, raw)


def shards(cell_index, weights, block_tile, spread):
    rows_n, cols_n = lax.axis_size("row"), lax.axis_size("col")
    cells, points = exchange(cell_index, weights, block_tile, rows_n, cols_n)
    raw = scatter(cells, points)
    return smooth(spread, raw, rows_n, cols_n)


def solution(mesh):
    return jax.shard_map(
        shards,
        mesh=mesh,
        in_specs=(
            P(("groups", "row", "col"), None),
            P(("groups", "row", "col"), None),
            P(("groups", "row", "col")),
            P(),
        ),
        out_specs=P(None, ("groups", "row"), "col"),
        check_vma=False,
    )
```

```python
import functools

import jax
import jax.numpy as jnp
from jax import lax
from jax.experimental import pallas as pl
from jax.experimental.pallas import tpu as pltpu
from jax.sharding import PartitionSpec as P

REACH = 16
TILE_ROWS = 256
TILE_COLS = 1024
CAPACITY = 3
LANES = 128
WINDOW = 64
LEAD = 24
CHUNK_ROWS = 2
UNROLL = 5
MESH = pl.DeviceIdType.MESH
F32 = jnp.float32
BF16 = jnp.bfloat16


def iota(shape, dim):
    return lax.broadcasted_iota(jnp.int32, shape, dim)


def in_hbm(value):
    return pltpu.with_memory_space_constraint(value, pltpu.MemorySpace.HBM)


def dot(a, b):
    return lax.dot_general(a, b, (((1,), (0,)), ((), ())), preferred_element_type=F32)


def exchange_kernel(
    rows_n, cols_n, cell_hbm, weight_hbm, tile_hbm, cells_out, weights_out,
    cell_ref, weight_ref, tile_ref, values, keys_t, sorted_points, send_cells, send_weights,
    send_sem, recv_sem, local_sem
):
    loads = [
        pltpu.make_async_copy(source, target, local_sem.at[2 + i])
        for i, (source, target) in enumerate(
            ((cell_hbm, cell_ref), (weight_hbm, weight_ref), (tile_hbm, tile_ref))
        )
    ]
    for load in loads:
        load.start()
    blocks, points = cell_ref.shape
    channels = weight_ref.shape[1] // points
    peers = rows_n * cols_n
    my_row, my_col = lax.axis_index("row"), lax.axis_index("col")
    me = my_row * cols_n + my_col

    offsets = []
    for distance in range(rows_n // 2, 0, -1):
        for step in (distance, rows_n - distance):
            if step not in [o[0] for o in offsets]:
                offsets += [(step, c) for c in range(cols_n)]
    offsets += [(0, c) for c in range(1, cols_n)]

    barrier = pltpu.get_barrier_semaphore()
    targets = []
    for step, turn in offsets:
        row = lax.rem(my_row + step, rows_n)
        col = lax.rem(my_col + turn, cols_n)
        targets.append((row, col))
        pl.semaphore_signal(
            barrier, inc=1, device_id={"row": row, "col": col}, device_id_type=MESH
        )

    for load in loads:
        load.wait()
    tile = tile_ref[...]
    square = (blocks, blocks)
    tile_down = jnp.sum(
        jnp.where(iota(square, 0) == iota(square, 1), tile, 0), axis=1, keepdims=True
    )
    earlier = (tile_down == tile) & (iota(square, 0) < iota(square, 1))
    turn_of = jnp.sum(earlier.astype(jnp.int32), axis=0, keepdims=True)
    cells = cell_ref[...]
    within = cells & (TILE_COLS - 1)
    parts = [weight_ref[:, c * points : (c + 1) * points] for c in range(channels)] + [
        part.astype(F32).astype(BF16)
        for part in (
            cells >> (TILE_COLS.bit_length() - 1),
            within >> (LANES.bit_length() - 1),
            within & (LANES - 1),
        )
    ]
    group = CAPACITY * points
    ramp = (iota((1, points), 1) * (TILE_ROWS // points)).astype(F32)
    keys = []
    for k in range(CAPACITY):
        chosen = ((iota((peers, blocks), 0) == tile) & (turn_of == k)).astype(F32)
        empty = jnp.sum(chosen, axis=1, keepdims=True) < 0.5
        placed = dot(chosen.astype(BF16), jnp.concatenate(parts, axis=1))
        for v in range(channels + 3):
            piece = placed[:, v * points : (v + 1) * points]
            if v == channels:
                piece = jnp.where(empty, ramp, piece)
                keys.append(piece * 512.0 + (iota((1, points), 1) + k * points).astype(F32))
            values[v, :, k * points : (k + 1) * points] = piece
    pad = jnp.zeros((points - peers, points), F32)
    keys_t[...] = jnp.concatenate(
        [jnp.transpose(jnp.concatenate([key, pad], axis=0)) for key in keys], axis=0
    )
    keys = jnp.concatenate(keys, axis=1)
    quarter = points // 4
    chunks = quarter // CHUNK_ROWS
    share = group // chunks
    for t in range(peers):
        less = (keys_t[:, t : t + 1] < keys[t : t + 1, :]).astype(F32)
        rank = jnp.sum(less, axis=0, keepdims=True).astype(jnp.int32)
        chunk = (rank * (65536 // share + 1)) >> 16
        inside = rank - chunk * share
        third = (inside * (512 // CAPACITY + 1)) >> 9
        lane = (inside - third * CAPACITY) * points
        lane = lane + (third & 3) * quarter + chunk * CHUNK_ROWS + (third >> 2)
        hot = (iota((group, group), 0) == lane).astype(F32).astype(BF16)
        piece = jnp.concatenate(
            [values[v, t : t + 1, :] for v in range(channels + 3)] + [jnp.zeros((1, group), F32)],
            axis=0,
        ).astype(BF16)
        sorted_points[t] = lax.dot_general(
            piece, hot, (((1,), (1,)), ((), ())), preferred_element_type=F32
        )
    for k in range(CAPACITY):
        part = slice(k * points, (k + 1) * points)
        cell = sorted_points[:, channels, part] * TILE_COLS
        cell = cell + sorted_points[:, channels + 1, part] * LANES + sorted_points[:, channels + 2, part]
        send_cells[:, k, :] = cell.astype(jnp.int32)
        for c in range(channels):
            send_weights[:, k * channels + c, :] = sorted_points[:, c, part].astype(BF16)

    own = [
        pltpu.make_async_copy(send_cells.at[me], cells_out.at[me], local_sem.at[0]),
        pltpu.make_async_copy(send_weights.at[me], weights_out.at[me], local_sem.at[1]),
    ]
    pl.semaphore_wait(barrier, peers - 1)
    copies = []
    for i, (row, col) in enumerate(targets):
        peer = row * cols_n + col
        for a, (source, out) in enumerate(
            ((send_cells, cells_out), (send_weights, weights_out))
        ):
            copy = pltpu.make_async_remote_copy(
                src_ref=source.at[peer],
                dst_ref=out.at[me],
                send_sem=send_sem.at[a, i],
                recv_sem=recv_sem.at[a, i],
                device_id={"row": row, "col": col},
                device_id_type=MESH,
            )
            copy.start()
            copies.append(copy)
    for copy in own:
        copy.start()
    for copy in own:
        copy.wait()
    for copy in copies:
        copy.wait_recv()
    for copy in copies:
        copy.wait_send()


def exchange(cell_index, weights, block_tile, rows_n, cols_n):
    blocks, points = cell_index.shape
    channels = weights.shape[1] // points
    peers = rows_n * cols_n
    vmem = pl.BlockSpec(memory_space=pltpu.VMEM)
    return pl.pallas_call(
        functools.partial(exchange_kernel, rows_n, cols_n),
        name="exchange",
        out_shape=(
            jax.ShapeDtypeStruct((peers, CAPACITY, points), jnp.int32),
            jax.ShapeDtypeStruct((peers, CAPACITY * channels, points), BF16),
        ),
        in_specs=[pl.BlockSpec(memory_space=pltpu.MemorySpace.HBM)] * 3,
        out_specs=(vmem, vmem),
        scratch_shapes=[
            pltpu.VMEM(cell_index.shape, jnp.int32),
            pltpu.VMEM(weights.shape, BF16),
            pltpu.VMEM((1, blocks), jnp.int32),
            pltpu.VMEM((3 + channels, peers, CAPACITY * points), F32),
            pltpu.VMEM((CAPACITY * points, points), F32),
            pltpu.VMEM((peers, 8, CAPACITY * points), F32),
            pltpu.VMEM((peers, CAPACITY, points), jnp.int32),
            pltpu.VMEM((peers, CAPACITY * channels, points), BF16),
            pltpu.SemaphoreType.DMA((2, peers - 1)),
            pltpu.SemaphoreType.DMA((2, peers - 1)),
            pltpu.SemaphoreType.DMA((5,)),
        ],
        compiler_params=pltpu.CompilerParams(collective_id=0, has_side_effects=True, vmem_limit_bytes=8 << 20),
    )(*(in_hbm(x) for x in (cell_index, weights, block_tile.reshape(1, -1))))


def turned(slots, quarter):
    wide = jnp.concatenate(
        [
            jnp.concatenate([s[:, v * quarter : (v + 1) * quarter] for v in range(4)], axis=0)
            for s in slots
        ]
        + [jnp.zeros((LANES, LANES - len(slots) * quarter), F32)],
        axis=1,
    )
    return jnp.transpose(wide)


def add_window(raw_ref, rows_s, cols_s, weights_s, j, low, stop, base):
    channels = raw_ref.shape[0]
    quarter = LANES // 4
    span = 256

    def take(ref):
        return jnp.concatenate(
            [
                ref[pl.ds(quarter * k + CHUNK_ROWS * j + i, 1), :]
                for k in range(CAPACITY)
                for i in range(CHUNK_ROWS)
            ],
            axis=1,
        )

    row = take(rows_s)
    col = take(cols_s)
    count = row.shape[1]
    offset = jnp.where((row >= low) & (row < stop), row - base, -1)
    hot = iota((WINDOW, count), 0) == offset
    left = jnp.concatenate(
        [jnp.where(hot, take(weights_s.at[c]), 0.0).astype(BF16) for c in range(channels)],
        axis=0,
    )
    for g in range(TILE_COLS // span):
        right = (iota((span, count), 0) == col - g * span).astype(F32).astype(BF16)
        layer = lax.dot_general(
            left, right, (((1,), (1,)), ((), ())), preferred_element_type=F32
        )
        for c in range(channels):
            raw_ref[c, pl.ds(base, WINDOW), g * span : (g + 1) * span] += layer[
                c * WINDOW : (c + 1) * WINDOW
            ]


def inner_chunks(chunks):
    tall = TILE_ROWS // chunks
    inner = [
        j
        for j in range(chunks)
        if tall * j - LEAD >= REACH and tall * j - LEAD + WINDOW <= TILE_ROWS - REACH
    ]
    return tall, inner[0], inner[-1] + 1


def outer_kernel(
    cells_ref, weights_ref, raw_ref, rows_s, cols_s, weights_s, wide_s, first_s, last_s, next_s
):
    senders, slots, points = cells_ref.shape
    channels = weights_ref.shape[1] // slots
    quarter = points // 4
    chunks = quarter // CHUNK_ROWS
    wide_s[...] = weights_ref[...].astype(F32)
    cells = turned([cells_ref[:, k, :].astype(F32) for k in range(slots)], quarter).astype(jnp.int32)
    rows = cells >> (TILE_COLS.bit_length() - 1)
    rows_s[...] = rows
    cols_s[...] = cells & (TILE_COLS - 1)
    for c in range(channels):
        weights_s[c] = turned([wide_s[:, k * channels + c, :] for k in range(slots)], quarter)
    low, high = rows[:quarter], rows[:quarter]
    for k in range(1, slots):
        low = jnp.minimum(low, rows[quarter * k : quarter * (k + 1)])
        high = jnp.maximum(high, rows[quarter * k : quarter * (k + 1)])
    low = jnp.min(low, axis=1, keepdims=True)
    high = jnp.max(high, axis=1, keepdims=True)
    tall, begin, end = inner_chunks(chunks)
    for j in range(chunks):
        lows = [low[CHUNK_ROWS * j + i, 0] for i in range(CHUNK_ROWS)]
        highs = [high[CHUNK_ROWS * j + i, 0] for i in range(CHUNK_ROWS)]
        first = (functools.reduce(jnp.minimum, lows) >> 3) << 3
        done = tall * j - LEAD if begin <= j < end else first
        first_s[j] = first
        last_s[j] = functools.reduce(jnp.maximum, highs)
        next_s[j] = jnp.where(first < done, first, done + WINDOW)
    raw_ref[...] = jnp.zeros_like(raw_ref)

    def add(j, low, stop):
        base = pl.multiple_of(jnp.minimum(low, TILE_ROWS - WINDOW), 8)
        add_window(raw_ref, rows_s, cols_s, weights_s, j, low, stop, base)

    def common(i, carry):
        j = jnp.where(i < begin, i, i + end - begin)
        low = first_s[j]
        add(j, low, low + WINDOW)
        return carry

    lax.fori_loop(0, chunks - (end - begin), common, 0, unroll=True)

    def rest(j, carry):
        done = jnp.where((j >= begin) & (j < end), tall * j - LEAD, first_s[j])

        def more(low):
            stop = jnp.where(low < done, jnp.minimum(low + WINDOW, done), low + WINDOW)
            add(j, low, stop)
            return jnp.where(stop == done, done + WINDOW, stop)

        lax.while_loop(lambda low: low <= last_s[j], more, next_s[j])
        return carry

    lax.fori_loop(0, chunks, rest, 0)


def outer(cells, weights):
    senders, slots, points = cells.shape
    channels = weights.shape[1] // slots
    vmem = pl.BlockSpec(memory_space=pltpu.VMEM)
    turns = points // 4 // CHUNK_ROWS
    return pl.pallas_call(
        outer_kernel,
        name="outer",
        out_shape=(
            jax.ShapeDtypeStruct((channels, TILE_ROWS, TILE_COLS), F32),
            jax.ShapeDtypeStruct((LANES, LANES), jnp.int32),
            jax.ShapeDtypeStruct((LANES, LANES), jnp.int32),
            jax.ShapeDtypeStruct((channels, LANES, LANES), F32),
        ),
        in_specs=[vmem] * 2,
        out_specs=(vmem,) * 4,
        scratch_shapes=[pltpu.VMEM((senders, slots * channels, points), F32)]
        + [pltpu.SMEM((turns,), jnp.int32)] * 3,
        compiler_params=pltpu.CompilerParams(vmem_limit_bytes=16 << 20),
    )(cells, weights)


def split(value):
    high = value.astype(BF16)
    return high, (value - high.astype(F32)).astype(BF16)


def tap(offset, width):
    near = jnp.abs(offset) <= REACH
    far = offset.astype(F32)
    return jnp.where(near, jnp.exp(-(far * far) / (2.0 * width * width)), 0.0)


def col_band(width):
    source = iota((2 * LANES, LANES), 0)
    source = jnp.where(source < LANES + LANES // 2, source, source - 2 * LANES)
    high, low = split(tap(source - iota((2 * LANES, LANES), 1), width))
    return jnp.concatenate([high, low], axis=1), high


def along_cols(block, beyond, count, my_col, cols_n, band, high, store):
    for n in range(count):
        own = block(n)
        before = block(n - 1) if n else jnp.where(my_col > 0, beyond, 0.0)
        after = block(n + 1) if n + 1 < count else jnp.where(my_col + 1 < cols_n, beyond, 0.0)
        edge = jnp.where(iota(own.shape, 1) < LANES // 2, after, before)
        x_high, x_low = split(jnp.concatenate([own, edge], axis=1))
        both = dot(x_high, band)
        store(n, both[:, :LANES] + both[:, LANES:] + dot(x_low, high))


def inner_kernel(
    rows_n, cols_n, spread_hbm, raw_ref, rows_s, cols_s, weights_s,
    out_ref, tall, above, below, spread_ref, acc, side, send_sem, recv_sem, load_sem
):
    channels, height, width = raw_ref.shape
    my_row, my_col = lax.axis_index("row"), lax.axis_index("col")
    other = lax.rem(my_col + 1, cols_n)
    prev = lax.rem(my_row + rows_n - 1, rows_n)
    following = lax.rem(my_row + 1, rows_n)

    def at(row, col):
        return {"row": row, "col": col}

    barrier = pltpu.get_barrier_semaphore()
    peers = [at(prev, my_col), at(following, my_col), at(prev, other), at(following, other), at(my_row, other)]
    for peer in peers:
        pl.semaphore_signal(barrier, inc=1, device_id=peer, device_id_type=MESH)
    pl.semaphore_wait(barrier, len(peers))
    near = pl.ds(pl.multiple_of((1 - my_col) * (width - LANES), LANES), LANES)
    main = pl.ds(0, width)
    beyond = pl.ds(width, LANES)
    top, bottom = pl.ds(0, REACH), pl.ds(height - REACH, REACH)

    def remote(i, source, target, peer):
        return pltpu.make_async_remote_copy(
            src_ref=source, dst_ref=target, send_sem=send_sem.at[i], recv_sem=recv_sem.at[i],
            device_id=peer, device_id_type=MESH,
        )

    halo = [
        remote(0, raw_ref.at[:, bottom, main], above.at[:, :, main], peers[1]),
        remote(1, raw_ref.at[:, top, main], below.at[:, :, main], peers[0]),
        remote(2, raw_ref.at[:, bottom, near], above.at[:, :, beyond], peers[3]),
        remote(3, raw_ref.at[:, top, near], below.at[:, :, beyond], peers[2]),
    ]
    for copy in halo:
        copy.start()
    load = pltpu.make_async_copy(spread_hbm, spread_ref, load_sem)
    load.start()

    acc[...] = raw_ref[...]
    tall_rows, begin, end = inner_chunks(LANES // 4 // CHUNK_ROWS)

    def chunk(j, carry):
        base = pl.multiple_of(tall_rows * j - LEAD, 8)
        add_window(acc, rows_s, cols_s, weights_s, j, base, base + WINDOW, base)
        return carry

    lax.fori_loop(begin, end, chunk, 0, unroll=UNROLL)

    def row_band(c):
        return split(tap(iota((height, height), 1) - iota((height, height), 0), spread_ref[0, c]))

    def along_rows(high, low, x):
        x_high, x_low = split(x)
        both = dot(jnp.concatenate([high, low], axis=0), x_high)
        return both[:height] + both[height:] + dot(high, x_low)

    step = 2 * LANES
    load.wait()

    def own_rows(c, carry):
        high, low = row_band(c)
        for g in range(width // step):
            cols = slice(g * step, (g + 1) * step)
            tall[c, :, cols] = along_rows(high, low, acc[c, :, cols])
        return carry

    own_rows(0, 0)
    partner = remote(4, acc.at[:, :, near], side, peers[4])
    partner.start()
    lax.fori_loop(1, channels, own_rows, 0)
    partner.wait_recv()

    def inner_cols(c, carry):
        high, low = row_band(c)
        tall[c, :, width:] = along_rows(high, low, side[c])
        band, high = col_band(spread_ref[1, c])
        rows = slice(REACH, height - REACH)

        def block(n):
            return tall[c, rows, n * LANES : (n + 1) * LANES]

        def store(n, value):
            out_ref[c, rows, n * LANES : (n + 1) * LANES] = value

        count = width // LANES
        along_cols(block, block(count), count, my_col, cols_n, band, high, store)
        return carry

    lax.fori_loop(0, channels, inner_cols, 0)
    for copy in halo:
        copy.wait_recv()
    for copy in halo + [partner]:
        copy.wait_send()


def inner(spread, raw, rows, cols, weights, rows_n, cols_n):
    channels, height, width = raw.shape
    vmem = pl.BlockSpec(memory_space=pltpu.VMEM)
    return pl.pallas_call(
        functools.partial(inner_kernel, rows_n, cols_n),
        name="inner",
        out_shape=(
            jax.ShapeDtypeStruct(raw.shape, F32),
            jax.ShapeDtypeStruct((channels, height, width + LANES), F32),
            jax.ShapeDtypeStruct((channels, REACH, width + LANES), F32),
            jax.ShapeDtypeStruct((channels, REACH, width + LANES), F32),
        ),
        in_specs=[pl.BlockSpec(memory_space=pltpu.MemorySpace.HBM)] + [vmem] * 4,
        out_specs=(vmem,) * 4,
        scratch_shapes=[
            pltpu.SMEM(spread.shape, F32),
            pltpu.VMEM(raw.shape, F32),
            pltpu.VMEM((channels, height, LANES), F32),
            pltpu.SemaphoreType.DMA((5,)),
            pltpu.SemaphoreType.DMA((5,)),
            pltpu.SemaphoreType.DMA,
        ],
        compiler_params=pltpu.CompilerParams(
            collective_id=1, has_side_effects=True, vmem_limit_bytes=24 << 20
        ),
    )(in_hbm(spread), raw, rows, cols, weights)


def finish_kernel(
    rows_n, cols_n, spread_ref, done_ref, tall, above, below, out_ref, edge, inner_sem, edge_sem
):
    channels, height, width = done_ref.shape
    my_row, my_col = lax.axis_index("row"), lax.axis_index("col")
    copies = []
    for c in range(channels):
        rows = pl.ds(REACH, height - 2 * REACH)
        copies.append(
            pltpu.make_async_copy(done_ref.at[c, rows], out_ref.at[c, rows], inner_sem.at[c])
        )
        copies[-1].start()
    shape = (REACH, 3 * REACH)
    part = iota(shape, 1) >> (REACH.bit_length() - 1)
    offset = (iota(shape, 1) & (REACH - 1)) - iota(shape, 0)
    for c in range(channels):
        sides = []
        for halo, start, shift, real in (
            (above, 0, -REACH, my_row > 0),
            (below, height - REACH, REACH, my_row + 1 < rows_n),
        ):
            taps = jnp.where(real, tap(offset + shift, spread_ref[0, c]), 0.0)
            high = taps.astype(BF16).astype(F32)
            taps = jnp.where(part == 1, taps - high, high).astype(BF16)
            x_high, x_low = split(halo[c])
            sides.append(
                tall[c, start : start + REACH, :]
                + dot(taps, jnp.concatenate([x_high, x_high, x_low], axis=0))
            )
        rows = jnp.concatenate(sides, axis=0)
        band, high = col_band(spread_ref[1, c])

        def block(n):
            return rows[:, n * LANES : (n + 1) * LANES]

        def store(n, value):
            edge[c, :, n * LANES : (n + 1) * LANES] = value

        count = width // LANES
        along_cols(block, block(count), count, my_col, cols_n, band, high, store)
        for i, start in enumerate((0, height - REACH)):
            copies.append(
                pltpu.make_async_copy(
                    edge.at[c, pl.ds(i * REACH, REACH)],
                    out_ref.at[c, pl.ds(start, REACH)],
                    edge_sem.at[i, c],
                )
            )
            copies[-1].start()
    for copy in copies:
        copy.wait()


def finish(spread, done, tall, above, below, rows_n, cols_n):
    channels, height, width = done.shape
    vmem = pl.BlockSpec(memory_space=pltpu.VMEM)
    return pl.pallas_call(
        functools.partial(finish_kernel, rows_n, cols_n),
        name="finish",
        out_shape=jax.ShapeDtypeStruct(done.shape, F32),
        in_specs=[pl.BlockSpec(memory_space=pltpu.SMEM)] + [vmem] * 4,
        out_specs=pl.BlockSpec(memory_space=pltpu.MemorySpace.HBM),
        scratch_shapes=[
            pltpu.VMEM((channels, 2 * REACH, width), F32),
            pltpu.SemaphoreType.DMA((channels,)),
            pltpu.SemaphoreType.DMA((2, channels)),
        ],
        compiler_params=pltpu.CompilerParams(vmem_limit_bytes=12 << 20),
    )(spread, done, tall, above, below)


def shards(cell_index, weights, block_tile, spread):
    rows_n, cols_n = lax.axis_size("row"), lax.axis_size("col")
    cells, points = exchange(cell_index, weights, block_tile, rows_n, cols_n)
    raw, rows, cols, values = outer(cells, points)
    done = inner(spread, raw, rows, cols, values, rows_n, cols_n)
    return finish(spread, *done, rows_n, cols_n)


def solution(mesh):
    return jax.shard_map(
        shards,
        mesh=mesh,
        in_specs=(
            P(("groups", "row", "col"), None),
            P(("groups", "row", "col"), None),
            P(("groups", "row", "col")),
            P(),
        ),
        out_specs=P(None, ("groups", "row"), "col"),
        check_vma=False,
    )
```

```python
import functools

import jax
import jax.numpy as jnp
from jax import lax
from jax.experimental import pallas as pl
from jax.experimental.pallas import tpu as pltpu
from jax.sharding import PartitionSpec as P

REACH = 16
TILE_ROWS = 256
TILE_COLS = 1024
CAPACITY = 3
LANES = 128
WINDOW = 64
LEAD = 24
BITS = 9
HALF = 1 << (BITS - 1)
CHUNK_ROWS = 2
UNROLL = 5
MESH = pl.DeviceIdType.MESH
F32 = jnp.float32
BF16 = jnp.bfloat16


def iota(shape, dim):
    return lax.broadcasted_iota(jnp.int32, shape, dim)


def in_hbm(value):
    return pltpu.with_memory_space_constraint(value, pltpu.MemorySpace.HBM)


def dot(a, b):
    return lax.dot_general(a, b, (((1,), (0,)), ((), ())), preferred_element_type=F32)


def exchange_kernel(
    rows_n, cols_n, cell_hbm, weight_hbm, tile_hbm, message_out,
    cell_ref, weight_ref, tile_ref, values, keys_t, sorted_points, send_message,
    send_sem, recv_sem, local_sem
):
    loads = [
        pltpu.make_async_copy(source, target, local_sem.at[i])
        for i, (source, target) in enumerate(
            ((cell_hbm, cell_ref), (weight_hbm, weight_ref), (tile_hbm, tile_ref))
        )
    ]
    for load in loads:
        load.start()
    blocks, points = cell_ref.shape
    channels = weight_ref.shape[1] // points
    peers = rows_n * cols_n
    my_row, my_col = lax.axis_index("row"), lax.axis_index("col")
    me = my_row * cols_n + my_col

    offsets = []
    for distance in range(rows_n // 2, 0, -1):
        for step in (distance, rows_n - distance):
            if step not in [o[0] for o in offsets]:
                offsets += [(step, c) for c in range(cols_n)]
    offsets += [(0, c) for c in range(1, cols_n)]

    barrier = pltpu.get_barrier_semaphore()
    targets = []
    for step, turn in offsets:
        row = lax.rem(my_row + step, rows_n)
        col = lax.rem(my_col + turn, cols_n)
        targets.append((row, col))
        pl.semaphore_signal(
            barrier, inc=1, device_id={"row": row, "col": col}, device_id_type=MESH
        )

    for load in loads:
        load.wait()
    tile = tile_ref[...]
    square = (blocks, blocks)
    tile_down = jnp.sum(
        jnp.where(iota(square, 0) == iota(square, 1), tile, 0), axis=1, keepdims=True
    )
    earlier = (tile_down == tile) & (iota(square, 0) < iota(square, 1))
    turn_of = jnp.sum(earlier.astype(jnp.int32), axis=0, keepdims=True)
    cells = cell_ref[...]
    rows_each = channels + 2
    parts = [weight_ref[:, c * points : (c + 1) * points] for c in range(channels)] + [
        (part - HALF).astype(F32).astype(BF16)
        for part in (cells >> BITS, cells & (2 * HALF - 1))
    ]
    group = CAPACITY * points
    ramp = (iota((1, points), 1) * (TILE_ROWS // points * TILE_COLS // (2 * HALF)) - HALF).astype(F32)
    keys = []
    for k in range(CAPACITY):
        chosen = ((iota((peers, blocks), 0) == tile) & (turn_of == k)).astype(F32)
        empty = jnp.sum(chosen, axis=1, keepdims=True) < 0.5
        placed = dot(chosen.astype(BF16), jnp.concatenate(parts, axis=1))
        for v in range(rows_each):
            piece = placed[:, v * points : (v + 1) * points]
            if v == channels:
                piece = jnp.where(empty, ramp, piece)
                index = (iota((1, points), 1) + k * points).astype(F32)
                keys.append((piece + float(HALF)) * 512.0 + index)
            if v == channels + 1:
                piece = jnp.where(empty, -float(HALF), piece)
            values[v, :, k * points : (k + 1) * points] = piece
    pad = jnp.zeros((points - peers, points), F32)
    keys_t[...] = jnp.concatenate(
        [jnp.transpose(jnp.concatenate([key, pad], axis=0)) for key in keys], axis=0
    )
    keys = jnp.concatenate(keys, axis=1)
    quarter = points // 4
    chunks = quarter // CHUNK_ROWS
    share = group // chunks
    for t in range(peers):
        less = (keys_t[:, t : t + 1] < keys[t : t + 1, :]).astype(F32)
        rank = jnp.sum(less, axis=0, keepdims=True).astype(jnp.int32)
        chunk = (rank * (65536 // share + 1)) >> 16
        inside = rank - chunk * share
        third = (inside * (512 // CAPACITY + 1)) >> 9
        lane = (inside - third * CAPACITY) * points
        lane = lane + (third & 3) * quarter + chunk * CHUNK_ROWS + (third >> 2)
        hot = (iota((group, group), 0) == lane).astype(F32).astype(BF16)
        piece = jnp.concatenate(
            [values[v, t : t + 1, :] for v in range(rows_each)]
            + [jnp.zeros((8 - rows_each, group), F32)],
            axis=0,
        ).astype(BF16)
        sorted_points[t] = lax.dot_general(
            piece, hot, (((1,), (1,)), ((), ())), preferred_element_type=F32
        )
    for k in range(CAPACITY):
        part = slice(k * points, (k + 1) * points)
        for v in range(rows_each):
            send_message[:, k * rows_each + v, :] = sorted_points[:, v, part].astype(BF16)

    own = pltpu.make_async_copy(send_message.at[me], message_out.at[me], local_sem.at[3])
    pl.semaphore_wait(barrier, peers - 1)
    copies = []
    for i, (row, col) in enumerate(targets):
        copy = pltpu.make_async_remote_copy(
            src_ref=send_message.at[row * cols_n + col],
            dst_ref=message_out.at[me],
            send_sem=send_sem.at[i],
            recv_sem=recv_sem.at[i],
            device_id={"row": row, "col": col},
            device_id_type=MESH,
        )
        copy.start()
        copies.append(copy)
    own.start()
    own.wait()
    for copy in copies:
        copy.wait_recv()
    for copy in copies:
        copy.wait_send()


def exchange(cell_index, weights, block_tile, rows_n, cols_n):
    blocks, points = cell_index.shape
    channels = weights.shape[1] // points
    peers = rows_n * cols_n
    message = (peers, CAPACITY * (channels + 2), points)
    return pl.pallas_call(
        functools.partial(exchange_kernel, rows_n, cols_n),
        name="exchange",
        out_shape=jax.ShapeDtypeStruct(message, BF16),
        in_specs=[pl.BlockSpec(memory_space=pltpu.MemorySpace.HBM)] * 3,
        out_specs=pl.BlockSpec(memory_space=pltpu.VMEM),
        scratch_shapes=[
            pltpu.VMEM(cell_index.shape, jnp.int32),
            pltpu.VMEM(weights.shape, BF16),
            pltpu.VMEM((1, blocks), jnp.int32),
            pltpu.VMEM((channels + 2, peers, CAPACITY * points), F32),
            pltpu.VMEM((CAPACITY * points, points), F32),
            pltpu.VMEM((peers, 8, CAPACITY * points), F32),
            pltpu.VMEM(message, BF16),
            pltpu.SemaphoreType.DMA((peers - 1,)),
            pltpu.SemaphoreType.DMA((peers - 1,)),
            pltpu.SemaphoreType.DMA((4,)),
        ],
        compiler_params=pltpu.CompilerParams(
            collective_id=0, has_side_effects=True, vmem_limit_bytes=8 << 20
        ),
    )(*(in_hbm(x) for x in (cell_index, weights, block_tile.reshape(1, -1))))


def widened(slots, quarter):
    return jnp.concatenate(
        [
            jnp.concatenate([s[:, v * quarter : (v + 1) * quarter] for v in range(4)], axis=0)
            for s in slots
        ]
        + [jnp.zeros((LANES, LANES - len(slots) * quarter), F32)],
        axis=1,
    )


def add_window(raw_ref, rows_s, cols_s, weights_s, j, low, stop, base):
    channels = raw_ref.shape[0]
    quarter = LANES // 4
    span = 256

    def take(ref):
        return jnp.concatenate(
            [
                ref[pl.ds(quarter * k + CHUNK_ROWS * j + i, 1), :]
                for k in range(CAPACITY)
                for i in range(CHUNK_ROWS)
            ],
            axis=1,
        )

    row = take(rows_s)
    count = row.shape[1]
    cols = pltpu.roll(cols_s[...], lax.rem(LANES - CHUNK_ROWS * j, LANES), axis=1)
    offset = jnp.where((row >= low) & (row < stop), row - base, -1)
    hot = iota((WINDOW, count), 0) == offset
    left = jnp.concatenate(
        [jnp.where(hot, take(weights_s.at[c]), 0.0).astype(BF16) for c in range(channels)],
        axis=0,
    )
    for g in range(TILE_COLS // span):
        target = iota((LANES, span), 1) + g * span
        right = jnp.concatenate(
            [
                (target == cols[:, quarter * k + i : quarter * k + i + 1]).astype(F32).astype(BF16)
                for k in range(CAPACITY)
                for i in range(CHUNK_ROWS)
            ],
            axis=0,
        )
        layer = dot(left, right)
        for c in range(channels):
            raw_ref[c, pl.ds(base, WINDOW), g * span : (g + 1) * span] += layer[
                c * WINDOW : (c + 1) * WINDOW
            ]


def inner_chunks(chunks):
    tall = TILE_ROWS // chunks
    inner = [
        j
        for j in range(chunks)
        if tall * j - LEAD >= REACH and tall * j - LEAD + WINDOW <= TILE_ROWS - REACH
    ]
    return tall, inner[0], inner[-1] + 1


def outer_kernel(
    message_ref, raw_ref, rows_s, cols_s, weights_s, wide_s, first_s, last_s, next_s
):
    senders, rows_all, points = message_ref.shape
    rows_each = rows_all // CAPACITY
    channels = rows_each - 2
    quarter = points // 4
    chunks = quarter // CHUNK_ROWS
    wide_s[...] = message_ref[...].astype(F32)

    def wide(v):
        return widened([wide_s[:, k * rows_each + v, :] for k in range(CAPACITY)], quarter)

    cells = (wide(channels) + HALF) * (2 * HALF) + (wide(channels + 1) + HALF)
    cols_s[...] = cells.astype(jnp.int32) & (TILE_COLS - 1)
    rows = jnp.transpose(cells).astype(jnp.int32) >> (TILE_COLS.bit_length() - 1)
    rows_s[...] = rows
    for c in range(channels):
        weights_s[c] = jnp.transpose(wide(c))
    low, high = rows[:quarter], rows[:quarter]
    for k in range(1, CAPACITY):
        low = jnp.minimum(low, rows[quarter * k : quarter * (k + 1)])
        high = jnp.maximum(high, rows[quarter * k : quarter * (k + 1)])
    low = jnp.min(low, axis=1, keepdims=True)
    high = jnp.max(high, axis=1, keepdims=True)
    tall, begin, end = inner_chunks(chunks)
    for j in range(chunks):
        lows = [low[CHUNK_ROWS * j + i, 0] for i in range(CHUNK_ROWS)]
        highs = [high[CHUNK_ROWS * j + i, 0] for i in range(CHUNK_ROWS)]
        first = (functools.reduce(jnp.minimum, lows) >> 3) << 3
        done = tall * j - LEAD if begin <= j < end else first
        first_s[j] = first
        last_s[j] = functools.reduce(jnp.maximum, highs)
        next_s[j] = jnp.where(first < done, first, done + WINDOW)
    raw_ref[...] = jnp.zeros_like(raw_ref)

    def add(j, low, stop):
        base = pl.multiple_of(jnp.minimum(low, TILE_ROWS - WINDOW), 8)
        add_window(raw_ref, rows_s, cols_s, weights_s, j, low, stop, base)

    def common(i, carry):
        j = jnp.where(i < begin, i, i + end - begin)
        low = first_s[j]
        add(j, low, low + WINDOW)
        return carry

    lax.fori_loop(0, chunks - (end - begin), common, 0, unroll=True)

    def rest(j, carry):
        done = jnp.where((j >= begin) & (j < end), tall * j - LEAD, first_s[j])

        def more(low):
            stop = jnp.where(low < done, jnp.minimum(low + WINDOW, done), low + WINDOW)
            add(j, low, stop)
            return jnp.where(stop == done, done + WINDOW, stop)

        lax.while_loop(lambda low: low <= last_s[j], more, next_s[j])
        return carry

    lax.fori_loop(0, chunks, rest, 0)


def outer(message):
    senders, rows_all, points = message.shape
    channels = rows_all // CAPACITY - 2
    vmem = pl.BlockSpec(memory_space=pltpu.VMEM)
    turns = points // 4 // CHUNK_ROWS
    return pl.pallas_call(
        outer_kernel,
        name="outer",
        out_shape=(
            jax.ShapeDtypeStruct((channels, TILE_ROWS, TILE_COLS), F32),
            jax.ShapeDtypeStruct((LANES, LANES), jnp.int32),
            jax.ShapeDtypeStruct((LANES, LANES), jnp.int32),
            jax.ShapeDtypeStruct((channels, LANES, LANES), F32),
        ),
        in_specs=[vmem],
        out_specs=(vmem,) * 4,
        scratch_shapes=[pltpu.VMEM(message.shape, F32)]
        + [pltpu.SMEM((turns,), jnp.int32)] * 3,
        compiler_params=pltpu.CompilerParams(vmem_limit_bytes=16 << 20),
    )(message)


def split(value):
    high = value.astype(BF16)
    return high, (value - high.astype(F32)).astype(BF16)


def tap(offset, width):
    near = jnp.abs(offset) <= REACH
    far = offset.astype(F32)
    return jnp.where(near, jnp.exp(-(far * far) / (2.0 * width * width)), 0.0)


def col_band(width):
    source = iota((2 * LANES, LANES), 0)
    source = jnp.where(source < LANES + LANES // 2, source, source - 2 * LANES)
    high, low = split(tap(source - iota((2 * LANES, LANES), 1), width))
    return jnp.concatenate([high, low], axis=1), high


def along_cols(block, beyond, count, my_col, cols_n, band, high, store):
    for n in range(count):
        own = block(n)
        before = block(n - 1) if n else jnp.where(my_col > 0, beyond, 0.0)
        after = block(n + 1) if n + 1 < count else jnp.where(my_col + 1 < cols_n, beyond, 0.0)
        edge = jnp.where(iota(own.shape, 1) < LANES // 2, after, before)
        x_high, x_low = split(jnp.concatenate([own, edge], axis=1))
        both = dot(x_high, band)
        store(n, both[:, :LANES] + both[:, LANES:] + dot(x_low, high))


def inner_kernel(
    rows_n, cols_n, spread_hbm, raw_ref, rows_s, cols_s, weights_s,
    out_ref, tall, above, below, spread_ref, acc, send_sem, recv_sem, load_sem
):
    channels, height, width = raw_ref.shape
    my_row, my_col = lax.axis_index("row"), lax.axis_index("col")
    other = lax.rem(my_col + 1, cols_n)
    prev = lax.rem(my_row + rows_n - 1, rows_n)
    following = lax.rem(my_row + 1, rows_n)

    def at(row, col):
        return {"row": row, "col": col}

    barrier = pltpu.get_barrier_semaphore()
    peers = [at(prev, my_col), at(following, my_col), at(prev, other), at(following, other), at(my_row, other)]
    for peer in peers:
        pl.semaphore_signal(barrier, inc=1, device_id=peer, device_id_type=MESH)
    pl.semaphore_wait(barrier, len(peers))
    near = pl.ds(pl.multiple_of((1 - my_col) * (width - LANES), LANES), LANES)
    main = pl.ds(0, width)
    beyond = pl.ds(width, LANES)
    top, bottom = pl.ds(0, REACH), pl.ds(height - REACH, REACH)

    def remote(i, source, target, peer):
        return pltpu.make_async_remote_copy(
            src_ref=source, dst_ref=target, send_sem=send_sem.at[i], recv_sem=recv_sem.at[i],
            device_id=peer, device_id_type=MESH,
        )

    halo = [
        remote(0, raw_ref.at[:, bottom, main], above.at[:, :, main], peers[1]),
        remote(1, raw_ref.at[:, top, main], below.at[:, :, main], peers[0]),
        remote(2, raw_ref.at[:, bottom, near], above.at[:, :, beyond], peers[3]),
        remote(3, raw_ref.at[:, top, near], below.at[:, :, beyond], peers[2]),
    ]
    for copy in halo:
        copy.start()
    load = pltpu.make_async_copy(spread_hbm, spread_ref, load_sem)
    load.start()

    acc[...] = raw_ref[...]
    tall_rows, begin, end = inner_chunks(LANES // 4 // CHUNK_ROWS)

    def chunk(j, carry):
        base = pl.multiple_of(tall_rows * j - LEAD, 8)
        add_window(acc, rows_s, cols_s, weights_s, j, base, base + WINDOW, base)
        return carry

    lax.fori_loop(begin, end, chunk, 0, unroll=UNROLL)

    def row_band(c):
        return split(tap(iota((height, height), 1) - iota((height, height), 0), spread_ref[0, c]))

    def along_rows(high, low, x):
        x_high, x_low = split(x)
        both = dot(jnp.concatenate([high, low], axis=0), x_high)
        return both[:height] + both[height:] + dot(high, x_low)

    step = 2 * LANES
    load.wait()

    def own_rows(c, carry):
        high, low = row_band(c)
        for g in range(width // step):
            cols = slice(g * step, (g + 1) * step)
            tall[c, :, cols] = along_rows(high, low, acc[c, :, cols])
        return carry

    def partner(c):
        return remote(4 + c, tall.at[c, :, near], tall.at[c, :, beyond], peers[4])

    def next_rows(c, carry):
        own_rows(c, carry)
        partner(c - 1).start()
        return carry

    own_rows(0, 0)
    lax.fori_loop(1, channels, next_rows, 0)
    partner(channels - 1).start()

    def inner_cols(c, carry):
        partner(c).wait_recv()
        band, high = col_band(spread_ref[1, c])
        rows = slice(REACH, height - REACH)

        def block(n):
            return tall[c, rows, n * LANES : (n + 1) * LANES]

        def store(n, value):
            out_ref[c, rows, n * LANES : (n + 1) * LANES] = value

        count = width // LANES
        along_cols(block, block(count), count, my_col, cols_n, band, high, store)
        return carry

    lax.fori_loop(0, channels, inner_cols, 0)
    for copy in halo:
        copy.wait_recv()
    for copy in halo + [partner(c) for c in range(channels)]:
        copy.wait_send()


def inner(spread, raw, rows, cols, weights, rows_n, cols_n):
    channels, height, width = raw.shape
    vmem = pl.BlockSpec(memory_space=pltpu.VMEM)
    return pl.pallas_call(
        functools.partial(inner_kernel, rows_n, cols_n),
        name="inner",
        out_shape=(
            jax.ShapeDtypeStruct(raw.shape, F32),
            jax.ShapeDtypeStruct((channels, height, width + LANES), F32),
            jax.ShapeDtypeStruct((channels, REACH, width + LANES), F32),
            jax.ShapeDtypeStruct((channels, REACH, width + LANES), F32),
        ),
        in_specs=[pl.BlockSpec(memory_space=pltpu.MemorySpace.HBM)] + [vmem] * 4,
        out_specs=(vmem,) * 4,
        scratch_shapes=[
            pltpu.SMEM(spread.shape, F32),
            pltpu.VMEM(raw.shape, F32),
            pltpu.SemaphoreType.DMA((4 + channels,)),
            pltpu.SemaphoreType.DMA((4 + channels,)),
            pltpu.SemaphoreType.DMA,
        ],
        compiler_params=pltpu.CompilerParams(
            collective_id=1, has_side_effects=True, vmem_limit_bytes=24 << 20
        ),
    )(in_hbm(spread), raw, rows, cols, weights)


def finish_kernel(
    rows_n, cols_n, spread_ref, done_ref, tall, above, below, out_ref, edge, inner_sem, edge_sem
):
    channels, height, width = done_ref.shape
    my_row, my_col = lax.axis_index("row"), lax.axis_index("col")
    copies = []
    for c in range(channels):
        rows = pl.ds(REACH, height - 2 * REACH)
        copies.append(
            pltpu.make_async_copy(done_ref.at[c, rows], out_ref.at[c, rows], inner_sem.at[c])
        )
        copies[-1].start()
    shape = (REACH, 3 * REACH)
    part = iota(shape, 1) >> (REACH.bit_length() - 1)
    offset = (iota(shape, 1) & (REACH - 1)) - iota(shape, 0)
    for c in range(channels):
        sides = []
        for halo, start, shift, real in (
            (above, 0, -REACH, my_row > 0),
            (below, height - REACH, REACH, my_row + 1 < rows_n),
        ):
            taps = jnp.where(real, tap(offset + shift, spread_ref[0, c]), 0.0)
            high = taps.astype(BF16).astype(F32)
            taps = jnp.where(part == 1, taps - high, high).astype(BF16)
            x_high, x_low = split(halo[c])
            sides.append(
                tall[c, start : start + REACH, :]
                + dot(taps, jnp.concatenate([x_high, x_high, x_low], axis=0))
            )
        rows = jnp.concatenate(sides, axis=0)
        band, high = col_band(spread_ref[1, c])

        def block(n):
            return rows[:, n * LANES : (n + 1) * LANES]

        def store(n, value):
            edge[c, :, n * LANES : (n + 1) * LANES] = value

        count = width // LANES
        along_cols(block, block(count), count, my_col, cols_n, band, high, store)
        for i, start in enumerate((0, height - REACH)):
            copies.append(
                pltpu.make_async_copy(
                    edge.at[c, pl.ds(i * REACH, REACH)],
                    out_ref.at[c, pl.ds(start, REACH)],
                    edge_sem.at[i, c],
                )
            )
            copies[-1].start()
    for copy in copies:
        copy.wait()


def finish(spread, done, tall, above, below, rows_n, cols_n):
    channels, height, width = done.shape
    vmem = pl.BlockSpec(memory_space=pltpu.VMEM)
    return pl.pallas_call(
        functools.partial(finish_kernel, rows_n, cols_n),
        name="finish",
        out_shape=jax.ShapeDtypeStruct(done.shape, F32),
        in_specs=[pl.BlockSpec(memory_space=pltpu.SMEM)] + [vmem] * 4,
        out_specs=pl.BlockSpec(memory_space=pltpu.MemorySpace.HBM),
        scratch_shapes=[
            pltpu.VMEM((channels, 2 * REACH, width), F32),
            pltpu.SemaphoreType.DMA((channels,)),
            pltpu.SemaphoreType.DMA((2, channels)),
        ],
        compiler_params=pltpu.CompilerParams(vmem_limit_bytes=12 << 20),
    )(spread, done, tall, above, below)


def shards(cell_index, weights, block_tile, spread):
    rows_n, cols_n = lax.axis_size("row"), lax.axis_size("col")
    message = exchange(cell_index, weights, block_tile, rows_n, cols_n)
    raw, rows, cols, values = outer(message)
    done = inner(spread, raw, rows, cols, values, rows_n, cols_n)
    return finish(spread, *done, rows_n, cols_n)


def solution(mesh):
    return jax.shard_map(
        shards,
        mesh=mesh,
        in_specs=(
            P(("groups", "row", "col"), None),
            P(("groups", "row", "col"), None),
            P(("groups", "row", "col")),
            P(),
        ),
        out_specs=P(None, ("groups", "row"), "col"),
        check_vma=False,
    )
```

```python
import functools

import jax
import jax.numpy as jnp
from jax import lax
from jax.experimental import pallas as pl
from jax.experimental.pallas import tpu as pltpu
from jax.sharding import PartitionSpec as P

REACH = 16
TILE_ROWS = 256
TILE_COLS = 1024
CAPACITY = 3
LANES = 128
WINDOW = 64
LEAD = 24
BITS = 9
HALF = 1 << (BITS - 1)
CHUNK_ROWS = 2
UNROLL = 3
MESH = pl.DeviceIdType.MESH
F32 = jnp.float32
BF16 = jnp.bfloat16


def iota(shape, dim):
    return lax.broadcasted_iota(jnp.int32, shape, dim)


def in_hbm(value):
    return pltpu.with_memory_space_constraint(value, pltpu.MemorySpace.HBM)


def dot(a, b):
    return lax.dot_general(a, b, (((1,), (0,)), ((), ())), preferred_element_type=F32)


def exchange_kernel(
    rows_n, cols_n, cell_hbm, weight_hbm, tile_hbm, message_out, zeros_out,
    cell_ref, weight_ref, tile_ref, values, keys_t, sorted_points, send_message,
    send_sem, recv_sem, local_sem
):
    loads = [
        pltpu.make_async_copy(source, target, local_sem.at[i])
        for i, (source, target) in enumerate(
            ((cell_hbm, cell_ref), (weight_hbm, weight_ref), (tile_hbm, tile_ref))
        )
    ]
    for load in loads:
        load.start()
    blocks, points = cell_ref.shape
    channels = weight_ref.shape[1] // points
    peers = rows_n * cols_n
    my_row, my_col = lax.axis_index("row"), lax.axis_index("col")
    me = my_row * cols_n + my_col

    offsets = []
    for distance in range(rows_n // 2, 0, -1):
        for step in (distance, rows_n - distance):
            if step not in [o[0] for o in offsets]:
                offsets += [(step, c) for c in range(cols_n)]
    offsets += [(0, c) for c in range(1, cols_n)]

    barrier = pltpu.get_barrier_semaphore()
    targets = []
    for step, turn in offsets:
        row = lax.rem(my_row + step, rows_n)
        col = lax.rem(my_col + turn, cols_n)
        targets.append((row, col))
        pl.semaphore_signal(
            barrier, inc=1, device_id={"row": row, "col": col}, device_id_type=MESH
        )

    for load in loads:
        load.wait()
    tile = tile_ref[...]
    square = (blocks, blocks)
    tile_down = jnp.sum(
        jnp.where(iota(square, 0) == iota(square, 1), tile, 0), axis=1, keepdims=True
    )
    earlier = (tile_down == tile) & (iota(square, 0) < iota(square, 1))
    turn_of = jnp.sum(earlier.astype(jnp.int32), axis=0, keepdims=True)
    cells = cell_ref[...]
    rows_each = channels + 2
    parts = [weight_ref[:, c * points : (c + 1) * points] for c in range(channels)] + [
        (part - HALF).astype(F32).astype(BF16)
        for part in (cells >> BITS, cells & (2 * HALF - 1))
    ]
    group = CAPACITY * points
    ramp = (iota((1, points), 1) * (TILE_ROWS // points * TILE_COLS // (2 * HALF)) - HALF).astype(F32)
    keys = []
    for k in range(CAPACITY):
        chosen = ((iota((peers, blocks), 0) == tile) & (turn_of == k)).astype(F32)
        empty = jnp.sum(chosen, axis=1, keepdims=True) < 0.5
        placed = dot(chosen.astype(BF16), jnp.concatenate(parts, axis=1))
        for v in range(rows_each):
            piece = placed[:, v * points : (v + 1) * points]
            if v == channels:
                piece = jnp.where(empty, ramp, piece)
                index = (iota((1, points), 1) + k * points).astype(F32)
                keys.append((piece + float(HALF)) * 512.0 + index)
            if v == channels + 1:
                piece = jnp.where(empty, -float(HALF), piece)
            values[v, :, k * points : (k + 1) * points] = piece
    pad = jnp.zeros((points - peers, points), F32)
    keys_t[...] = jnp.concatenate(
        [jnp.transpose(jnp.concatenate([key, pad], axis=0)) for key in keys], axis=0
    )
    keys = jnp.concatenate(keys, axis=1)
    quarter = points // 4
    chunks = quarter // CHUNK_ROWS
    share = group // chunks
    for t in range(peers):
        less = (keys_t[:, t : t + 1] < keys[t : t + 1, :]).astype(F32)
        rank = jnp.sum(less, axis=0, keepdims=True).astype(jnp.int32)
        chunk = (rank * (65536 // share + 1)) >> 16
        inside = rank - chunk * share
        third = (inside * (512 // CAPACITY + 1)) >> 9
        lane = (inside - third * CAPACITY) * points
        lane = lane + (third & 3) * quarter + chunk * CHUNK_ROWS + (third >> 2)
        hot = (iota((group, group), 0) == lane).astype(F32).astype(BF16)
        piece = jnp.concatenate(
            [values[v, t : t + 1, :] for v in range(rows_each)]
            + [jnp.zeros((8 - rows_each, group), F32)],
            axis=0,
        ).astype(BF16)
        sorted_points[t] = lax.dot_general(
            piece, hot, (((1,), (1,)), ((), ())), preferred_element_type=F32
        )
    for k in range(CAPACITY):
        part = slice(k * points, (k + 1) * points)
        for v in range(rows_each):
            send_message[:, k * rows_each + v, :] = sorted_points[:, v, part].astype(BF16)

    zeros_out[...] = jnp.zeros_like(zeros_out)
    own = pltpu.make_async_copy(send_message.at[me], message_out.at[me], local_sem.at[3])
    pl.semaphore_wait(barrier, peers - 1)
    copies = []
    for i, (row, col) in enumerate(targets):
        copy = pltpu.make_async_remote_copy(
            src_ref=send_message.at[row * cols_n + col],
            dst_ref=message_out.at[me],
            send_sem=send_sem.at[i],
            recv_sem=recv_sem.at[i],
            device_id={"row": row, "col": col},
            device_id_type=MESH,
        )
        copy.start()
        copies.append(copy)
    own.start()
    own.wait()
    for copy in copies:
        copy.wait_recv()
    for copy in copies:
        copy.wait_send()


def exchange(cell_index, weights, block_tile, rows_n, cols_n):
    blocks, points = cell_index.shape
    channels = weights.shape[1] // points
    peers = rows_n * cols_n
    message = (peers, CAPACITY * (channels + 2), points)
    return pl.pallas_call(
        functools.partial(exchange_kernel, rows_n, cols_n),
        name="exchange",
        out_shape=(
            jax.ShapeDtypeStruct(message, BF16),
            jax.ShapeDtypeStruct((channels, TILE_ROWS, TILE_COLS), F32),
        ),
        in_specs=[pl.BlockSpec(memory_space=pltpu.MemorySpace.HBM)] * 3,
        out_specs=(pl.BlockSpec(memory_space=pltpu.VMEM),) * 2,
        scratch_shapes=[
            pltpu.VMEM(cell_index.shape, jnp.int32),
            pltpu.VMEM(weights.shape, BF16),
            pltpu.VMEM((1, blocks), jnp.int32),
            pltpu.VMEM((channels + 2, peers, CAPACITY * points), F32),
            pltpu.VMEM((CAPACITY * points, points), F32),
            pltpu.VMEM((peers, 8, CAPACITY * points), F32),
            pltpu.VMEM(message, BF16),
            pltpu.SemaphoreType.DMA((peers - 1,)),
            pltpu.SemaphoreType.DMA((peers - 1,)),
            pltpu.SemaphoreType.DMA((4,)),
        ],
        compiler_params=pltpu.CompilerParams(
            collective_id=0, has_side_effects=True, vmem_limit_bytes=8 << 20
        ),
    )(*(in_hbm(x) for x in (cell_index, weights, block_tile.reshape(1, -1))))


def widened(slots, quarter):
    return jnp.concatenate(
        [
            jnp.concatenate([s[:, v * quarter : (v + 1) * quarter] for v in range(4)], axis=0)
            for s in slots
        ]
        + [jnp.zeros((LANES, LANES - len(slots) * quarter), F32)],
        axis=1,
    )


def add_window(raw_ref, rows_s, cols_s, weights_s, j, low, stop, base):
    channels = raw_ref.shape[0]
    quarter = LANES // 4
    span = 256

    def take(ref):
        return jnp.concatenate(
            [
                ref[pl.ds(quarter * k + CHUNK_ROWS * j + i, 1), :]
                for k in range(CAPACITY)
                for i in range(CHUNK_ROWS)
            ],
            axis=1,
        )

    row = take(rows_s)
    count = row.shape[1]
    cols = pltpu.roll(cols_s[...], lax.rem(LANES - CHUNK_ROWS * j, LANES), axis=1)
    offset = jnp.where((row >= low) & (row < stop), row - base, -1)
    hot = iota((WINDOW, count), 0) == offset
    left = jnp.concatenate(
        [jnp.where(hot, take(weights_s.at[c]), 0.0).astype(BF16) for c in range(channels)],
        axis=0,
    )
    for g in range(TILE_COLS // span):
        target = iota((LANES, span), 1) + g * span
        right = jnp.concatenate(
            [
                (target == cols[:, quarter * k + i : quarter * k + i + 1]).astype(F32).astype(BF16)
                for k in range(CAPACITY)
                for i in range(CHUNK_ROWS)
            ],
            axis=0,
        )
        layer = dot(left, right)
        for c in range(channels):
            raw_ref[c, pl.ds(base, WINDOW), g * span : (g + 1) * span] += layer[
                c * WINDOW : (c + 1) * WINDOW
            ]


def inner_chunks(chunks):
    tall = TILE_ROWS // chunks
    inner = [
        j
        for j in range(chunks)
        if tall * j - LEAD >= REACH and tall * j - LEAD + WINDOW <= TILE_ROWS - REACH
    ]
    return tall, inner[0], inner[-1] + 1


def outer_kernel(
    message_ref, zeros_ref, raw_ref, rows_s, cols_s, weights_s, wide_s, first_s, last_s, next_s
):
    senders, rows_all, points = message_ref.shape
    rows_each = rows_all // CAPACITY
    channels = rows_each - 2
    quarter = points // 4
    chunks = quarter // CHUNK_ROWS
    wide_s[...] = message_ref[...].astype(F32)

    def wide(v):
        return widened([wide_s[:, k * rows_each + v, :] for k in range(CAPACITY)], quarter)

    cells = (wide(channels) + HALF) * (2 * HALF) + (wide(channels + 1) + HALF)
    cols_s[...] = cells.astype(jnp.int32) & (TILE_COLS - 1)
    rows = jnp.transpose(cells).astype(jnp.int32) >> (TILE_COLS.bit_length() - 1)
    rows_s[...] = rows
    for c in range(channels):
        weights_s[c] = jnp.transpose(wide(c))
    low, high = rows[:quarter], rows[:quarter]
    for k in range(1, CAPACITY):
        low = jnp.minimum(low, rows[quarter * k : quarter * (k + 1)])
        high = jnp.maximum(high, rows[quarter * k : quarter * (k + 1)])
    low = jnp.min(low, axis=1, keepdims=True)
    high = jnp.max(high, axis=1, keepdims=True)
    tall, begin, end = inner_chunks(chunks)
    for j in range(chunks):
        lows = [low[CHUNK_ROWS * j + i, 0] for i in range(CHUNK_ROWS)]
        highs = [high[CHUNK_ROWS * j + i, 0] for i in range(CHUNK_ROWS)]
        first = (functools.reduce(jnp.minimum, lows) >> 3) << 3
        done = tall * j - LEAD if begin <= j < end else first
        first_s[j] = first
        last_s[j] = functools.reduce(jnp.maximum, highs)
        next_s[j] = jnp.where(first < done, first, done + WINDOW)

    def add(j, low, stop):
        base = pl.multiple_of(jnp.minimum(low, TILE_ROWS - WINDOW), 8)
        add_window(raw_ref, rows_s, cols_s, weights_s, j, low, stop, base)

    def common(i, carry):
        j = jnp.where(i < begin, i, i + end - begin)
        low = first_s[j]
        add(j, low, low + WINDOW)
        return carry

    lax.fori_loop(0, chunks - (end - begin), common, 0, unroll=True)

    def rest(j, carry):
        done = jnp.where((j >= begin) & (j < end), tall * j - LEAD, first_s[j])

        def more(low):
            stop = jnp.where(low < done, jnp.minimum(low + WINDOW, done), low + WINDOW)
            add(j, low, stop)
            return jnp.where(stop == done, done + WINDOW, stop)

        lax.while_loop(lambda low: low <= last_s[j], more, next_s[j])
        return carry

    lax.fori_loop(0, chunks, rest, 0)


def outer(message, zeros):
    senders, rows_all, points = message.shape
    channels = rows_all // CAPACITY - 2
    vmem = pl.BlockSpec(memory_space=pltpu.VMEM)
    turns = points // 4 // CHUNK_ROWS
    return pl.pallas_call(
        outer_kernel,
        name="outer",
        out_shape=(
            jax.ShapeDtypeStruct((channels, TILE_ROWS, TILE_COLS), F32),
            jax.ShapeDtypeStruct((LANES, LANES), jnp.int32),
            jax.ShapeDtypeStruct((LANES, LANES), jnp.int32),
            jax.ShapeDtypeStruct((channels, LANES, LANES), F32),
        ),
        in_specs=[vmem] * 2,
        input_output_aliases={1: 0},
        out_specs=(vmem,) * 4,
        scratch_shapes=[pltpu.VMEM(message.shape, F32)]
        + [pltpu.SMEM((turns,), jnp.int32)] * 3,
        compiler_params=pltpu.CompilerParams(vmem_limit_bytes=16 << 20),
    )(message, zeros)


def split(value):
    high = value.astype(BF16)
    return high, (value - high.astype(F32)).astype(BF16)


def tap(offset, width):
    near = jnp.abs(offset) <= REACH
    far = offset.astype(F32)
    return jnp.where(near, jnp.exp(-(far * far) / (2.0 * width * width)), 0.0)


def col_band(width):
    source = iota((2 * LANES, LANES), 0)
    source = jnp.where(source < LANES + LANES // 2, source, source - 2 * LANES)
    high, low = split(tap(source - iota((2 * LANES, LANES), 1), width))
    return jnp.concatenate([high, low], axis=1), high


def along_cols(block, beyond, count, my_col, cols_n, band, high, store):
    for n in range(count):
        own = block(n)
        before = block(n - 1) if n else jnp.where(my_col > 0, beyond, 0.0)
        after = block(n + 1) if n + 1 < count else jnp.where(my_col + 1 < cols_n, beyond, 0.0)
        edge = jnp.where(iota(own.shape, 1) < LANES // 2, after, before)
        x_high, x_low = split(jnp.concatenate([own, edge], axis=1))
        both = dot(x_high, band)
        store(n, both[:, :LANES] + both[:, LANES:] + dot(x_low, high))


def inner_kernel(
    rows_n, cols_n, spread_hbm, raw_ref, rows_s, cols_s, weights_s,
    out_ref, tall, above, below, spread_ref, acc, send_sem, recv_sem, load_sem
):
    channels, height, width = raw_ref.shape
    my_row, my_col = lax.axis_index("row"), lax.axis_index("col")
    other = lax.rem(my_col + 1, cols_n)
    prev = lax.rem(my_row + rows_n - 1, rows_n)
    following = lax.rem(my_row + 1, rows_n)

    def at(row, col):
        return {"row": row, "col": col}

    barrier = pltpu.get_barrier_semaphore()
    peers = [at(prev, my_col), at(following, my_col), at(prev, other), at(following, other), at(my_row, other)]
    for peer in peers:
        pl.semaphore_signal(barrier, inc=1, device_id=peer, device_id_type=MESH)
    load = pltpu.make_async_copy(spread_hbm, spread_ref, load_sem)
    load.start()
    acc[...] = raw_ref[...]
    tall_rows, begin, end = inner_chunks(LANES // 4 // CHUNK_ROWS)

    def chunk(j, carry):
        base = pl.multiple_of(tall_rows * j - LEAD, 8)
        add_window(acc, rows_s, cols_s, weights_s, j, base, base + WINDOW, base)
        return carry

    chunk(begin, 0)
    pl.semaphore_wait(barrier, len(peers))
    near = pl.ds(pl.multiple_of((1 - my_col) * (width - LANES), LANES), LANES)
    main = pl.ds(0, width)
    beyond = pl.ds(width, LANES)
    top, bottom = pl.ds(0, REACH), pl.ds(height - REACH, REACH)

    def remote(i, source, target, peer):
        return pltpu.make_async_remote_copy(
            src_ref=source, dst_ref=target, send_sem=send_sem.at[i], recv_sem=recv_sem.at[i],
            device_id=peer, device_id_type=MESH,
        )

    halo = [
        remote(0, raw_ref.at[:, bottom, main], above.at[:, :, main], peers[1]),
        remote(1, raw_ref.at[:, top, main], below.at[:, :, main], peers[0]),
        remote(2, raw_ref.at[:, bottom, near], above.at[:, :, beyond], peers[3]),
        remote(3, raw_ref.at[:, top, near], below.at[:, :, beyond], peers[2]),
    ]
    for copy in halo:
        copy.start()
    lax.fori_loop(begin + 1, end, chunk, 0, unroll=UNROLL)

    def row_band(c):
        return split(tap(iota((height, height), 1) - iota((height, height), 0), spread_ref[0, c]))

    def along_rows(high, low, x):
        x_high, x_low = split(x)
        both = dot(jnp.concatenate([high, low], axis=0), x_high)
        return both[:height] + both[height:] + dot(high, x_low)

    step = 2 * LANES
    load.wait()

    def own_rows(c, carry):
        high, low = row_band(c)
        for g in range(width // step):
            cols = slice(g * step, (g + 1) * step)
            tall[c, :, cols] = along_rows(high, low, acc[c, :, cols])
        return carry

    def partner(c):
        return remote(4 + c, tall.at[c, :, near], tall.at[c, :, beyond], peers[4])

    def next_rows(c, carry):
        own_rows(c, carry)
        partner(c - 1).start()
        return carry

    own_rows(0, 0)
    lax.fori_loop(1, channels, next_rows, 0)
    partner(channels - 1).start()

    def inner_cols(c, carry):
        partner(c).wait_recv()
        band, high = col_band(spread_ref[1, c])
        rows = slice(REACH, height - REACH)

        def block(n):
            return tall[c, rows, n * LANES : (n + 1) * LANES]

        def store(n, value):
            out_ref[c, rows, n * LANES : (n + 1) * LANES] = value

        count = width // LANES
        along_cols(block, block(count), count, my_col, cols_n, band, high, store)
        return carry

    lax.fori_loop(0, channels, inner_cols, 0)
    for copy in halo:
        copy.wait_recv()
    for copy in halo + [partner(c) for c in range(channels)]:
        copy.wait_send()


def inner(spread, raw, rows, cols, weights, rows_n, cols_n):
    channels, height, width = raw.shape
    vmem = pl.BlockSpec(memory_space=pltpu.VMEM)
    return pl.pallas_call(
        functools.partial(inner_kernel, rows_n, cols_n),
        name="inner",
        out_shape=(
            jax.ShapeDtypeStruct(raw.shape, F32),
            jax.ShapeDtypeStruct((channels, height, width + LANES), F32),
            jax.ShapeDtypeStruct((channels, REACH, width + LANES), F32),
            jax.ShapeDtypeStruct((channels, REACH, width + LANES), F32),
        ),
        in_specs=[pl.BlockSpec(memory_space=pltpu.MemorySpace.HBM)] + [vmem] * 4,
        out_specs=(vmem,) * 4,
        scratch_shapes=[
            pltpu.SMEM(spread.shape, F32),
            pltpu.VMEM(raw.shape, F32),
            pltpu.SemaphoreType.DMA((4 + channels,)),
            pltpu.SemaphoreType.DMA((4 + channels,)),
            pltpu.SemaphoreType.DMA,
        ],
        compiler_params=pltpu.CompilerParams(
            collective_id=1, has_side_effects=True, vmem_limit_bytes=24 << 20
        ),
    )(in_hbm(spread), raw, rows, cols, weights)


def finish_kernel(
    rows_n, cols_n, spread_ref, done_ref, tall, above, below, out_ref, edge, inner_sem, edge_sem
):
    channels, height, width = done_ref.shape
    my_row, my_col = lax.axis_index("row"), lax.axis_index("col")
    copies = []
    for c in range(channels):
        rows = pl.ds(REACH, height - 2 * REACH)
        copies.append(
            pltpu.make_async_copy(done_ref.at[c, rows], out_ref.at[c, rows], inner_sem.at[c])
        )
        copies[-1].start()
    shape = (REACH, 3 * REACH)
    part = iota(shape, 1) >> (REACH.bit_length() - 1)
    offset = (iota(shape, 1) & (REACH - 1)) - iota(shape, 0)
    for c in range(channels):
        sides = []
        for halo, start, shift, real in (
            (above, 0, -REACH, my_row > 0),
            (below, height - REACH, REACH, my_row + 1 < rows_n),
        ):
            taps = jnp.where(real, tap(offset + shift, spread_ref[0, c]), 0.0)
            high = taps.astype(BF16).astype(F32)
            taps = jnp.where(part == 1, taps - high, high).astype(BF16)
            x_high, x_low = split(halo[c])
            sides.append(
                tall[c, start : start + REACH, :]
                + dot(taps, jnp.concatenate([x_high, x_high, x_low], axis=0))
            )
        rows = jnp.concatenate(sides, axis=0)
        band, high = col_band(spread_ref[1, c])

        def block(n):
            return rows[:, n * LANES : (n + 1) * LANES]

        def store(n, value):
            edge[c, :, n * LANES : (n + 1) * LANES] = value

        count = width // LANES
        along_cols(block, block(count), count, my_col, cols_n, band, high, store)
        for i, start in enumerate((0, height - REACH)):
            copies.append(
                pltpu.make_async_copy(
                    edge.at[c, pl.ds(i * REACH, REACH)],
                    out_ref.at[c, pl.ds(start, REACH)],
                    edge_sem.at[i, c],
                )
            )
            copies[-1].start()
    for copy in copies:
        copy.wait()


def finish(spread, done, tall, above, below, rows_n, cols_n):
    channels, height, width = done.shape
    vmem = pl.BlockSpec(memory_space=pltpu.VMEM)
    return pl.pallas_call(
        functools.partial(finish_kernel, rows_n, cols_n),
        name="finish",
        out_shape=jax.ShapeDtypeStruct(done.shape, F32),
        in_specs=[pl.BlockSpec(memory_space=pltpu.SMEM)] + [vmem] * 4,
        out_specs=pl.BlockSpec(memory_space=pltpu.MemorySpace.HBM),
        scratch_shapes=[
            pltpu.VMEM((channels, 2 * REACH, width), F32),
            pltpu.SemaphoreType.DMA((channels,)),
            pltpu.SemaphoreType.DMA((2, channels)),
        ],
        compiler_params=pltpu.CompilerParams(vmem_limit_bytes=12 << 20),
    )(spread, done, tall, above, below)


def shards(cell_index, weights, block_tile, spread):
    rows_n, cols_n = lax.axis_size("row"), lax.axis_size("col")
    raw, rows, cols, values = outer(*exchange(cell_index, weights, block_tile, rows_n, cols_n))
    done = inner(spread, raw, rows, cols, values, rows_n, cols_n)
    return finish(spread, *done, rows_n, cols_n)


def solution(mesh):
    return jax.shard_map(
        shards,
        mesh=mesh,
        in_specs=(
            P(("groups", "row", "col"), None),
            P(("groups", "row", "col"), None),
            P(("groups", "row", "col")),
            P(),
        ),
        out_specs=P(None, ("groups", "row"), "col"),
        check_vma=False,
    )
```

```python
import functools

import jax
import jax.numpy as jnp
from jax import lax
from jax.experimental import pallas as pl
from jax.experimental.pallas import tpu as pltpu
from jax.sharding import PartitionSpec as P

REACH = 16
TILE_ROWS = 256
TILE_COLS = 1024
CAPACITY = 3
LANES = 128
WINDOW = 64
LEAD = 24
BITS = 9
HALF = 1 << (BITS - 1)
CHUNK_ROWS = 2
UNROLL = 3
MESH = pl.DeviceIdType.MESH
F32 = jnp.float32
BF16 = jnp.bfloat16


def iota(shape, dim):
    return lax.broadcasted_iota(jnp.int32, shape, dim)


def in_hbm(value):
    return pltpu.with_memory_space_constraint(value, pltpu.MemorySpace.HBM)


def dot(a, b):
    return lax.dot_general(a, b, (((1,), (0,)), ((), ())), preferred_element_type=F32)


def exchange_kernel(
    rows_n, cols_n, cell_hbm, weight_hbm, tile_hbm, message_out, zeros_out,
    cell_ref, weight_ref, tile_ref, values, keys_t, sorted_points, send_message,
    send_sem, recv_sem, local_sem
):
    loads = [
        pltpu.make_async_copy(source, target, local_sem.at[i])
        for i, (source, target) in enumerate(
            ((cell_hbm, cell_ref), (weight_hbm, weight_ref), (tile_hbm, tile_ref))
        )
    ]
    for load in loads:
        load.start()
    blocks, points = cell_ref.shape
    channels = weight_ref.shape[1] // points
    peers = rows_n * cols_n
    my_row, my_col = lax.axis_index("row"), lax.axis_index("col")
    me = my_row * cols_n + my_col

    offsets = []
    for distance in range(rows_n // 2, 0, -1):
        for step in (distance, rows_n - distance):
            if step not in [o[0] for o in offsets]:
                offsets += [(step, c) for c in range(cols_n)]
    offsets += [(0, c) for c in range(1, cols_n)]

    barrier = pltpu.get_barrier_semaphore()
    targets = []
    for step, turn in offsets:
        row = lax.rem(my_row + step, rows_n)
        col = lax.rem(my_col + turn, cols_n)
        targets.append((row, col))
        pl.semaphore_signal(
            barrier, inc=1, device_id={"row": row, "col": col}, device_id_type=MESH
        )

    for load in loads:
        load.wait()
    tile = tile_ref[...]
    square = (blocks, blocks)
    tile_down = jnp.sum(
        jnp.where(iota(square, 0) == iota(square, 1), tile, 0), axis=1, keepdims=True
    )
    earlier = (tile_down == tile) & (iota(square, 0) < iota(square, 1))
    turn_of = jnp.sum(earlier.astype(jnp.int32), axis=0, keepdims=True)
    cells = cell_ref[...]
    rows_each = channels + 2
    parts = [weight_ref[:, c * points : (c + 1) * points] for c in range(channels)] + [
        (part - HALF).astype(F32).astype(BF16)
        for part in (cells >> BITS, cells & (2 * HALF - 1))
    ]
    group = CAPACITY * points
    ramp = (iota((1, points), 1) * (TILE_ROWS // points * TILE_COLS // (2 * HALF)) - HALF).astype(F32)
    keys = []
    for k in range(CAPACITY):
        chosen = ((iota((peers, blocks), 0) == tile) & (turn_of == k)).astype(F32)
        empty = jnp.sum(chosen, axis=1, keepdims=True) < 0.5
        placed = dot(chosen.astype(BF16), jnp.concatenate(parts, axis=1))
        for v in range(rows_each):
            piece = placed[:, v * points : (v + 1) * points]
            if v == channels:
                piece = jnp.where(empty, ramp, piece)
                index = (iota((1, points), 1) + k * points).astype(F32)
                keys.append((piece + float(HALF)) * 512.0 + index)
            if v == channels + 1:
                piece = jnp.where(empty, -float(HALF), piece)
            values[v, :, k * points : (k + 1) * points] = piece
    pad = jnp.zeros((points - peers, points), F32)
    keys_t[...] = jnp.concatenate(
        [jnp.transpose(jnp.concatenate([key, pad], axis=0)) for key in keys], axis=0
    )
    keys = jnp.concatenate(keys, axis=1)
    quarter = points // 4
    chunks = quarter // CHUNK_ROWS
    share = group // chunks
    for t in range(peers):
        less = (keys_t[:, t : t + 1] < keys[t : t + 1, :]).astype(F32)
        rank = jnp.sum(less, axis=0, keepdims=True).astype(jnp.int32)
        chunk = (rank * (65536 // share + 1)) >> 16
        inside = rank - chunk * share
        third = (inside * (512 // CAPACITY + 1)) >> 9
        lane = (inside - third * CAPACITY) * points
        lane = lane + (third & 3) * quarter + chunk * CHUNK_ROWS + (third >> 2)
        hot = (iota((group, group), 0) == lane).astype(F32).astype(BF16)
        piece = jnp.concatenate(
            [values[v, t : t + 1, :] for v in range(rows_each)]
            + [jnp.zeros((8 - rows_each, group), F32)],
            axis=0,
        ).astype(BF16)
        sorted_points[t] = lax.dot_general(
            piece, hot, (((1,), (1,)), ((), ())), preferred_element_type=F32
        )
    for k in range(CAPACITY):
        part = slice(k * points, (k + 1) * points)
        for v in range(rows_each):
            send_message[:, k * rows_each + v, :] = sorted_points[:, v, part].astype(BF16)

    zeros_out[...] = jnp.zeros_like(zeros_out)
    own = pltpu.make_async_copy(send_message.at[me], message_out.at[me], local_sem.at[3])
    pl.semaphore_wait(barrier, peers - 1)
    copies = []
    for i, (row, col) in enumerate(targets):
        copy = pltpu.make_async_remote_copy(
            src_ref=send_message.at[row * cols_n + col],
            dst_ref=message_out.at[me],
            send_sem=send_sem.at[i],
            recv_sem=recv_sem.at[i],
            device_id={"row": row, "col": col},
            device_id_type=MESH,
        )
        copy.start()
        copies.append(copy)
    own.start()
    own.wait()
    for copy in copies:
        copy.wait_recv()
    for copy in copies:
        copy.wait_send()


def exchange(cell_index, weights, block_tile, rows_n, cols_n):
    blocks, points = cell_index.shape
    channels = weights.shape[1] // points
    peers = rows_n * cols_n
    message = (peers, CAPACITY * (channels + 2), points)
    return pl.pallas_call(
        functools.partial(exchange_kernel, rows_n, cols_n),
        name="exchange",
        out_shape=(
            jax.ShapeDtypeStruct(message, BF16),
            jax.ShapeDtypeStruct((channels, TILE_ROWS, TILE_COLS), F32),
        ),
        in_specs=[pl.BlockSpec(memory_space=pltpu.MemorySpace.HBM)] * 3,
        out_specs=(pl.BlockSpec(memory_space=pltpu.VMEM),) * 2,
        scratch_shapes=[
            pltpu.VMEM(cell_index.shape, jnp.int32),
            pltpu.VMEM(weights.shape, BF16),
            pltpu.VMEM((1, blocks), jnp.int32),
            pltpu.VMEM((channels + 2, peers, CAPACITY * points), F32),
            pltpu.VMEM((CAPACITY * points, points), F32),
            pltpu.VMEM((peers, 8, CAPACITY * points), F32),
            pltpu.VMEM(message, BF16),
            pltpu.SemaphoreType.DMA((peers - 1,)),
            pltpu.SemaphoreType.DMA((peers - 1,)),
            pltpu.SemaphoreType.DMA((4,)),
        ],
        compiler_params=pltpu.CompilerParams(
            collective_id=0, has_side_effects=True, vmem_limit_bytes=8 << 20
        ),
    )(*(in_hbm(x) for x in (cell_index, weights, block_tile.reshape(1, -1))))


def widened(slots, quarter):
    return jnp.concatenate(
        [
            jnp.concatenate([s[:, v * quarter : (v + 1) * quarter] for v in range(4)], axis=0)
            for s in slots
        ]
        + [jnp.zeros((LANES, LANES - len(slots) * quarter), F32)],
        axis=1,
    )


def add_window(raw_ref, rows_s, cols_s, weights_s, j, low, stop, base):
    channels = raw_ref.shape[0]
    quarter = LANES // 4
    span = 256

    def take(ref):
        return jnp.concatenate(
            [
                ref[pl.ds(quarter * k + CHUNK_ROWS * j + i, 1), :]
                for k in range(CAPACITY)
                for i in range(CHUNK_ROWS)
            ],
            axis=1,
        )

    row = take(rows_s)
    count = row.shape[1]
    cols = pltpu.roll(cols_s[...], lax.rem(LANES - CHUNK_ROWS * j, LANES), axis=1)
    offset = jnp.where((row >= low) & (row < stop), row - base, -1)
    hot = iota((WINDOW, count), 0) == offset
    left = jnp.concatenate(
        [jnp.where(hot, take(weights_s.at[c]), 0.0).astype(BF16) for c in range(channels)],
        axis=0,
    )
    for g in range(TILE_COLS // span):
        target = iota((LANES, span), 1) + g * span
        right = jnp.concatenate(
            [
                (target == cols[:, quarter * k + i : quarter * k + i + 1]).astype(F32).astype(BF16)
                for k in range(CAPACITY)
                for i in range(CHUNK_ROWS)
            ],
            axis=0,
        )
        layer = dot(left, right)
        for c in range(channels):
            raw_ref[c, pl.ds(base, WINDOW), g * span : (g + 1) * span] += layer[
                c * WINDOW : (c + 1) * WINDOW
            ]


def inner_chunks(chunks):
    tall = TILE_ROWS // chunks
    inner = [
        j
        for j in range(chunks)
        if tall * j - LEAD >= REACH and tall * j - LEAD + WINDOW <= TILE_ROWS - REACH
    ]
    return tall, inner[0], inner[-1] + 1


def outer_kernel(
    cols_n, message_ref, zeros_ref, raw_ref, rows_s, cols_s, weights_s, corner_ref, wide_s, first_s, last_s, next_s
):
    senders, rows_all, points = message_ref.shape
    rows_each = rows_all // CAPACITY
    channels = rows_each - 2
    quarter = points // 4
    chunks = quarter // CHUNK_ROWS
    wide_s[...] = message_ref[...].astype(F32)

    def wide(v):
        return widened([wide_s[:, k * rows_each + v, :] for k in range(CAPACITY)], quarter)

    cells = (wide(channels) + HALF) * (2 * HALF) + (wide(channels + 1) + HALF)
    cols_s[...] = cells.astype(jnp.int32) & (TILE_COLS - 1)
    rows = jnp.transpose(cells).astype(jnp.int32) >> (TILE_COLS.bit_length() - 1)
    rows_s[...] = rows
    for c in range(channels):
        weights_s[c] = jnp.transpose(wide(c))
    low, high = rows[:quarter], rows[:quarter]
    for k in range(1, CAPACITY):
        low = jnp.minimum(low, rows[quarter * k : quarter * (k + 1)])
        high = jnp.maximum(high, rows[quarter * k : quarter * (k + 1)])
    low = jnp.min(low, axis=1, keepdims=True)
    high = jnp.max(high, axis=1, keepdims=True)
    tall, begin, end = inner_chunks(chunks)
    for j in range(chunks):
        lows = [low[CHUNK_ROWS * j + i, 0] for i in range(CHUNK_ROWS)]
        highs = [high[CHUNK_ROWS * j + i, 0] for i in range(CHUNK_ROWS)]
        first = (functools.reduce(jnp.minimum, lows) >> 3) << 3
        done = tall * j - LEAD if begin <= j < end else first
        first_s[j] = first
        last_s[j] = functools.reduce(jnp.maximum, highs)
        next_s[j] = jnp.where(first < done, first, done + WINDOW)

    def add(j, low, stop):
        base = pl.multiple_of(jnp.minimum(low, TILE_ROWS - WINDOW), 8)
        add_window(raw_ref, rows_s, cols_s, weights_s, j, low, stop, base)

    def common(i, carry):
        j = jnp.where(i < begin, i, i + end - begin)
        low = first_s[j]
        add(j, low, low + WINDOW)
        return carry

    lax.fori_loop(0, chunks - (end - begin), common, 0, unroll=True)

    def rest(j, carry):
        done = jnp.where((j >= begin) & (j < end), tall * j - LEAD, first_s[j])

        def more(low):
            stop = jnp.where(low < done, jnp.minimum(low + WINDOW, done), low + WINDOW)
            add(j, low, stop)
            return jnp.where(stop == done, done + WINDOW, stop)

        lax.while_loop(lambda low: low <= last_s[j], more, next_s[j])
        return carry

    lax.fori_loop(0, chunks, rest, 0)
    my_col = lax.axis_index("col")
    near = pl.ds(pl.multiple_of((1 - my_col) * (TILE_COLS - LANES), LANES), LANES)
    for i, start in enumerate((0, TILE_ROWS - REACH)):
        packed = jnp.zeros((REACH, LANES), F32)
        lane = iota(packed.shape, 1)
        for c in range(channels):
            block = raw_ref[c, start : start + REACH, near]
            block = pltpu.roll(block, REACH * c + REACH * (1 - my_col), axis=1)
            mine = (lane >= REACH * c) & (lane < REACH * (c + 1))
            packed = jnp.where(mine, block, packed)
        corner_ref[i] = packed


def outer(message, zeros, cols_n):
    senders, rows_all, points = message.shape
    channels = rows_all // CAPACITY - 2
    vmem = pl.BlockSpec(memory_space=pltpu.VMEM)
    turns = points // 4 // CHUNK_ROWS
    return pl.pallas_call(
        functools.partial(outer_kernel, cols_n),
        name="outer",
        out_shape=(
            jax.ShapeDtypeStruct((channels, TILE_ROWS, TILE_COLS), F32),
            jax.ShapeDtypeStruct((LANES, LANES), jnp.int32),
            jax.ShapeDtypeStruct((LANES, LANES), jnp.int32),
            jax.ShapeDtypeStruct((channels, LANES, LANES), F32),
            jax.ShapeDtypeStruct((2, REACH, LANES), F32),
        ),
        in_specs=[vmem] * 2,
        input_output_aliases={1: 0},
        out_specs=(vmem,) * 5,
        scratch_shapes=[pltpu.VMEM(message.shape, F32)]
        + [pltpu.SMEM((turns,), jnp.int32)] * 3,
        compiler_params=pltpu.CompilerParams(vmem_limit_bytes=16 << 20),
    )(message, zeros)


def split(value):
    high = value.astype(BF16)
    return high, (value - high.astype(F32)).astype(BF16)


def tap(offset, width):
    near = jnp.abs(offset) <= REACH
    far = offset.astype(F32)
    return jnp.where(near, jnp.exp(-(far * far) / (2.0 * width * width)), 0.0)


def col_band(width):
    source = iota((2 * LANES, LANES), 0)
    source = jnp.where(source < LANES + LANES // 2, source, source - 2 * LANES)
    high, low = split(tap(source - iota((2 * LANES, LANES), 1), width))
    return jnp.concatenate([high, low], axis=1), high


def along_cols(block, beyond, count, my_col, cols_n, band, high, store):
    for n in range(count):
        own = block(n)
        before = block(n - 1) if n else jnp.where(my_col > 0, beyond, 0.0)
        after = block(n + 1) if n + 1 < count else jnp.where(my_col + 1 < cols_n, beyond, 0.0)
        edge = jnp.where(iota(own.shape, 1) < LANES // 2, after, before)
        x_high, x_low = split(jnp.concatenate([own, edge], axis=1))
        both = dot(x_high, band)
        store(n, both[:, :LANES] + both[:, LANES:] + dot(x_low, high))


def inner_kernel(
    rows_n, cols_n, spread_hbm, raw_ref, rows_s, cols_s, weights_s, corner_ref,
    out_ref, tall, above, below, corners, spread_ref, acc, send_sem, recv_sem, load_sem
):
    channels, height, width = raw_ref.shape
    my_row, my_col = lax.axis_index("row"), lax.axis_index("col")
    other = lax.rem(my_col + 1, cols_n)
    prev = lax.rem(my_row + rows_n - 1, rows_n)
    following = lax.rem(my_row + 1, rows_n)

    def at(row, col):
        return {"row": row, "col": col}

    barrier = pltpu.get_barrier_semaphore()
    peers = [at(prev, my_col), at(following, my_col), at(prev, other), at(following, other), at(my_row, other)]
    for peer in peers:
        pl.semaphore_signal(barrier, inc=1, device_id=peer, device_id_type=MESH)
    load = pltpu.make_async_copy(spread_hbm, spread_ref, load_sem)
    load.start()
    acc[...] = raw_ref[...]
    tall_rows, begin, end = inner_chunks(LANES // 4 // CHUNK_ROWS)

    def chunk(j, carry):
        base = pl.multiple_of(tall_rows * j - LEAD, 8)
        add_window(acc, rows_s, cols_s, weights_s, j, base, base + WINDOW, base)
        return carry

    chunk(begin, 0)
    pl.semaphore_wait(barrier, len(peers))
    near = pl.ds(pl.multiple_of((1 - my_col) * (width - LANES), LANES), LANES)
    beyond = pl.ds(width, LANES)
    top, bottom = pl.ds(0, REACH), pl.ds(height - REACH, REACH)

    def remote(i, source, target, peer):
        return pltpu.make_async_remote_copy(
            src_ref=source, dst_ref=target, send_sem=send_sem.at[i], recv_sem=recv_sem.at[i],
            device_id=peer, device_id_type=MESH,
        )

    halo = [
        remote(0, raw_ref.at[:, bottom, :], above, peers[1]),
        remote(1, raw_ref.at[:, top, :], below, peers[0]),
        remote(2, corner_ref.at[1], corners.at[0], peers[3]),
        remote(3, corner_ref.at[0], corners.at[1], peers[2]),
    ]
    for copy in halo:
        copy.start()
    lax.fori_loop(begin + 1, end, chunk, 0, unroll=UNROLL)

    def row_band(c):
        return split(tap(iota((height, height), 1) - iota((height, height), 0), spread_ref[0, c]))

    def along_rows(high, low, x):
        x_high, x_low = split(x)
        both = dot(jnp.concatenate([high, low], axis=0), x_high)
        return both[:height] + both[height:] + dot(high, x_low)

    step = 2 * LANES
    load.wait()

    def own_rows(c, carry):
        high, low = row_band(c)
        for g in range(width // step):
            cols = slice(g * step, (g + 1) * step)
            tall[c, :, cols] = along_rows(high, low, acc[c, :, cols])
        return carry

    def partner(c):
        return remote(4 + c, tall.at[c, :, near], tall.at[c, :, beyond], peers[4])

    def next_rows(c, carry):
        own_rows(c, carry)
        partner(c - 1).start()
        return carry

    own_rows(0, 0)
    lax.fori_loop(1, channels, next_rows, 0)
    partner(channels - 1).start()

    def inner_cols(c, carry):
        partner(c).wait_recv()
        band, high = col_band(spread_ref[1, c])
        rows = slice(REACH, height - REACH)

        def block(n):
            return tall[c, rows, n * LANES : (n + 1) * LANES]

        def store(n, value):
            out_ref[c, rows, n * LANES : (n + 1) * LANES] = value

        count = width // LANES
        along_cols(block, block(count), count, my_col, cols_n, band, high, store)
        return carry

    lax.fori_loop(0, channels - 1, inner_cols, 0)
    partner(channels - 1).wait_recv()
    for copy in halo:
        copy.wait_recv()
    for copy in halo + [partner(c) for c in range(channels)]:
        copy.wait_send()


def inner(spread, raw, rows, cols, weights, corner, rows_n, cols_n):
    channels, height, width = raw.shape
    vmem = pl.BlockSpec(memory_space=pltpu.VMEM)
    return pl.pallas_call(
        functools.partial(inner_kernel, rows_n, cols_n),
        name="inner",
        out_shape=(
            jax.ShapeDtypeStruct((channels - 1, height, width), F32),
            jax.ShapeDtypeStruct((channels, height, width + LANES), F32),
            jax.ShapeDtypeStruct((channels, REACH, width), F32),
            jax.ShapeDtypeStruct((channels, REACH, width), F32),
            jax.ShapeDtypeStruct(corner.shape, F32),
        ),
        in_specs=[pl.BlockSpec(memory_space=pltpu.MemorySpace.HBM)] + [vmem] * 5,
        out_specs=(vmem,) * 5,
        scratch_shapes=[
            pltpu.SMEM(spread.shape, F32),
            pltpu.VMEM(raw.shape, F32),
            pltpu.SemaphoreType.DMA((4 + channels,)),
            pltpu.SemaphoreType.DMA((4 + channels,)),
            pltpu.SemaphoreType.DMA,
        ],
        compiler_params=pltpu.CompilerParams(
            collective_id=1, has_side_effects=True, vmem_limit_bytes=24 << 20
        ),
    )(in_hbm(spread), raw, rows, cols, weights, corner)


def finish_kernel(
    rows_n, cols_n, spread_ref, done_ref, tall, above, below, corners, out_ref,
    last, edge, inner_sem, edge_sem
):
    channels, height, width = out_ref.shape
    my_row, my_col = lax.axis_index("row"), lax.axis_index("col")
    count = width // LANES
    rows = pl.ds(REACH, height - 2 * REACH)
    copies = [
        pltpu.make_async_copy(done_ref.at[c, rows], out_ref.at[c, rows], inner_sem.at[c])
        for c in range(channels - 1)
    ]
    for copy in copies:
        copy.start()
    c = channels - 1

    def last_block(n):
        return tall[c, REACH : height - REACH, n * LANES : (n + 1) * LANES]

    def last_store(n, value):
        last[:, n * LANES : (n + 1) * LANES] = value

    band, high = col_band(spread_ref[1, c])
    along_cols(last_block, last_block(count), count, my_col, cols_n, band, high, last_store)
    copies.append(pltpu.make_async_copy(last, out_ref.at[c, rows], inner_sem.at[c]))
    copies[-1].start()
    shape = (REACH, 3 * REACH)
    part = iota(shape, 1) >> (REACH.bit_length() - 1)
    offset = (iota(shape, 1) & (REACH - 1)) - iota(shape, 0)
    for c in range(channels):
        sides = []
        turn = lax.rem(my_col * (LANES - REACH) + LANES - REACH * c, LANES)
        for i, (halo, start, shift, real) in enumerate(
            (
                (above, 0, -REACH, my_row > 0),
                (below, height - REACH, REACH, my_row + 1 < rows_n),
            )
        ):
            taps = jnp.where(real, tap(offset + shift, spread_ref[0, c]), 0.0)
            high = taps.astype(BF16).astype(F32)
            taps = jnp.where(part == 1, taps - high, high).astype(BF16)
            beyond = pltpu.roll(corners[i], turn, axis=1)
            x_high, x_low = split(jnp.concatenate([halo[c], beyond], axis=1))
            sides.append(
                tall[c, start : start + REACH, :]
                + dot(taps, jnp.concatenate([x_high, x_high, x_low], axis=0))
            )
        rows = jnp.concatenate(sides, axis=0)
        band, high = col_band(spread_ref[1, c])

        def block(n):
            return rows[:, n * LANES : (n + 1) * LANES]

        def store(n, value):
            edge[c, :, n * LANES : (n + 1) * LANES] = value

        along_cols(block, block(count), count, my_col, cols_n, band, high, store)
        for i, start in enumerate((0, height - REACH)):
            copies.append(
                pltpu.make_async_copy(
                    edge.at[c, pl.ds(i * REACH, REACH)],
                    out_ref.at[c, pl.ds(start, REACH)],
                    edge_sem.at[i, c],
                )
            )
            copies[-1].start()
    for copy in copies:
        copy.wait()


def finish(spread, done, tall, above, below, corners, rows_n, cols_n):
    channels, height, wide = tall.shape
    width = wide - LANES
    vmem = pl.BlockSpec(memory_space=pltpu.VMEM)
    return pl.pallas_call(
        functools.partial(finish_kernel, rows_n, cols_n),
        name="finish",
        out_shape=jax.ShapeDtypeStruct((channels, height, width), F32),
        in_specs=[pl.BlockSpec(memory_space=pltpu.SMEM)] + [vmem] * 5,
        out_specs=pl.BlockSpec(memory_space=pltpu.MemorySpace.HBM),
        scratch_shapes=[
            pltpu.VMEM((height - 2 * REACH, width), F32),
            pltpu.VMEM((channels, 2 * REACH, width), F32),
            pltpu.SemaphoreType.DMA((channels,)),
            pltpu.SemaphoreType.DMA((2, channels)),
        ],
        compiler_params=pltpu.CompilerParams(vmem_limit_bytes=12 << 20),
    )(spread, done, tall, above, below, corners)


def shards(cell_index, weights, block_tile, spread):
    rows_n, cols_n = lax.axis_size("row"), lax.axis_size("col")
    message, zeros = exchange(cell_index, weights, block_tile, rows_n, cols_n)
    points = outer(message, zeros, cols_n)
    done = inner(spread, *points, rows_n, cols_n)
    return finish(spread, *done, rows_n, cols_n)


def solution(mesh):
    return jax.shard_map(
        shards,
        mesh=mesh,
        in_specs=(
            P(("groups", "row", "col"), None),
            P(("groups", "row", "col"), None),
            P(("groups", "row", "col")),
            P(),
        ),
        out_specs=P(None, ("groups", "row"), "col"),
        check_vma=False,
    )
```

```python
import functools

import jax
import jax.numpy as jnp
from jax import lax
from jax.experimental import pallas as pl
from jax.experimental.pallas import tpu as pltpu
from jax.sharding import PartitionSpec as P

REACH = 16
TILE_ROWS = 256
TILE_COLS = 1024
CAPACITY = 3
LANES = 128
WINDOW = 64
LEAD = 24
BITS = 9
HALF = 1 << (BITS - 1)
CHUNK_ROWS = 2
UNROLL = 3
MESH = pl.DeviceIdType.MESH
F32 = jnp.float32
BF16 = jnp.bfloat16


def iota(shape, dim):
    return lax.broadcasted_iota(jnp.int32, shape, dim)


def in_hbm(value):
    return pltpu.with_memory_space_constraint(value, pltpu.MemorySpace.HBM)


def dot(a, b):
    return lax.dot_general(a, b, (((1,), (0,)), ((), ())), preferred_element_type=F32)


def exchange_kernel(
    rows_n, cols_n, cell_hbm, weight_hbm, tile_hbm, message_out, zeros_out,
    cell_ref, weight_ref, tile_ref, values, keys_t, sorted_points, send_message,
    send_sem, recv_sem, local_sem
):
    loads = [
        pltpu.make_async_copy(source, target, local_sem.at[i])
        for i, (source, target) in enumerate(
            ((cell_hbm, cell_ref), (weight_hbm, weight_ref), (tile_hbm, tile_ref))
        )
    ]
    for load in loads:
        load.start()
    blocks, points = cell_ref.shape
    channels = weight_ref.shape[1] // points
    peers = rows_n * cols_n
    my_row, my_col = lax.axis_index("row"), lax.axis_index("col")
    me = my_row * cols_n + my_col

    offsets = []
    for distance in range(rows_n // 2, 0, -1):
        for step in (distance, rows_n - distance):
            if step not in [o[0] for o in offsets]:
                offsets += [(step, c) for c in range(cols_n)]
    offsets += [(0, c) for c in range(1, cols_n)]

    barrier = pltpu.get_barrier_semaphore()
    targets = []
    for step, turn in offsets:
        row = lax.rem(my_row + step, rows_n)
        col = lax.rem(my_col + turn, cols_n)
        targets.append((row, col))
        pl.semaphore_signal(
            barrier, inc=1, device_id={"row": row, "col": col}, device_id_type=MESH
        )

    for load in loads:
        load.wait()
    tile = tile_ref[...]
    square = (blocks, blocks)
    tile_down = jnp.sum(
        jnp.where(iota(square, 0) == iota(square, 1), tile, 0), axis=1, keepdims=True
    )
    earlier = (tile_down == tile) & (iota(square, 0) < iota(square, 1))
    turn_of = jnp.sum(earlier.astype(jnp.int32), axis=0, keepdims=True)
    cells = cell_ref[...]
    rows_each = channels + 2
    parts = [weight_ref[:, c * points : (c + 1) * points] for c in range(channels)] + [
        (part - HALF).astype(F32).astype(BF16)
        for part in (cells >> BITS, cells & (2 * HALF - 1))
    ]
    group = CAPACITY * points
    ramp = (iota((1, points), 1) * (TILE_ROWS // points * TILE_COLS // (2 * HALF)) - HALF).astype(F32)
    keys = []
    for k in range(CAPACITY):
        chosen = ((iota((peers, blocks), 0) == tile) & (turn_of == k)).astype(F32)
        empty = jnp.sum(chosen, axis=1, keepdims=True) < 0.5
        placed = dot(chosen.astype(BF16), jnp.concatenate(parts, axis=1))
        for v in range(rows_each):
            piece = placed[:, v * points : (v + 1) * points]
            if v == channels:
                piece = jnp.where(empty, ramp, piece)
                index = (iota((1, points), 1) + k * points).astype(F32)
                keys.append((piece + float(HALF)) * 512.0 + index)
            if v == channels + 1:
                piece = jnp.where(empty, -float(HALF), piece)
            values[v, :, k * points : (k + 1) * points] = piece
    pad = jnp.zeros((points - peers, points), F32)
    keys_t[...] = jnp.concatenate(
        [jnp.transpose(jnp.concatenate([key, pad], axis=0)) for key in keys], axis=0
    )
    keys = jnp.concatenate(keys, axis=1)
    quarter = points // 4
    chunks = quarter // CHUNK_ROWS
    share = group // chunks
    for t in range(peers):
        less = (keys_t[:, t : t + 1] < keys[t : t + 1, :]).astype(F32)
        rank = jnp.sum(less, axis=0, keepdims=True).astype(jnp.int32)
        chunk = (rank * (65536 // share + 1)) >> 16
        inside = rank - chunk * share
        third = (inside * (512 // CAPACITY + 1)) >> 9
        lane = (inside - third * CAPACITY) * points
        lane = lane + (third & 3) * quarter + chunk * CHUNK_ROWS + (third >> 2)
        hot = (iota((group, group), 0) == lane).astype(F32).astype(BF16)
        piece = jnp.concatenate(
            [values[v, t : t + 1, :] for v in range(rows_each)]
            + [jnp.zeros((8 - rows_each, group), F32)],
            axis=0,
        ).astype(BF16)
        sorted_points[t] = lax.dot_general(
            piece, hot, (((1,), (1,)), ((), ())), preferred_element_type=F32
        )
    for k in range(CAPACITY):
        part = slice(k * points, (k + 1) * points)
        for v in range(rows_each):
            send_message[:, k * rows_each + v, :] = sorted_points[:, v, part].astype(BF16)

    zeros_out[...] = jnp.zeros_like(zeros_out)
    own = pltpu.make_async_copy(send_message.at[me], message_out.at[me], local_sem.at[3])
    pl.semaphore_wait(barrier, peers - 1)
    copies = []
    for i, (row, col) in enumerate(targets):
        copy = pltpu.make_async_remote_copy(
            src_ref=send_message.at[row * cols_n + col],
            dst_ref=message_out.at[me],
            send_sem=send_sem.at[i],
            recv_sem=recv_sem.at[i],
            device_id={"row": row, "col": col},
            device_id_type=MESH,
        )
        copy.start()
        copies.append(copy)
    own.start()
    own.wait()
    for copy in copies:
        copy.wait_recv()
    for copy in copies:
        copy.wait_send()


def exchange(cell_index, weights, block_tile, rows_n, cols_n):
    blocks, points = cell_index.shape
    channels = weights.shape[1] // points
    peers = rows_n * cols_n
    message = (peers, CAPACITY * (channels + 2), points)
    return pl.pallas_call(
        functools.partial(exchange_kernel, rows_n, cols_n),
        name="exchange",
        out_shape=(
            jax.ShapeDtypeStruct(message, BF16),
            jax.ShapeDtypeStruct((channels, TILE_ROWS, TILE_COLS), F32),
        ),
        in_specs=[pl.BlockSpec(memory_space=pltpu.MemorySpace.HBM)] * 3,
        out_specs=(pl.BlockSpec(memory_space=pltpu.VMEM),) * 2,
        scratch_shapes=[
            pltpu.VMEM(cell_index.shape, jnp.int32),
            pltpu.VMEM(weights.shape, BF16),
            pltpu.VMEM((1, blocks), jnp.int32),
            pltpu.VMEM((channels + 2, peers, CAPACITY * points), F32),
            pltpu.VMEM((CAPACITY * points, points), F32),
            pltpu.VMEM((peers, 8, CAPACITY * points), F32),
            pltpu.VMEM(message, BF16),
            pltpu.SemaphoreType.DMA((peers - 1,)),
            pltpu.SemaphoreType.DMA((peers - 1,)),
            pltpu.SemaphoreType.DMA((4,)),
        ],
        compiler_params=pltpu.CompilerParams(
            collective_id=0, has_side_effects=True, vmem_limit_bytes=8 << 20
        ),
    )(*(in_hbm(x) for x in (cell_index, weights, block_tile.reshape(1, -1))))


def widened(slots, quarter):
    return jnp.concatenate(
        [
            jnp.concatenate([s[:, v * quarter : (v + 1) * quarter] for v in range(4)], axis=0)
            for s in slots
        ]
        + [jnp.zeros((LANES, LANES - len(slots) * quarter), F32)],
        axis=1,
    )


def add_window(raw_ref, rows_s, cols_s, weights_s, j, low, stop, base):
    channels = raw_ref.shape[0]
    quarter = LANES // 4
    span = 256

    def take(ref):
        return jnp.concatenate(
            [
                ref[pl.ds(quarter * k + CHUNK_ROWS * j + i, 1), :]
                for k in range(CAPACITY)
                for i in range(CHUNK_ROWS)
            ],
            axis=1,
        )

    row = take(rows_s)
    count = row.shape[1]
    cols = pltpu.roll(cols_s[...], lax.rem(LANES - CHUNK_ROWS * j, LANES), axis=1)
    offset = jnp.where((row >= low) & (row < stop), row - base, -1)
    hot = iota((WINDOW, count), 0) == offset
    left = jnp.concatenate(
        [jnp.where(hot, take(weights_s.at[c]), 0.0).astype(BF16) for c in range(channels)],
        axis=0,
    )
    for g in range(TILE_COLS // span):
        target = iota((LANES, span), 1) + g * span
        right = jnp.concatenate(
            [
                (target == cols[:, quarter * k + i : quarter * k + i + 1]).astype(F32).astype(BF16)
                for k in range(CAPACITY)
                for i in range(CHUNK_ROWS)
            ],
            axis=0,
        )
        layer = dot(left, right)
        for c in range(channels):
            raw_ref[c, pl.ds(base, WINDOW), g * span : (g + 1) * span] += layer[
                c * WINDOW : (c + 1) * WINDOW
            ]


def fixed_row(j, chunks):
    row = TILE_ROWS // chunks * j - LEAD
    return min(max(row, REACH), TILE_ROWS - REACH - WINDOW)


def inner_chunks(chunks):
    tall = TILE_ROWS // chunks
    inner = [
        j
        for j in range(chunks)
        if tall * (j - 1) >= REACH and tall * (j + 2) <= TILE_ROWS - REACH
    ]
    return inner[0], inner[-1] + 1


def outer_kernel(
    cols_n, message_ref, zeros_ref, raw_ref, rows_s, cols_s, weights_s, corner_ref, wide_s, first_s, last_s, next_s, done_s
):
    senders, rows_all, points = message_ref.shape
    rows_each = rows_all // CAPACITY
    channels = rows_each - 2
    quarter = points // 4
    chunks = quarter // CHUNK_ROWS
    wide_s[...] = message_ref[...].astype(F32)

    def wide(v):
        return widened([wide_s[:, k * rows_each + v, :] for k in range(CAPACITY)], quarter)

    cells = (wide(channels) + HALF) * (2 * HALF) + (wide(channels + 1) + HALF)
    cols_s[...] = cells.astype(jnp.int32) & (TILE_COLS - 1)
    rows = jnp.transpose(cells).astype(jnp.int32) >> (TILE_COLS.bit_length() - 1)
    rows_s[...] = rows
    for c in range(channels):
        weights_s[c] = jnp.transpose(wide(c))
    low, high = rows[:quarter], rows[:quarter]
    for k in range(1, CAPACITY):
        low = jnp.minimum(low, rows[quarter * k : quarter * (k + 1)])
        high = jnp.maximum(high, rows[quarter * k : quarter * (k + 1)])
    low = jnp.min(low, axis=1, keepdims=True)
    high = jnp.max(high, axis=1, keepdims=True)
    begin, end = inner_chunks(chunks)
    for j in range(chunks):
        lows = [low[CHUNK_ROWS * j + i, 0] for i in range(CHUNK_ROWS)]
        highs = [high[CHUNK_ROWS * j + i, 0] for i in range(CHUNK_ROWS)]
        first = (functools.reduce(jnp.minimum, lows) >> 3) << 3
        done = fixed_row(j, chunks) if begin <= j < end else first
        done_s[j] = done
        first_s[j] = first
        last_s[j] = functools.reduce(jnp.maximum, highs)
        next_s[j] = jnp.where(first < done, first, done + WINDOW)

    def add(j, low, stop):
        base = pl.multiple_of(jnp.minimum(low, TILE_ROWS - WINDOW), 8)
        add_window(raw_ref, rows_s, cols_s, weights_s, j, low, stop, base)

    def common(i, carry):
        j = jnp.where(i < begin, i, i + end - begin)
        low = first_s[j]
        add(j, low, low + WINDOW)
        return carry

    lax.fori_loop(0, chunks - (end - begin), common, 0, unroll=True)

    def rest(j, carry):
        done = done_s[j]

        def more(low):
            stop = jnp.where(low < done, jnp.minimum(low + WINDOW, done), low + WINDOW)
            add(j, low, stop)
            return jnp.where(stop == done, done + WINDOW, stop)

        lax.while_loop(lambda low: low <= last_s[j], more, next_s[j])
        return carry

    lax.fori_loop(0, chunks, rest, 0)
    my_col = lax.axis_index("col")
    near = pl.ds(pl.multiple_of((1 - my_col) * (TILE_COLS - LANES), LANES), LANES)
    for i, start in enumerate((0, TILE_ROWS - REACH)):
        packed = jnp.zeros((REACH, LANES), F32)
        lane = iota(packed.shape, 1)
        for c in range(channels):
            block = raw_ref[c, start : start + REACH, near]
            block = pltpu.roll(block, REACH * c + REACH * (1 - my_col), axis=1)
            mine = (lane >= REACH * c) & (lane < REACH * (c + 1))
            packed = jnp.where(mine, block, packed)
        corner_ref[i] = packed


def outer(message, zeros, cols_n):
    senders, rows_all, points = message.shape
    channels = rows_all // CAPACITY - 2
    vmem = pl.BlockSpec(memory_space=pltpu.VMEM)
    turns = points // 4 // CHUNK_ROWS
    return pl.pallas_call(
        functools.partial(outer_kernel, cols_n),
        name="outer",
        out_shape=(
            jax.ShapeDtypeStruct((channels, TILE_ROWS, TILE_COLS), F32),
            jax.ShapeDtypeStruct((LANES, LANES), jnp.int32),
            jax.ShapeDtypeStruct((LANES, LANES), jnp.int32),
            jax.ShapeDtypeStruct((channels, LANES, LANES), F32),
            jax.ShapeDtypeStruct((2, REACH, LANES), F32),
        ),
        in_specs=[vmem] * 2,
        input_output_aliases={1: 0},
        out_specs=(vmem,) * 5,
        scratch_shapes=[pltpu.VMEM(message.shape, F32)]
        + [pltpu.SMEM((turns,), jnp.int32)] * 4,
        compiler_params=pltpu.CompilerParams(vmem_limit_bytes=16 << 20),
    )(message, zeros)


def split(value):
    high = value.astype(BF16)
    return high, (value - high.astype(F32)).astype(BF16)


def tap(offset, width):
    near = jnp.abs(offset) <= REACH
    far = offset.astype(F32)
    return jnp.where(near, jnp.exp(-(far * far) / (2.0 * width * width)), 0.0)


def col_band(width):
    source = iota((2 * LANES, LANES), 0)
    source = jnp.where(source < LANES + LANES // 2, source, source - 2 * LANES)
    high, low = split(tap(source - iota((2 * LANES, LANES), 1), width))
    return jnp.concatenate([high, low], axis=1), high


def along_cols(block, beyond, count, my_col, cols_n, band, high, store):
    for n in range(count):
        own = block(n)
        before = block(n - 1) if n else jnp.where(my_col > 0, beyond, 0.0)
        after = block(n + 1) if n + 1 < count else jnp.where(my_col + 1 < cols_n, beyond, 0.0)
        edge = jnp.where(iota(own.shape, 1) < LANES // 2, after, before)
        x_high, x_low = split(jnp.concatenate([own, edge], axis=1))
        both = dot(x_high, band)
        store(n, both[:, :LANES] + both[:, LANES:] + dot(x_low, high))


def inner_kernel(
    rows_n, cols_n, spread_hbm, raw_ref, rows_s, cols_s, weights_s, corner_ref,
    out_ref, tall, above, below, corners, spread_ref, acc, send_sem, recv_sem, load_sem
):
    channels, height, width = raw_ref.shape
    my_row, my_col = lax.axis_index("row"), lax.axis_index("col")
    other = lax.rem(my_col + 1, cols_n)
    prev = lax.rem(my_row + rows_n - 1, rows_n)
    following = lax.rem(my_row + 1, rows_n)

    def at(row, col):
        return {"row": row, "col": col}

    barrier = pltpu.get_barrier_semaphore()
    peers = [at(prev, my_col), at(following, my_col), at(prev, other), at(following, other), at(my_row, other)]
    for peer in peers:
        pl.semaphore_signal(barrier, inc=1, device_id=peer, device_id_type=MESH)
    load = pltpu.make_async_copy(spread_hbm, spread_ref, load_sem)
    load.start()
    acc[...] = raw_ref[...]
    chunks = LANES // 4 // CHUNK_ROWS
    begin, end = inner_chunks(chunks)

    def add(j, base):
        add_window(acc, rows_s, cols_s, weights_s, j, base, base + WINDOW, base)

    def chunk(j, carry):
        add(j, pl.multiple_of(TILE_ROWS // chunks * j - LEAD, 8))
        return carry

    for j in (begin, end - 1, begin + 1):
        add(j, fixed_row(j, chunks))
    pl.semaphore_wait(barrier, len(peers))
    near = pl.ds(pl.multiple_of((1 - my_col) * (width - LANES), LANES), LANES)
    beyond = pl.ds(width, LANES)
    top, bottom = pl.ds(0, REACH), pl.ds(height - REACH, REACH)

    def remote(i, source, target, peer):
        return pltpu.make_async_remote_copy(
            src_ref=source, dst_ref=target, send_sem=send_sem.at[i], recv_sem=recv_sem.at[i],
            device_id=peer, device_id_type=MESH,
        )

    halo = [
        remote(0, raw_ref.at[:, bottom, :], above, peers[1]),
        remote(1, raw_ref.at[:, top, :], below, peers[0]),
        remote(2, corner_ref.at[1], corners.at[0], peers[3]),
        remote(3, corner_ref.at[0], corners.at[1], peers[2]),
    ]
    for copy in halo:
        copy.start()
    lax.fori_loop(begin + 2, end - 1, chunk, 0, unroll=UNROLL)

    def row_band(c):
        return split(tap(iota((height, height), 1) - iota((height, height), 0), spread_ref[0, c]))

    def along_rows(high, low, x):
        x_high, x_low = split(x)
        both = dot(jnp.concatenate([high, low], axis=0), x_high)
        return both[:height] + both[height:] + dot(high, x_low)

    step = 2 * LANES
    load.wait()

    def own_rows(c, carry):
        high, low = row_band(c)
        for g in range(width // step):
            cols = slice(g * step, (g + 1) * step)
            tall[c, :, cols] = along_rows(high, low, acc[c, :, cols])
        return carry

    def partner(c):
        return remote(4 + c, tall.at[c, :, near], tall.at[c, :, beyond], peers[4])

    def next_rows(c, carry):
        own_rows(c, carry)
        partner(c - 1).start()
        return carry

    own_rows(0, 0)
    lax.fori_loop(1, channels, next_rows, 0)
    partner(channels - 1).start()

    def inner_cols(c, carry):
        partner(c).wait_recv()
        band, high = col_band(spread_ref[1, c])
        rows = slice(REACH, height - REACH)

        def block(n):
            return tall[c, rows, n * LANES : (n + 1) * LANES]

        def store(n, value):
            out_ref[c, rows, n * LANES : (n + 1) * LANES] = value

        count = width // LANES
        along_cols(block, block(count), count, my_col, cols_n, band, high, store)
        return carry

    lax.fori_loop(0, channels - 1, inner_cols, 0)
    partner(channels - 1).wait_recv()
    for copy in halo:
        copy.wait_recv()
    for copy in halo + [partner(c) for c in range(channels)]:
        copy.wait_send()


def inner(spread, raw, rows, cols, weights, corner, rows_n, cols_n):
    channels, height, width = raw.shape
    vmem = pl.BlockSpec(memory_space=pltpu.VMEM)
    return pl.pallas_call(
        functools.partial(inner_kernel, rows_n, cols_n),
        name="inner",
        out_shape=(
            jax.ShapeDtypeStruct((channels - 1, height, width), F32),
            jax.ShapeDtypeStruct((channels, height, width + LANES), F32),
            jax.ShapeDtypeStruct((channels, REACH, width), F32),
            jax.ShapeDtypeStruct((channels, REACH, width), F32),
            jax.ShapeDtypeStruct(corner.shape, F32),
        ),
        in_specs=[pl.BlockSpec(memory_space=pltpu.MemorySpace.HBM)] + [vmem] * 5,
        out_specs=(vmem,) * 5,
        scratch_shapes=[
            pltpu.SMEM(spread.shape, F32),
            pltpu.VMEM(raw.shape, F32),
            pltpu.SemaphoreType.DMA((4 + channels,)),
            pltpu.SemaphoreType.DMA((4 + channels,)),
            pltpu.SemaphoreType.DMA,
        ],
        compiler_params=pltpu.CompilerParams(
            collective_id=1, has_side_effects=True, vmem_limit_bytes=24 << 20
        ),
    )(in_hbm(spread), raw, rows, cols, weights, corner)


def finish_kernel(
    rows_n, cols_n, spread_ref, done_ref, tall, above, below, corners, out_ref,
    last, edge, inner_sem, edge_sem
):
    channels, height, width = out_ref.shape
    my_row, my_col = lax.axis_index("row"), lax.axis_index("col")
    count = width // LANES
    rows = pl.ds(REACH, height - 2 * REACH)
    copies = [
        pltpu.make_async_copy(done_ref.at[c, rows], out_ref.at[c, rows], inner_sem.at[c])
        for c in range(channels - 1)
    ]
    for copy in copies:
        copy.start()
    c = channels - 1

    def last_block(n):
        return tall[c, REACH : height - REACH, n * LANES : (n + 1) * LANES]

    def last_store(n, value):
        last[:, n * LANES : (n + 1) * LANES] = value

    band, high = col_band(spread_ref[1, c])
    along_cols(last_block, last_block(count), count, my_col, cols_n, band, high, last_store)
    copies.append(pltpu.make_async_copy(last, out_ref.at[c, rows], inner_sem.at[c]))
    copies[-1].start()
    shape = (REACH, 3 * REACH)
    part = iota(shape, 1) >> (REACH.bit_length() - 1)
    offset = (iota(shape, 1) & (REACH - 1)) - iota(shape, 0)
    for c in range(channels):
        sides = []
        turn = lax.rem(my_col * (LANES - REACH) + LANES - REACH * c, LANES)
        for i, (halo, start, shift, real) in enumerate(
            (
                (above, 0, -REACH, my_row > 0),
                (below, height - REACH, REACH, my_row + 1 < rows_n),
            )
        ):
            taps = jnp.where(real, tap(offset + shift, spread_ref[0, c]), 0.0)
            high = taps.astype(BF16).astype(F32)
            taps = jnp.where(part == 1, taps - high, high).astype(BF16)
            beyond = pltpu.roll(corners[i], turn, axis=1)
            x_high, x_low = split(jnp.concatenate([halo[c], beyond], axis=1))
            sides.append(
                tall[c, start : start + REACH, :]
                + dot(taps, jnp.concatenate([x_high, x_high, x_low], axis=0))
            )
        rows = jnp.concatenate(sides, axis=0)
        band, high = col_band(spread_ref[1, c])

        def block(n):
            return rows[:, n * LANES : (n + 1) * LANES]

        def store(n, value):
            edge[c, :, n * LANES : (n + 1) * LANES] = value

        along_cols(block, block(count), count, my_col, cols_n, band, high, store)
        for i, start in enumerate((0, height - REACH)):
            copies.append(
                pltpu.make_async_copy(
                    edge.at[c, pl.ds(i * REACH, REACH)],
                    out_ref.at[c, pl.ds(start, REACH)],
                    edge_sem.at[i, c],
                )
            )
            copies[-1].start()
    for copy in copies:
        copy.wait()


def finish(spread, done, tall, above, below, corners, rows_n, cols_n):
    channels, height, wide = tall.shape
    width = wide - LANES
    vmem = pl.BlockSpec(memory_space=pltpu.VMEM)
    return pl.pallas_call(
        functools.partial(finish_kernel, rows_n, cols_n),
        name="finish",
        out_shape=jax.ShapeDtypeStruct((channels, height, width), F32),
        in_specs=[pl.BlockSpec(memory_space=pltpu.SMEM)] + [vmem] * 5,
        out_specs=pl.BlockSpec(memory_space=pltpu.MemorySpace.HBM),
        scratch_shapes=[
            pltpu.VMEM((height - 2 * REACH, width), F32),
            pltpu.VMEM((channels, 2 * REACH, width), F32),
            pltpu.SemaphoreType.DMA((channels,)),
            pltpu.SemaphoreType.DMA((2, channels)),
        ],
        compiler_params=pltpu.CompilerParams(vmem_limit_bytes=12 << 20),
    )(spread, done, tall, above, below, corners)


def shards(cell_index, weights, block_tile, spread):
    rows_n, cols_n = lax.axis_size("row"), lax.axis_size("col")
    message, zeros = exchange(cell_index, weights, block_tile, rows_n, cols_n)
    points = outer(message, zeros, cols_n)
    done = inner(spread, *points, rows_n, cols_n)
    return finish(spread, *done, rows_n, cols_n)


def solution(mesh):
    return jax.shard_map(
        shards,
        mesh=mesh,
        in_specs=(
            P(("groups", "row", "col"), None),
            P(("groups", "row", "col"), None),
            P(("groups", "row", "col")),
            P(),
        ),
        out_specs=P(None, ("groups", "row"), "col"),
        check_vma=False,
    )
```

```python
import functools

import jax
import jax.numpy as jnp
from jax import lax
from jax.experimental import pallas as pl
from jax.experimental.pallas import tpu as pltpu
from jax.sharding import PartitionSpec as P

REACH = 16
TILE_ROWS = 256
TILE_COLS = 1024
CAPACITY = 3
LANES = 128
WINDOW = 64
LEAD = 24
BITS = 9
HALF = 1 << (BITS - 1)
CHUNK_ROWS = 2
UNROLL = 9
MESH = pl.DeviceIdType.MESH
F32 = jnp.float32
BF16 = jnp.bfloat16


def iota(shape, dim):
    return lax.broadcasted_iota(jnp.int32, shape, dim)


def in_hbm(value):
    return pltpu.with_memory_space_constraint(value, pltpu.MemorySpace.HBM)


def dot(a, b):
    return lax.dot_general(a, b, (((1,), (0,)), ((), ())), preferred_element_type=F32)


def exchange_kernel(
    rows_n, cols_n, cell_hbm, weight_hbm, tile_hbm, message_out, zeros_out,
    cell_ref, weight_ref, tile_ref, values, keys_t, sorted_points, send_message,
    send_sem, recv_sem, local_sem
):
    loads = [
        pltpu.make_async_copy(source, target, local_sem.at[i])
        for i, (source, target) in enumerate(
            ((cell_hbm, cell_ref), (weight_hbm, weight_ref), (tile_hbm, tile_ref))
        )
    ]
    for load in loads:
        load.start()
    blocks, points = cell_ref.shape
    channels = weight_ref.shape[1] // points
    peers = rows_n * cols_n
    my_row, my_col = lax.axis_index("row"), lax.axis_index("col")
    me = my_row * cols_n + my_col

    offsets = []
    for distance in range(rows_n // 2, 0, -1):
        for step in (distance, rows_n - distance):
            if step not in [o[0] for o in offsets]:
                offsets += [(step, c) for c in range(cols_n)]
    offsets += [(0, c) for c in range(1, cols_n)]

    barrier = pltpu.get_barrier_semaphore()
    targets = []
    for step, turn in offsets:
        row = lax.rem(my_row + step, rows_n)
        col = lax.rem(my_col + turn, cols_n)
        targets.append((row, col))
        pl.semaphore_signal(
            barrier, inc=1, device_id={"row": row, "col": col}, device_id_type=MESH
        )

    for load in loads:
        load.wait()
    tile = tile_ref[...]
    square = (blocks, blocks)
    tile_down = jnp.sum(
        jnp.where(iota(square, 0) == iota(square, 1), tile, 0), axis=1, keepdims=True
    )
    earlier = (tile_down == tile) & (iota(square, 0) < iota(square, 1))
    turn_of = jnp.sum(earlier.astype(jnp.int32), axis=0, keepdims=True)
    cells = cell_ref[...]
    rows_each = channels + 2
    parts = [weight_ref[:, c * points : (c + 1) * points] for c in range(channels)] + [
        (part - HALF).astype(F32).astype(BF16)
        for part in (cells >> BITS, cells & (2 * HALF - 1))
    ]
    group = CAPACITY * points
    ramp = (iota((1, points), 1) * (TILE_ROWS // points * TILE_COLS // (2 * HALF)) - HALF).astype(F32)
    keys = []
    for k in range(CAPACITY):
        chosen = ((iota((peers, blocks), 0) == tile) & (turn_of == k)).astype(F32)
        empty = jnp.sum(chosen, axis=1, keepdims=True) < 0.5
        placed = dot(chosen.astype(BF16), jnp.concatenate(parts, axis=1))
        for v in range(rows_each):
            piece = placed[:, v * points : (v + 1) * points]
            if v == channels:
                piece = jnp.where(empty, ramp, piece)
                index = (iota((1, points), 1) + k * points).astype(F32)
                keys.append((piece + float(HALF)) * 512.0 + index)
            if v == channels + 1:
                piece = jnp.where(empty, -float(HALF), piece)
            values[v, :, k * points : (k + 1) * points] = piece
    pad = jnp.zeros((points - peers, points), F32)
    keys_t[...] = jnp.concatenate(
        [jnp.transpose(jnp.concatenate([key, pad], axis=0)) for key in keys], axis=0
    )
    keys = jnp.concatenate(keys, axis=1)
    quarter = points // 4
    chunks = quarter // CHUNK_ROWS
    share = group // chunks
    for t in range(peers):
        less = (keys_t[:, t : t + 1] < keys[t : t + 1, :]).astype(F32)
        rank = jnp.sum(less, axis=0, keepdims=True).astype(jnp.int32)
        chunk = (rank * (65536 // share + 1)) >> 16
        inside = rank - chunk * share
        third = (inside * (512 // CAPACITY + 1)) >> 9
        lane = (inside - third * CAPACITY) * points
        lane = lane + (third & 3) * quarter + chunk * CHUNK_ROWS + (third >> 2)
        hot = (iota((group, group), 0) == lane).astype(F32).astype(BF16)
        piece = jnp.concatenate(
            [values[v, t : t + 1, :] for v in range(rows_each)]
            + [jnp.zeros((8 - rows_each, group), F32)],
            axis=0,
        ).astype(BF16)
        sorted_points[t] = lax.dot_general(
            piece, hot, (((1,), (1,)), ((), ())), preferred_element_type=F32
        )
    for k in range(CAPACITY):
        part = slice(k * points, (k + 1) * points)
        for v in range(rows_each):
            send_message[:, k * rows_each + v, :] = sorted_points[:, v, part].astype(BF16)

    zeros_out[...] = jnp.zeros_like(zeros_out)
    own = pltpu.make_async_copy(send_message.at[me], message_out.at[me], local_sem.at[3])
    pl.semaphore_wait(barrier, peers - 1)
    copies = []
    for i, (row, col) in enumerate(targets):
        copy = pltpu.make_async_remote_copy(
            src_ref=send_message.at[row * cols_n + col],
            dst_ref=message_out.at[me],
            send_sem=send_sem.at[i],
            recv_sem=recv_sem.at[i],
            device_id={"row": row, "col": col},
            device_id_type=MESH,
        )
        copy.start()
        copies.append(copy)
    own.start()
    own.wait()
    for copy in copies:
        copy.wait_recv()
    for copy in copies:
        copy.wait_send()


def exchange(cell_index, weights, block_tile, rows_n, cols_n):
    blocks, points = cell_index.shape
    channels = weights.shape[1] // points
    peers = rows_n * cols_n
    message = (peers, CAPACITY * (channels + 2), points)
    return pl.pallas_call(
        functools.partial(exchange_kernel, rows_n, cols_n),
        name="exchange",
        out_shape=(
            jax.ShapeDtypeStruct(message, BF16),
            jax.ShapeDtypeStruct((channels, TILE_ROWS, TILE_COLS), F32),
        ),
        in_specs=[pl.BlockSpec(memory_space=pltpu.MemorySpace.HBM)] * 3,
        out_specs=(pl.BlockSpec(memory_space=pltpu.VMEM),) * 2,
        scratch_shapes=[
            pltpu.VMEM(cell_index.shape, jnp.int32),
            pltpu.VMEM(weights.shape, BF16),
            pltpu.VMEM((1, blocks), jnp.int32),
            pltpu.VMEM((channels + 2, peers, CAPACITY * points), F32),
            pltpu.VMEM((CAPACITY * points, points), F32),
            pltpu.VMEM((peers, 8, CAPACITY * points), F32),
            pltpu.VMEM(message, BF16),
            pltpu.SemaphoreType.DMA((peers - 1,)),
            pltpu.SemaphoreType.DMA((peers - 1,)),
            pltpu.SemaphoreType.DMA((4,)),
        ],
        compiler_params=pltpu.CompilerParams(
            collective_id=0, has_side_effects=True, vmem_limit_bytes=8 << 20
        ),
    )(*(in_hbm(x) for x in (cell_index, weights, block_tile.reshape(1, -1))))


def widened(slots, quarter):
    return jnp.concatenate(
        [
            jnp.concatenate([s[:, v * quarter : (v + 1) * quarter] for v in range(4)], axis=0)
            for s in slots
        ]
        + [jnp.zeros((LANES, LANES - len(slots) * quarter), F32)],
        axis=1,
    )


def add_window(raw_ref, rows_s, cols_s, weights_s, j, low, stop, base):
    channels = raw_ref.shape[0]
    quarter = LANES // 4
    span = 256

    def take(ref):
        return jnp.concatenate(
            [
                ref[pl.ds(quarter * k + CHUNK_ROWS * j + i, 1), :]
                for k in range(CAPACITY)
                for i in range(CHUNK_ROWS)
            ],
            axis=1,
        )

    row = take(rows_s)
    count = row.shape[1]
    cols = pltpu.roll(cols_s[...], lax.rem(LANES - CHUNK_ROWS * j, LANES), axis=1)
    offset = jnp.where((row >= low) & (row < stop), row - base, -1)
    hot = iota((WINDOW, count), 0) == offset
    left = jnp.concatenate(
        [jnp.where(hot, take(weights_s.at[c]), 0.0).astype(BF16) for c in range(channels)],
        axis=0,
    )
    for g in range(TILE_COLS // span):
        target = iota((LANES, span), 1) + g * span
        right = jnp.concatenate(
            [
                (target == cols[:, quarter * k + i : quarter * k + i + 1]).astype(F32).astype(BF16)
                for k in range(CAPACITY)
                for i in range(CHUNK_ROWS)
            ],
            axis=0,
        )
        layer = dot(left, right)
        for c in range(channels):
            raw_ref[c, pl.ds(base, WINDOW), g * span : (g + 1) * span] += layer[
                c * WINDOW : (c + 1) * WINDOW
            ]


def fixed_row(j, chunks):
    row = TILE_ROWS // chunks * j - LEAD
    return min(max(row, REACH), TILE_ROWS - REACH - WINDOW)


def inner_chunks(chunks):
    tall = TILE_ROWS // chunks
    inner = [
        j
        for j in range(chunks)
        if tall * (j - 1) >= REACH and tall * (j + 2) <= TILE_ROWS - REACH
    ]
    return inner[0], inner[-1] + 1


def outer_kernel(
    cols_n, message_ref, zeros_ref, raw_ref, rows_s, cols_s, weights_s, corner_ref, wide_s, first_s, last_s, next_s, done_s
):
    senders, rows_all, points = message_ref.shape
    rows_each = rows_all // CAPACITY
    channels = rows_each - 2
    quarter = points // 4
    chunks = quarter // CHUNK_ROWS
    wide_s[...] = message_ref[...].astype(F32)

    def wide(v):
        return widened([wide_s[:, k * rows_each + v, :] for k in range(CAPACITY)], quarter)

    cells = (wide(channels) + HALF) * (2 * HALF) + (wide(channels + 1) + HALF)
    cols_s[...] = cells.astype(jnp.int32) & (TILE_COLS - 1)
    rows = jnp.transpose(cells).astype(jnp.int32) >> (TILE_COLS.bit_length() - 1)
    rows_s[...] = rows
    for c in range(channels):
        weights_s[c] = jnp.transpose(wide(c))
    low, high = rows[:quarter], rows[:quarter]
    for k in range(1, CAPACITY):
        low = jnp.minimum(low, rows[quarter * k : quarter * (k + 1)])
        high = jnp.maximum(high, rows[quarter * k : quarter * (k + 1)])
    low = jnp.min(low, axis=1, keepdims=True)
    high = jnp.max(high, axis=1, keepdims=True)
    begin, end = inner_chunks(chunks)
    for j in range(chunks):
        lows = [low[CHUNK_ROWS * j + i, 0] for i in range(CHUNK_ROWS)]
        highs = [high[CHUNK_ROWS * j + i, 0] for i in range(CHUNK_ROWS)]
        first = (functools.reduce(jnp.minimum, lows) >> 3) << 3
        done = fixed_row(j, chunks) if begin <= j < end else first
        done_s[j] = done
        first_s[j] = first
        last_s[j] = functools.reduce(jnp.maximum, highs)
        next_s[j] = jnp.where(first < done, first, done + WINDOW)

    def add(j, low, stop):
        base = pl.multiple_of(jnp.minimum(low, TILE_ROWS - WINDOW), 8)
        add_window(raw_ref, rows_s, cols_s, weights_s, j, low, stop, base)

    def common(i, carry):
        j = jnp.where(i < begin, i, i + end - begin)
        low = first_s[j]
        add(j, low, low + WINDOW)
        return carry

    lax.fori_loop(0, chunks - (end - begin), common, 0, unroll=True)

    def rest(j, carry):
        done = done_s[j]

        def more(low):
            stop = jnp.where(low < done, jnp.minimum(low + WINDOW, done), low + WINDOW)
            add(j, low, stop)
            return jnp.where(stop == done, done + WINDOW, stop)

        lax.while_loop(lambda low: low <= last_s[j], more, next_s[j])
        return carry

    lax.fori_loop(0, chunks, rest, 0)
    my_col = lax.axis_index("col")
    near = pl.ds(pl.multiple_of((1 - my_col) * (TILE_COLS - LANES), LANES), LANES)
    for i, start in enumerate((0, TILE_ROWS - REACH)):
        packed = jnp.zeros((REACH, LANES), F32)
        lane = iota(packed.shape, 1)
        for c in range(channels):
            block = raw_ref[c, start : start + REACH, near]
            block = pltpu.roll(block, REACH * c + REACH * (1 - my_col), axis=1)
            mine = (lane >= REACH * c) & (lane < REACH * (c + 1))
            packed = jnp.where(mine, block, packed)
        corner_ref[i] = packed


def outer(message, zeros, cols_n):
    senders, rows_all, points = message.shape
    channels = rows_all // CAPACITY - 2
    vmem = pl.BlockSpec(memory_space=pltpu.VMEM)
    turns = points // 4 // CHUNK_ROWS
    return pl.pallas_call(
        functools.partial(outer_kernel, cols_n),
        name="outer",
        out_shape=(
            jax.ShapeDtypeStruct((channels, TILE_ROWS, TILE_COLS), F32),
            jax.ShapeDtypeStruct((LANES, LANES), jnp.int32),
            jax.ShapeDtypeStruct((LANES, LANES), jnp.int32),
            jax.ShapeDtypeStruct((channels, LANES, LANES), F32),
            jax.ShapeDtypeStruct((2, REACH, LANES), F32),
        ),
        in_specs=[vmem] * 2,
        input_output_aliases={1: 0},
        out_specs=(vmem,) * 5,
        scratch_shapes=[pltpu.VMEM(message.shape, F32)]
        + [pltpu.SMEM((turns,), jnp.int32)] * 4,
        compiler_params=pltpu.CompilerParams(vmem_limit_bytes=16 << 20),
    )(message, zeros)


def split(value):
    high = value.astype(BF16)
    return high, (value - high.astype(F32)).astype(BF16)


def tap(offset, width):
    near = jnp.abs(offset) <= REACH
    far = offset.astype(F32)
    return jnp.where(near, jnp.exp(-(far * far) / (2.0 * width * width)), 0.0)


def col_band(width):
    source = iota((2 * LANES, LANES), 0)
    source = jnp.where(source < LANES + LANES // 2, source, source - 2 * LANES)
    high, low = split(tap(source - iota((2 * LANES, LANES), 1), width))
    return jnp.concatenate([high, low], axis=1), high


def along_cols(block, beyond, count, my_col, cols_n, band, high, store):
    for n in range(count):
        own = block(n)
        before = block(n - 1) if n else jnp.where(my_col > 0, beyond, 0.0)
        after = block(n + 1) if n + 1 < count else jnp.where(my_col + 1 < cols_n, beyond, 0.0)
        edge = jnp.where(iota(own.shape, 1) < LANES // 2, after, before)
        x_high, x_low = split(jnp.concatenate([own, edge], axis=1))
        both = dot(x_high, band)
        store(n, both[:, :LANES] + both[:, LANES:] + dot(x_low, high))


def inner_kernel(
    rows_n, cols_n, spread_hbm, raw_ref, rows_s, cols_s, weights_s, corner_ref,
    out_ref, tall, above, below, corners, spread_ref, acc, send_sem, recv_sem, load_sem
):
    channels, height, width = raw_ref.shape
    my_row, my_col = lax.axis_index("row"), lax.axis_index("col")
    other = lax.rem(my_col + 1, cols_n)
    prev = lax.rem(my_row + rows_n - 1, rows_n)
    following = lax.rem(my_row + 1, rows_n)

    def at(row, col):
        return {"row": row, "col": col}

    barrier = pltpu.get_barrier_semaphore()
    peers = [at(prev, my_col), at(following, my_col), at(prev, other), at(following, other), at(my_row, other)]
    for peer in peers:
        pl.semaphore_signal(barrier, inc=1, device_id=peer, device_id_type=MESH)
    load = pltpu.make_async_copy(spread_hbm, spread_ref, load_sem)
    load.start()
    acc[...] = raw_ref[...]
    chunks = LANES // 4 // CHUNK_ROWS
    begin, end = inner_chunks(chunks)

    def add(j, base):
        add_window(acc, rows_s, cols_s, weights_s, j, base, base + WINDOW, base)

    def chunk(j, carry):
        add(j, pl.multiple_of(TILE_ROWS // chunks * j - LEAD, 8))
        return carry

    for j in (begin, end - 1, begin + 1):
        add(j, fixed_row(j, chunks))
    pl.semaphore_wait(barrier, len(peers))
    near = pl.ds(pl.multiple_of((1 - my_col) * (width - LANES), LANES), LANES)
    beyond = pl.ds(width, LANES)
    top, bottom = pl.ds(0, REACH), pl.ds(height - REACH, REACH)

    def remote(i, source, target, peer):
        return pltpu.make_async_remote_copy(
            src_ref=source, dst_ref=target, send_sem=send_sem.at[i], recv_sem=recv_sem.at[i],
            device_id=peer, device_id_type=MESH,
        )

    halo = [
        remote(0, raw_ref.at[:, bottom, :], above, peers[1]),
        remote(1, raw_ref.at[:, top, :], below, peers[0]),
        remote(2, corner_ref.at[1], corners.at[0], peers[3]),
        remote(3, corner_ref.at[0], corners.at[1], peers[2]),
    ]
    for copy in halo:
        copy.start()
    lax.fori_loop(begin + 2, end - 1, chunk, 0, unroll=UNROLL)

    def row_band(c):
        return split(tap(iota((height, height), 1) - iota((height, height), 0), spread_ref[0, c]))

    def along_rows(high, low, x):
        x_high, x_low = split(x)
        both = dot(jnp.concatenate([high, low], axis=0), x_high)
        return both[:height] + both[height:] + dot(high, x_low)

    step = 2 * LANES
    load.wait()

    def own_rows(c, carry):
        high, low = row_band(c)
        for g in range(width // step):
            cols = slice(g * step, (g + 1) * step)
            tall[c, :, cols] = along_rows(high, low, acc[c, :, cols])
        return carry

    def partner(c):
        return remote(4 + c, tall.at[c, :, near], tall.at[c, :, beyond], peers[4])

    def next_rows(c, carry):
        own_rows(c, carry)
        partner(c - 1).start()
        return carry

    own_rows(0, 0)
    lax.fori_loop(1, channels, next_rows, 0, unroll=True)
    partner(channels - 1).start()

    def inner_cols(c, carry):
        partner(c).wait_recv()
        band, high = col_band(spread_ref[1, c])
        rows = slice(REACH, height - REACH)

        def block(n):
            return tall[c, rows, n * LANES : (n + 1) * LANES]

        def store(n, value):
            out_ref[c, rows, n * LANES : (n + 1) * LANES] = value

        count = width // LANES
        along_cols(block, block(count), count, my_col, cols_n, band, high, store)
        return carry

    lax.fori_loop(0, channels - 1, inner_cols, 0, unroll=True)
    partner(channels - 1).wait_recv()
    for copy in halo:
        copy.wait_recv()
    for copy in halo + [partner(c) for c in range(channels)]:
        copy.wait_send()


def inner(spread, raw, rows, cols, weights, corner, rows_n, cols_n):
    channels, height, width = raw.shape
    vmem = pl.BlockSpec(memory_space=pltpu.VMEM)
    return pl.pallas_call(
        functools.partial(inner_kernel, rows_n, cols_n),
        name="inner",
        out_shape=(
            jax.ShapeDtypeStruct((channels - 1, height, width), F32),
            jax.ShapeDtypeStruct((channels, height, width + LANES), F32),
            jax.ShapeDtypeStruct((channels, REACH, width), F32),
            jax.ShapeDtypeStruct((channels, REACH, width), F32),
            jax.ShapeDtypeStruct(corner.shape, F32),
        ),
        in_specs=[pl.BlockSpec(memory_space=pltpu.MemorySpace.HBM)] + [vmem] * 5,
        out_specs=(vmem,) * 5,
        scratch_shapes=[
            pltpu.SMEM(spread.shape, F32),
            pltpu.VMEM(raw.shape, F32),
            pltpu.SemaphoreType.DMA((4 + channels,)),
            pltpu.SemaphoreType.DMA((4 + channels,)),
            pltpu.SemaphoreType.DMA,
        ],
        compiler_params=pltpu.CompilerParams(
            collective_id=1, has_side_effects=True, vmem_limit_bytes=24 << 20
        ),
    )(in_hbm(spread), raw, rows, cols, weights, corner)


def finish_kernel(
    rows_n, cols_n, spread_ref, done_ref, tall, above, below, corners, out_ref,
    last, edge, inner_sem, edge_sem
):
    channels, height, width = out_ref.shape
    my_row, my_col = lax.axis_index("row"), lax.axis_index("col")
    count = width // LANES
    rows = pl.ds(REACH, height - 2 * REACH)
    copies = [
        pltpu.make_async_copy(done_ref.at[c, rows], out_ref.at[c, rows], inner_sem.at[c])
        for c in range(channels - 1)
    ]
    for copy in copies:
        copy.start()
    c = channels - 1

    def last_block(n):
        return tall[c, REACH : height - REACH, n * LANES : (n + 1) * LANES]

    def last_store(n, value):
        last[:, n * LANES : (n + 1) * LANES] = value

    band, high = col_band(spread_ref[1, c])
    along_cols(last_block, last_block(count), count, my_col, cols_n, band, high, last_store)
    copies.append(pltpu.make_async_copy(last, out_ref.at[c, rows], inner_sem.at[c]))
    copies[-1].start()
    shape = (REACH, 3 * REACH)
    part = iota(shape, 1) >> (REACH.bit_length() - 1)
    offset = (iota(shape, 1) & (REACH - 1)) - iota(shape, 0)
    for c in range(channels):
        sides = []
        turn = lax.rem(my_col * (LANES - REACH) + LANES - REACH * c, LANES)
        for i, (halo, start, shift, real) in enumerate(
            (
                (above, 0, -REACH, my_row > 0),
                (below, height - REACH, REACH, my_row + 1 < rows_n),
            )
        ):
            taps = jnp.where(real, tap(offset + shift, spread_ref[0, c]), 0.0)
            high = taps.astype(BF16).astype(F32)
            taps = jnp.where(part == 1, taps - high, high).astype(BF16)
            beyond = pltpu.roll(corners[i], turn, axis=1)
            x_high, x_low = split(jnp.concatenate([halo[c], beyond], axis=1))
            sides.append(
                tall[c, start : start + REACH, :]
                + dot(taps, jnp.concatenate([x_high, x_high, x_low], axis=0))
            )
        rows = jnp.concatenate(sides, axis=0)
        band, high = col_band(spread_ref[1, c])

        def block(n):
            return rows[:, n * LANES : (n + 1) * LANES]

        def store(n, value):
            edge[c, :, n * LANES : (n + 1) * LANES] = value

        along_cols(block, block(count), count, my_col, cols_n, band, high, store)
        for i, start in enumerate((0, height - REACH)):
            copies.append(
                pltpu.make_async_copy(
                    edge.at[c, pl.ds(i * REACH, REACH)],
                    out_ref.at[c, pl.ds(start, REACH)],
                    edge_sem.at[i, c],
                )
            )
            copies[-1].start()
    for copy in copies:
        copy.wait()


def finish(spread, done, tall, above, below, corners, rows_n, cols_n):
    channels, height, wide = tall.shape
    width = wide - LANES
    vmem = pl.BlockSpec(memory_space=pltpu.VMEM)
    return pl.pallas_call(
        functools.partial(finish_kernel, rows_n, cols_n),
        name="finish",
        out_shape=jax.ShapeDtypeStruct((channels, height, width), F32),
        in_specs=[pl.BlockSpec(memory_space=pltpu.SMEM)] + [vmem] * 5,
        out_specs=pl.BlockSpec(memory_space=pltpu.MemorySpace.HBM),
        scratch_shapes=[
            pltpu.VMEM((height - 2 * REACH, width), F32),
            pltpu.VMEM((channels, 2 * REACH, width), F32),
            pltpu.SemaphoreType.DMA((channels,)),
            pltpu.SemaphoreType.DMA((2, channels)),
        ],
        compiler_params=pltpu.CompilerParams(vmem_limit_bytes=12 << 20),
    )(spread, done, tall, above, below, corners)


def shards(cell_index, weights, block_tile, spread):
    rows_n, cols_n = lax.axis_size("row"), lax.axis_size("col")
    message, zeros = exchange(cell_index, weights, block_tile, rows_n, cols_n)
    points = outer(message, zeros, cols_n)
    done = inner(spread, *points, rows_n, cols_n)
    return finish(spread, *done, rows_n, cols_n)


def solution(mesh):
    return jax.shard_map(
        shards,
        mesh=mesh,
        in_specs=(
            P(("groups", "row", "col"), None),
            P(("groups", "row", "col"), None),
            P(("groups", "row", "col")),
            P(),
        ),
        out_specs=P(None, ("groups", "row"), "col"),
        check_vma=False,
    )
```

```python
import functools

import jax
import jax.numpy as jnp
from jax import lax
from jax.experimental import pallas as pl
from jax.experimental.pallas import tpu as pltpu
from jax.sharding import PartitionSpec as P

REACH = 16
TILE_ROWS = 256
TILE_COLS = 1024
CAPACITY = 3
LANES = 128
WINDOW = 64
LEAD = 24
BITS = 9
HALF = 1 << (BITS - 1)
CHUNK_ROWS = 2
UNROLL = 9
MESH = pl.DeviceIdType.MESH
F32 = jnp.float32
BF16 = jnp.bfloat16


def iota(shape, dim):
    return lax.broadcasted_iota(jnp.int32, shape, dim)


def in_hbm(value):
    return pltpu.with_memory_space_constraint(value, pltpu.MemorySpace.HBM)


def dot(a, b):
    return lax.dot_general(a, b, (((1,), (0,)), ((), ())), preferred_element_type=F32)


def split(value):
    high = value.astype(BF16)
    return high, (value - high.astype(F32)).astype(BF16)


def tap(offset, width):
    near = jnp.abs(offset) <= REACH
    far = offset.astype(F32)
    return jnp.where(near, jnp.exp(-(far * far) / (2.0 * width * width)), 0.0)


def col_band(width):
    source = iota((2 * LANES, LANES), 0)
    source = jnp.where(source < LANES + LANES // 2, source, source - 2 * LANES)
    high, low = split(tap(source - iota((2 * LANES, LANES), 1), width))
    return jnp.concatenate([high, low], axis=1)


def exchange_kernel(
    rows_n, cols_n, cell_hbm, weight_hbm, tile_hbm, spread_hbm,
    message_out, zeros_out, row_bands, col_bands, halo_taps,
    cell_ref, weight_ref, tile_ref, spread_ref, values, keys_t, sorted_points, send_message,
    send_sem, recv_sem, local_sem
):
    loads = [
        pltpu.make_async_copy(source, target, local_sem.at[i])
        for i, (source, target) in enumerate(
            (
                (cell_hbm, cell_ref),
                (weight_hbm, weight_ref),
                (tile_hbm, tile_ref),
                (spread_hbm, spread_ref),
            )
        )
    ]
    for load in loads:
        load.start()
    blocks, points = cell_ref.shape
    channels = weight_ref.shape[1] // points
    peers = rows_n * cols_n
    my_row, my_col = lax.axis_index("row"), lax.axis_index("col")
    me = my_row * cols_n + my_col

    offsets = []
    for distance in range(rows_n // 2, 0, -1):
        for step in (distance, rows_n - distance):
            if step not in [o[0] for o in offsets]:
                offsets += [(step, c) for c in range(cols_n)]
    offsets += [(0, c) for c in range(1, cols_n)]

    barrier = pltpu.get_barrier_semaphore()
    targets = []
    for step, turn in offsets:
        row = lax.rem(my_row + step, rows_n)
        col = lax.rem(my_col + turn, cols_n)
        targets.append((row, col))
        pl.semaphore_signal(
            barrier, inc=1, device_id={"row": row, "col": col}, device_id_type=MESH
        )

    for load in loads:
        load.wait()
    tile = tile_ref[...]
    square = (blocks, blocks)
    tile_down = jnp.sum(
        jnp.where(iota(square, 0) == iota(square, 1), tile, 0), axis=1, keepdims=True
    )
    earlier = (tile_down == tile) & (iota(square, 0) < iota(square, 1))
    turn_of = jnp.sum(earlier.astype(jnp.int32), axis=0, keepdims=True)
    cells = cell_ref[...]
    rows_each = channels + 2
    parts = [weight_ref[:, c * points : (c + 1) * points] for c in range(channels)] + [
        (part - HALF).astype(F32).astype(BF16)
        for part in (cells >> BITS, cells & (2 * HALF - 1))
    ]
    group = CAPACITY * points
    ramp = (iota((1, points), 1) * (TILE_ROWS // points * TILE_COLS // (2 * HALF)) - HALF).astype(F32)
    keys = []
    for k in range(CAPACITY):
        chosen = ((iota((peers, blocks), 0) == tile) & (turn_of == k)).astype(F32)
        empty = jnp.sum(chosen, axis=1, keepdims=True) < 0.5
        placed = dot(chosen.astype(BF16), jnp.concatenate(parts, axis=1))
        for v in range(rows_each):
            piece = placed[:, v * points : (v + 1) * points]
            if v == channels:
                piece = jnp.where(empty, ramp, piece)
                index = (iota((1, points), 1) + k * points).astype(F32)
                keys.append((piece + float(HALF)) * 512.0 + index)
            if v == channels + 1:
                piece = jnp.where(empty, -float(HALF), piece)
            values[v, :, k * points : (k + 1) * points] = piece
    pad = jnp.zeros((points - peers, points), F32)
    keys_t[...] = jnp.concatenate(
        [jnp.transpose(jnp.concatenate([key, pad], axis=0)) for key in keys], axis=0
    )
    keys = jnp.concatenate(keys, axis=1)
    quarter = points // 4
    chunks = quarter // CHUNK_ROWS
    share = group // chunks
    for t in range(peers):
        less = (keys_t[:, t : t + 1] < keys[t : t + 1, :]).astype(F32)
        rank = jnp.sum(less, axis=0, keepdims=True).astype(jnp.int32)
        chunk = (rank * (65536 // share + 1)) >> 16
        inside = rank - chunk * share
        third = (inside * (512 // CAPACITY + 1)) >> 9
        lane = (inside - third * CAPACITY) * points
        lane = lane + (third & 3) * quarter + chunk * CHUNK_ROWS + (third >> 2)
        hot = (iota((group, group), 0) == lane).astype(F32).astype(BF16)
        piece = jnp.concatenate(
            [values[v, t : t + 1, :] for v in range(rows_each)]
            + [jnp.zeros((8 - rows_each, group), F32)],
            axis=0,
        ).astype(BF16)
        sorted_points[t] = lax.dot_general(
            piece, hot, (((1,), (1,)), ((), ())), preferred_element_type=F32
        )
    for k in range(CAPACITY):
        part = slice(k * points, (k + 1) * points)
        for v in range(rows_each):
            send_message[:, k * rows_each + v, :] = sorted_points[:, v, part].astype(BF16)

    own = pltpu.make_async_copy(send_message.at[me], message_out.at[me], local_sem.at[4])
    pl.semaphore_wait(barrier, peers - 1)
    copies = []
    for i, (row, col) in enumerate(targets):
        copy = pltpu.make_async_remote_copy(
            src_ref=send_message.at[row * cols_n + col],
            dst_ref=message_out.at[me],
            send_sem=send_sem.at[i],
            recv_sem=recv_sem.at[i],
            device_id={"row": row, "col": col},
            device_id_type=MESH,
        )
        copy.start()
        copies.append(copy)
    own.start()
    zeros_out[...] = jnp.zeros_like(zeros_out)
    square = (TILE_ROWS, TILE_ROWS)
    shape = (REACH, 3 * REACH)
    part = iota(shape, 1) >> (REACH.bit_length() - 1)
    offset = (iota(shape, 1) & (REACH - 1)) - iota(shape, 0)
    for c in range(channels):
        high, low = split(tap(iota(square, 1) - iota(square, 0), spread_ref[0, c]))
        row_bands[c, :TILE_ROWS] = high
        row_bands[c, TILE_ROWS:] = low
        col_bands[c] = col_band(spread_ref[1, c])
        for i, (shift, real) in enumerate(((-REACH, my_row > 0), (REACH, my_row + 1 < rows_n))):
            taps = jnp.where(real, tap(offset + shift, spread_ref[0, c]), 0.0)
            high = taps.astype(BF16).astype(F32)
            halo_taps[c, i] = jnp.where(part == 1, taps - high, high).astype(BF16)
    own.wait()
    for copy in copies:
        copy.wait_recv()
    for copy in copies:
        copy.wait_send()


def exchange(cell_index, weights, block_tile, spread, rows_n, cols_n):
    blocks, points = cell_index.shape
    channels = weights.shape[1] // points
    peers = rows_n * cols_n
    message = (peers, CAPACITY * (channels + 2), points)
    return pl.pallas_call(
        functools.partial(exchange_kernel, rows_n, cols_n),
        name="exchange",
        out_shape=(
            jax.ShapeDtypeStruct(message, BF16),
            jax.ShapeDtypeStruct((channels, TILE_ROWS, TILE_COLS), F32),
            jax.ShapeDtypeStruct((channels, 2 * TILE_ROWS, TILE_ROWS), BF16),
            jax.ShapeDtypeStruct((channels, 2 * LANES, 2 * LANES), BF16),
            jax.ShapeDtypeStruct((channels, 2, REACH, 3 * REACH), BF16),
        ),
        in_specs=[pl.BlockSpec(memory_space=pltpu.MemorySpace.HBM)] * 4,
        out_specs=(pl.BlockSpec(memory_space=pltpu.VMEM),) * 5,
        scratch_shapes=[
            pltpu.VMEM(cell_index.shape, jnp.int32),
            pltpu.VMEM(weights.shape, BF16),
            pltpu.VMEM((1, blocks), jnp.int32),
            pltpu.SMEM(spread.shape, F32),
            pltpu.VMEM((channels + 2, peers, CAPACITY * points), F32),
            pltpu.VMEM((CAPACITY * points, points), F32),
            pltpu.VMEM((peers, 8, CAPACITY * points), F32),
            pltpu.VMEM(message, BF16),
            pltpu.SemaphoreType.DMA((peers - 1,)),
            pltpu.SemaphoreType.DMA((peers - 1,)),
            pltpu.SemaphoreType.DMA((5,)),
        ],
        compiler_params=pltpu.CompilerParams(
            collective_id=0, has_side_effects=True, vmem_limit_bytes=8 << 20
        ),
    )(*(in_hbm(x) for x in (cell_index, weights, block_tile.reshape(1, -1), spread)))


def widened(slots, quarter):
    return jnp.concatenate(
        [
            jnp.concatenate([s[:, v * quarter : (v + 1) * quarter] for v in range(4)], axis=0)
            for s in slots
        ]
        + [jnp.zeros((LANES, LANES - len(slots) * quarter), F32)],
        axis=1,
    )


def add_window(raw_ref, rows_s, cols_s, weights_s, j, low, stop, base):
    channels = raw_ref.shape[0]
    quarter = LANES // 4
    span = 256

    def take(ref):
        return jnp.concatenate(
            [
                ref[pl.ds(quarter * k + CHUNK_ROWS * j + i, 1), :]
                for k in range(CAPACITY)
                for i in range(CHUNK_ROWS)
            ],
            axis=1,
        )

    row = take(rows_s)
    count = row.shape[1]
    cols = pltpu.roll(cols_s[...], lax.rem(LANES - CHUNK_ROWS * j, LANES), axis=1)
    offset = jnp.where((row >= low) & (row < stop), row - base, -1)
    hot = iota((WINDOW, count), 0) == offset
    left = jnp.concatenate(
        [jnp.where(hot, take(weights_s.at[c]), 0.0).astype(BF16) for c in range(channels)],
        axis=0,
    )
    for g in range(TILE_COLS // span):
        target = iota((LANES, span), 1) + g * span
        right = jnp.concatenate(
            [
                (target == cols[:, quarter * k + i : quarter * k + i + 1]).astype(F32).astype(BF16)
                for k in range(CAPACITY)
                for i in range(CHUNK_ROWS)
            ],
            axis=0,
        )
        layer = dot(left, right)
        for c in range(channels):
            raw_ref[c, pl.ds(base, WINDOW), g * span : (g + 1) * span] += layer[
                c * WINDOW : (c + 1) * WINDOW
            ]


def fixed_row(j, chunks):
    row = TILE_ROWS // chunks * j - LEAD
    return min(max(row, REACH), TILE_ROWS - REACH - WINDOW)


def inner_chunks(chunks):
    tall = TILE_ROWS // chunks
    inner = [
        j
        for j in range(chunks)
        if tall * (j - 1) >= REACH and tall * (j + 2) <= TILE_ROWS - REACH
    ]
    return inner[0], inner[-1] + 1


def outer_kernel(
    cols_n, message_ref, zeros_ref, raw_ref, rows_s, cols_s, weights_s, corner_ref, wide_s, first_s, last_s, next_s, done_s
):
    senders, rows_all, points = message_ref.shape
    rows_each = rows_all // CAPACITY
    channels = rows_each - 2
    quarter = points // 4
    chunks = quarter // CHUNK_ROWS
    wide_s[...] = message_ref[...].astype(F32)

    def wide(v):
        return widened([wide_s[:, k * rows_each + v, :] for k in range(CAPACITY)], quarter)

    cells = (wide(channels) + HALF) * (2 * HALF) + (wide(channels + 1) + HALF)
    cols_s[...] = cells.astype(jnp.int32) & (TILE_COLS - 1)
    rows = jnp.transpose(cells).astype(jnp.int32) >> (TILE_COLS.bit_length() - 1)
    rows_s[...] = rows
    for c in range(channels):
        weights_s[c] = jnp.transpose(wide(c))
    low, high = rows[:quarter], rows[:quarter]
    for k in range(1, CAPACITY):
        low = jnp.minimum(low, rows[quarter * k : quarter * (k + 1)])
        high = jnp.maximum(high, rows[quarter * k : quarter * (k + 1)])
    low = jnp.min(low, axis=1, keepdims=True)
    high = jnp.max(high, axis=1, keepdims=True)
    begin, end = inner_chunks(chunks)
    for j in range(chunks):
        lows = [low[CHUNK_ROWS * j + i, 0] for i in range(CHUNK_ROWS)]
        highs = [high[CHUNK_ROWS * j + i, 0] for i in range(CHUNK_ROWS)]
        first = (functools.reduce(jnp.minimum, lows) >> 3) << 3
        done = fixed_row(j, chunks) if begin <= j < end else first
        done_s[j] = done
        first_s[j] = first
        last_s[j] = functools.reduce(jnp.maximum, highs)
        next_s[j] = jnp.where(first < done, first, done + WINDOW)

    def add(j, low, stop):
        base = pl.multiple_of(jnp.minimum(low, TILE_ROWS - WINDOW), 8)
        add_window(raw_ref, rows_s, cols_s, weights_s, j, low, stop, base)

    def common(i, carry):
        j = jnp.where(i < begin, i, i + end - begin)
        low = first_s[j]
        add(j, low, low + WINDOW)
        return carry

    lax.fori_loop(0, chunks - (end - begin), common, 0, unroll=True)

    def rest(j, carry):
        done = done_s[j]

        def more(low):
            stop = jnp.where(low < done, jnp.minimum(low + WINDOW, done), low + WINDOW)
            add(j, low, stop)
            return jnp.where(stop == done, done + WINDOW, stop)

        lax.while_loop(lambda low: low <= last_s[j], more, next_s[j])
        return carry

    lax.fori_loop(0, chunks, rest, 0)
    my_col = lax.axis_index("col")
    near = pl.ds(pl.multiple_of((1 - my_col) * (TILE_COLS - LANES), LANES), LANES)
    for i, start in enumerate((0, TILE_ROWS - REACH)):
        packed = jnp.zeros((REACH, LANES), F32)
        lane = iota(packed.shape, 1)
        for c in range(channels):
            block = raw_ref[c, start : start + REACH, near]
            block = pltpu.roll(block, REACH * c + REACH * (1 - my_col), axis=1)
            mine = (lane >= REACH * c) & (lane < REACH * (c + 1))
            packed = jnp.where(mine, block, packed)
        corner_ref[i] = packed


def outer(message, zeros, cols_n):
    senders, rows_all, points = message.shape
    channels = rows_all // CAPACITY - 2
    vmem = pl.BlockSpec(memory_space=pltpu.VMEM)
    turns = points // 4 // CHUNK_ROWS
    return pl.pallas_call(
        functools.partial(outer_kernel, cols_n),
        name="outer",
        out_shape=(
            jax.ShapeDtypeStruct((channels, TILE_ROWS, TILE_COLS), F32),
            jax.ShapeDtypeStruct((LANES, LANES), jnp.int32),
            jax.ShapeDtypeStruct((LANES, LANES), jnp.int32),
            jax.ShapeDtypeStruct((channels, LANES, LANES), F32),
            jax.ShapeDtypeStruct((2, REACH, LANES), F32),
        ),
        in_specs=[vmem] * 2,
        input_output_aliases={1: 0},
        out_specs=(vmem,) * 5,
        scratch_shapes=[pltpu.VMEM(message.shape, F32)]
        + [pltpu.SMEM((turns,), jnp.int32)] * 4,
        compiler_params=pltpu.CompilerParams(vmem_limit_bytes=16 << 20),
    )(message, zeros)


def along_cols(block, beyond, count, my_col, cols_n, band, store):
    for n in range(count):
        own = block(n)
        before = block(n - 1) if n else jnp.where(my_col > 0, beyond, 0.0)
        after = block(n + 1) if n + 1 < count else jnp.where(my_col + 1 < cols_n, beyond, 0.0)
        edge = jnp.where(iota(own.shape, 1) < LANES // 2, after, before)
        x_high, x_low = split(jnp.concatenate([own, edge], axis=1))
        both = dot(x_high, band)
        store(n, both[:, :LANES] + both[:, LANES:] + dot(x_low, band[:, :LANES]))


def inner_kernel(
    rows_n, cols_n, row_bands, col_bands, raw_ref, rows_s, cols_s, weights_s, corner_ref,
    out_ref, tall, above, below, corners, acc, send_sem, recv_sem
):
    channels, height, width = raw_ref.shape
    my_row, my_col = lax.axis_index("row"), lax.axis_index("col")
    other = lax.rem(my_col + 1, cols_n)
    prev = lax.rem(my_row + rows_n - 1, rows_n)
    following = lax.rem(my_row + 1, rows_n)

    def at(row, col):
        return {"row": row, "col": col}

    barrier = pltpu.get_barrier_semaphore()
    peers = [at(prev, my_col), at(following, my_col), at(prev, other), at(following, other), at(my_row, other)]
    for peer in peers:
        pl.semaphore_signal(barrier, inc=1, device_id=peer, device_id_type=MESH)
    acc[...] = raw_ref[...]
    chunks = LANES // 4 // CHUNK_ROWS
    begin, end = inner_chunks(chunks)

    def add(j, base):
        add_window(acc, rows_s, cols_s, weights_s, j, base, base + WINDOW, base)

    def chunk(j, carry):
        add(j, pl.multiple_of(TILE_ROWS // chunks * j - LEAD, 8))
        return carry

    for j in (begin, end - 1, begin + 1):
        add(j, fixed_row(j, chunks))
    pl.semaphore_wait(barrier, len(peers))
    near = pl.ds(pl.multiple_of((1 - my_col) * (width - LANES), LANES), LANES)
    beyond = pl.ds(width, LANES)
    top, bottom = pl.ds(0, REACH), pl.ds(height - REACH, REACH)

    def remote(i, source, target, peer):
        return pltpu.make_async_remote_copy(
            src_ref=source, dst_ref=target, send_sem=send_sem.at[i], recv_sem=recv_sem.at[i],
            device_id=peer, device_id_type=MESH,
        )

    halo = [
        remote(0, raw_ref.at[:, bottom, :], above, peers[1]),
        remote(1, raw_ref.at[:, top, :], below, peers[0]),
        remote(2, corner_ref.at[1], corners.at[0], peers[3]),
        remote(3, corner_ref.at[0], corners.at[1], peers[2]),
    ]
    for copy in halo:
        copy.start()
    lax.fori_loop(begin + 2, end - 1, chunk, 0, unroll=UNROLL)

    step = 2 * LANES

    def own_rows(c, carry):
        bands = row_bands[c]
        for g in range(width // step):
            cols = slice(g * step, (g + 1) * step)
            x_high, x_low = split(acc[c, :, cols])
            both = dot(bands, x_high)
            tall[c, :, cols] = both[:height] + both[height:] + dot(bands[:height], x_low)
        return carry

    def partner(c):
        return remote(4 + c, tall.at[c, :, near], tall.at[c, :, beyond], peers[4])

    def next_rows(c, carry):
        own_rows(c, carry)
        partner(c - 1).start()
        return carry

    own_rows(0, 0)
    lax.fori_loop(1, channels, next_rows, 0, unroll=True)
    partner(channels - 1).start()

    def inner_cols(c, carry):
        partner(c).wait_recv()
        rows = slice(REACH, height - REACH)

        def block(n):
            return tall[c, rows, n * LANES : (n + 1) * LANES]

        def store(n, value):
            out_ref[c, rows, n * LANES : (n + 1) * LANES] = value

        count = width // LANES
        along_cols(block, block(count), count, my_col, cols_n, col_bands[c], store)
        return carry

    lax.fori_loop(0, channels - 1, inner_cols, 0, unroll=True)
    partner(channels - 1).wait_recv()
    for copy in halo:
        copy.wait_recv()
    for copy in halo + [partner(c) for c in range(channels)]:
        copy.wait_send()


def inner(row_bands, col_bands, raw, rows, cols, weights, corner, rows_n, cols_n):
    channels, height, width = raw.shape
    vmem = pl.BlockSpec(memory_space=pltpu.VMEM)
    return pl.pallas_call(
        functools.partial(inner_kernel, rows_n, cols_n),
        name="inner",
        out_shape=(
            jax.ShapeDtypeStruct((channels - 1, height, width), F32),
            jax.ShapeDtypeStruct((channels, height, width + LANES), F32),
            jax.ShapeDtypeStruct((channels, REACH, width), F32),
            jax.ShapeDtypeStruct((channels, REACH, width), F32),
            jax.ShapeDtypeStruct(corner.shape, F32),
        ),
        in_specs=[vmem] * 7,
        out_specs=(vmem,) * 5,
        scratch_shapes=[
            pltpu.VMEM(raw.shape, F32),
            pltpu.SemaphoreType.DMA((4 + channels,)),
            pltpu.SemaphoreType.DMA((4 + channels,)),
        ],
        compiler_params=pltpu.CompilerParams(
            collective_id=1, has_side_effects=True, vmem_limit_bytes=24 << 20
        ),
    )(row_bands, col_bands, raw, rows, cols, weights, corner)


def finish_kernel(
    cols_n, col_bands, halo_taps, done_ref, tall, above, below, corners, out_ref,
    last, edge, inner_sem, edge_sem
):
    channels, height, width = out_ref.shape
    my_col = lax.axis_index("col")
    count = width // LANES
    rows = pl.ds(REACH, height - 2 * REACH)
    copies = [
        pltpu.make_async_copy(done_ref.at[c, rows], out_ref.at[c, rows], inner_sem.at[c])
        for c in range(channels - 1)
    ]
    for copy in copies:
        copy.start()
    c = channels - 1

    def last_block(n):
        return tall[c, REACH : height - REACH, n * LANES : (n + 1) * LANES]

    def last_store(n, value):
        last[:, n * LANES : (n + 1) * LANES] = value

    along_cols(last_block, last_block(count), count, my_col, cols_n, col_bands[c], last_store)
    copies.append(pltpu.make_async_copy(last, out_ref.at[c, rows], inner_sem.at[c]))
    copies[-1].start()
    for c in range(channels):
        sides = []
        turn = lax.rem(my_col * (LANES - REACH) + LANES - REACH * c, LANES)
        for i, (halo, start) in enumerate(((above, 0), (below, height - REACH))):
            beyond = pltpu.roll(corners[i], turn, axis=1)
            x_high, x_low = split(jnp.concatenate([halo[c], beyond], axis=1))
            sides.append(
                tall[c, start : start + REACH, :]
                + dot(halo_taps[c, i], jnp.concatenate([x_high, x_high, x_low], axis=0))
            )
        rows = jnp.concatenate(sides, axis=0)

        def block(n):
            return rows[:, n * LANES : (n + 1) * LANES]

        def store(n, value):
            edge[c, :, n * LANES : (n + 1) * LANES] = value

        along_cols(block, block(count), count, my_col, cols_n, col_bands[c], store)
        for i, start in enumerate((0, height - REACH)):
            copies.append(
                pltpu.make_async_copy(
                    edge.at[c, pl.ds(i * REACH, REACH)],
                    out_ref.at[c, pl.ds(start, REACH)],
                    edge_sem.at[i, c],
                )
            )
            copies[-1].start()
    for copy in copies:
        copy.wait()


def finish(col_bands, halo_taps, done, tall, above, below, corners, cols_n):
    channels, height, wide = tall.shape
    width = wide - LANES
    vmem = pl.BlockSpec(memory_space=pltpu.VMEM)
    return pl.pallas_call(
        functools.partial(finish_kernel, cols_n),
        name="finish",
        out_shape=jax.ShapeDtypeStruct((channels, height, width), F32),
        in_specs=[vmem] * 7,
        out_specs=pl.BlockSpec(memory_space=pltpu.MemorySpace.HBM),
        scratch_shapes=[
            pltpu.VMEM((height - 2 * REACH, width), F32),
            pltpu.VMEM((channels, 2 * REACH, width), F32),
            pltpu.SemaphoreType.DMA((channels,)),
            pltpu.SemaphoreType.DMA((2, channels)),
        ],
        compiler_params=pltpu.CompilerParams(vmem_limit_bytes=12 << 20),
    )(col_bands, halo_taps, done, tall, above, below, corners)


def shards(cell_index, weights, block_tile, spread):
    rows_n, cols_n = lax.axis_size("row"), lax.axis_size("col")
    message, zeros, row_bands, col_bands, halo_taps = exchange(
        cell_index, weights, block_tile, spread, rows_n, cols_n
    )
    points = outer(message, zeros, cols_n)
    done = inner(row_bands, col_bands, *points, rows_n, cols_n)
    return finish(col_bands, halo_taps, *done, cols_n)


def solution(mesh):
    return jax.shard_map(
        shards,
        mesh=mesh,
        in_specs=(
            P(("groups", "row", "col"), None),
            P(("groups", "row", "col"), None),
            P(("groups", "row", "col")),
            P(),
        ),
        out_specs=P(None, ("groups", "row"), "col"),
        check_vma=False,
    )
```

```python
import functools

import jax
import jax.numpy as jnp
from jax import lax
from jax.experimental import pallas as pl
from jax.experimental.pallas import tpu as pltpu
from jax.sharding import PartitionSpec as P

REACH = 16
TILE_ROWS = 256
TILE_COLS = 1024
CAPACITY = 3
LANES = 128
WINDOW = 64
LEAD = 24
BITS = 9
HALF = 1 << (BITS - 1)
CHUNK_ROWS = 2
UNROLL = 9
MESH = pl.DeviceIdType.MESH
F32 = jnp.float32
BF16 = jnp.bfloat16


def iota(shape, dim):
    return lax.broadcasted_iota(jnp.int32, shape, dim)


def in_hbm(value):
    return pltpu.with_memory_space_constraint(value, pltpu.MemorySpace.HBM)


def dot(a, b):
    return lax.dot_general(a, b, (((1,), (0,)), ((), ())), preferred_element_type=F32)


def split(value):
    high = value.astype(BF16)
    return high, (value - high.astype(F32)).astype(BF16)


def tap(offset, width):
    near = jnp.abs(offset) <= REACH
    far = offset.astype(F32)
    return jnp.where(near, jnp.exp(-(far * far) / (2.0 * width * width)), 0.0)


def col_band(width):
    source = iota((2 * LANES, LANES), 0)
    source = jnp.where(source < LANES + LANES // 2, source, source - 2 * LANES)
    high, low = split(tap(source - iota((2 * LANES, LANES), 1), width))
    return jnp.concatenate([high, low], axis=1)


def exchange_kernel(
    rows_n, cols_n, cell_hbm, weight_hbm, tile_hbm, spread_hbm,
    message_out, zeros_out, row_bands, col_bands, halo_taps,
    cell_ref, weight_ref, tile_ref, spread_ref, values, keys_t, sorted_points, send_message,
    send_sem, recv_sem, local_sem
):
    loads = [
        pltpu.make_async_copy(source, target, local_sem.at[i])
        for i, (source, target) in enumerate(
            (
                (cell_hbm, cell_ref),
                (weight_hbm, weight_ref),
                (tile_hbm, tile_ref),
                (spread_hbm, spread_ref),
            )
        )
    ]
    for load in loads:
        load.start()
    blocks, points = cell_ref.shape
    channels = weight_ref.shape[1] // points
    peers = rows_n * cols_n
    my_row, my_col = lax.axis_index("row"), lax.axis_index("col")
    me = my_row * cols_n + my_col

    offsets = []
    for distance in range(rows_n // 2, 0, -1):
        for step in (distance, rows_n - distance):
            if step not in [o[0] for o in offsets]:
                offsets += [(step, c) for c in range(cols_n)]
    offsets += [(0, c) for c in range(1, cols_n)]

    barrier = pltpu.get_barrier_semaphore()
    targets = []
    for step, turn in offsets:
        row = lax.rem(my_row + step, rows_n)
        col = lax.rem(my_col + turn, cols_n)
        targets.append((row, col))
        pl.semaphore_signal(
            barrier, inc=1, device_id={"row": row, "col": col}, device_id_type=MESH
        )

    for load in loads:
        load.wait()
    tile = tile_ref[...]
    square = (blocks, blocks)
    tile_down = jnp.sum(
        jnp.where(iota(square, 0) == iota(square, 1), tile, 0), axis=1, keepdims=True
    )
    earlier = (tile_down == tile) & (iota(square, 0) < iota(square, 1))
    turn_of = jnp.sum(earlier.astype(jnp.int32), axis=0, keepdims=True)
    cells = cell_ref[...]
    rows_each = channels + 2
    parts = [weight_ref[:, c * points : (c + 1) * points] for c in range(channels)] + [
        (part - HALF).astype(F32).astype(BF16)
        for part in (cells >> BITS, cells & (2 * HALF - 1))
    ]
    group = CAPACITY * points
    ramp = (iota((1, points), 1) * (TILE_ROWS // points * TILE_COLS // (2 * HALF)) - HALF).astype(F32)
    keys = []
    for k in range(CAPACITY):
        chosen = ((iota((peers, blocks), 0) == tile) & (turn_of == k)).astype(F32)
        empty = jnp.sum(chosen, axis=1, keepdims=True) < 0.5
        placed = dot(chosen.astype(BF16), jnp.concatenate(parts, axis=1))
        for v in range(rows_each):
            piece = placed[:, v * points : (v + 1) * points]
            if v == channels:
                piece = jnp.where(empty, ramp, piece)
                index = (iota((1, points), 1) + k * points).astype(F32)
                keys.append((piece + float(HALF)) * 512.0 + index)
            if v == channels + 1:
                piece = jnp.where(empty, -float(HALF), piece)
            values[v, :, k * points : (k + 1) * points] = piece
    pad = jnp.zeros((points - peers, points), F32)
    keys_t[...] = jnp.concatenate(
        [jnp.transpose(jnp.concatenate([key, pad], axis=0)) for key in keys], axis=0
    )
    keys = jnp.concatenate(keys, axis=1)
    quarter = points // 4
    chunks = quarter // CHUNK_ROWS
    share = group // chunks
    for t in range(peers):
        less = (keys_t[:, t : t + 1] < keys[t : t + 1, :]).astype(F32)
        rank = jnp.sum(less, axis=0, keepdims=True).astype(jnp.int32)
        chunk = (rank * (65536 // share + 1)) >> 16
        inside = rank - chunk * share
        third = (inside * (512 // CAPACITY + 1)) >> 9
        lane = (inside - third * CAPACITY) * points
        lane = lane + (third & 3) * quarter + chunk * CHUNK_ROWS + (third >> 2)
        hot = (iota((group, group), 0) == lane).astype(F32).astype(BF16)
        piece = jnp.concatenate(
            [values[v, t : t + 1, :] for v in range(rows_each)]
            + [jnp.zeros((8 - rows_each, group), F32)],
            axis=0,
        ).astype(BF16)
        sorted_points[t] = lax.dot_general(
            piece, hot, (((1,), (1,)), ((), ())), preferred_element_type=F32
        )
    for k in range(CAPACITY):
        part = slice(k * points, (k + 1) * points)
        for v in range(rows_each):
            send_message[:, k * rows_each + v, :] = sorted_points[:, v, part].astype(BF16)

    own = pltpu.make_async_copy(send_message.at[me], message_out.at[me], local_sem.at[4])
    pl.semaphore_wait(barrier, peers - 1)
    copies = []
    for i, (row, col) in enumerate(targets):
        copy = pltpu.make_async_remote_copy(
            src_ref=send_message.at[row * cols_n + col],
            dst_ref=message_out.at[me],
            send_sem=send_sem.at[i],
            recv_sem=recv_sem.at[i],
            device_id={"row": row, "col": col},
            device_id_type=MESH,
        )
        copy.start()
        copies.append(copy)
    own.start()
    zeros_out[...] = jnp.zeros_like(zeros_out)
    square = (TILE_ROWS, TILE_ROWS)
    shape = (REACH, 3 * REACH)
    part = iota(shape, 1) >> (REACH.bit_length() - 1)
    offset = (iota(shape, 1) & (REACH - 1)) - iota(shape, 0)
    for c in range(channels):
        high, low = split(tap(iota(square, 1) - iota(square, 0), spread_ref[0, c]))
        row_bands[c, :TILE_ROWS] = high
        row_bands[c, TILE_ROWS:] = low
        col_bands[c] = col_band(spread_ref[1, c])
        for i, (shift, real) in enumerate(((-REACH, my_row > 0), (REACH, my_row + 1 < rows_n))):
            taps = jnp.where(real, tap(offset + shift, spread_ref[0, c]), 0.0)
            high = taps.astype(BF16).astype(F32)
            halo_taps[c, i] = jnp.where(part == 1, taps - high, high).astype(BF16)
    own.wait()
    for copy in copies:
        copy.wait_recv()
    for copy in copies:
        copy.wait_send()


def exchange(cell_index, weights, block_tile, spread, rows_n, cols_n):
    blocks, points = cell_index.shape
    channels = weights.shape[1] // points
    peers = rows_n * cols_n
    message = (peers, CAPACITY * (channels + 2), points)
    return pl.pallas_call(
        functools.partial(exchange_kernel, rows_n, cols_n),
        name="exchange",
        out_shape=(
            jax.ShapeDtypeStruct(message, BF16),
            jax.ShapeDtypeStruct((channels, TILE_ROWS, TILE_COLS), F32),
            jax.ShapeDtypeStruct((channels, 2 * TILE_ROWS, TILE_ROWS), BF16),
            jax.ShapeDtypeStruct((channels, 2 * LANES, 2 * LANES), BF16),
            jax.ShapeDtypeStruct((channels, 2, REACH, 3 * REACH), BF16),
        ),
        in_specs=[pl.BlockSpec(memory_space=pltpu.MemorySpace.HBM)] * 4,
        out_specs=(pl.BlockSpec(memory_space=pltpu.VMEM),) * 5,
        scratch_shapes=[
            pltpu.VMEM(cell_index.shape, jnp.int32),
            pltpu.VMEM(weights.shape, BF16),
            pltpu.VMEM((1, blocks), jnp.int32),
            pltpu.SMEM(spread.shape, F32),
            pltpu.VMEM((channels + 2, peers, CAPACITY * points), F32),
            pltpu.VMEM((CAPACITY * points, points), F32),
            pltpu.VMEM((peers, 8, CAPACITY * points), F32),
            pltpu.VMEM(message, BF16),
            pltpu.SemaphoreType.DMA((peers - 1,)),
            pltpu.SemaphoreType.DMA((peers - 1,)),
            pltpu.SemaphoreType.DMA((5,)),
        ],
        compiler_params=pltpu.CompilerParams(
            collective_id=0, has_side_effects=True, vmem_limit_bytes=8 << 20
        ),
    )(*(in_hbm(x) for x in (cell_index, weights, block_tile.reshape(1, -1), spread)))


def widened(slots, quarter):
    return jnp.concatenate(
        [
            jnp.concatenate([s[:, v * quarter : (v + 1) * quarter] for v in range(4)], axis=0)
            for s in slots
        ]
        + [jnp.zeros((LANES, LANES - len(slots) * quarter), F32)],
        axis=1,
    )


def add_window(raw_ref, rows_s, cols_s, weights_s, j, low, stop, base):
    channels = raw_ref.shape[0]
    quarter = LANES // 4
    span = 256

    def take(ref):
        return jnp.concatenate(
            [
                ref[pl.ds(quarter * k + CHUNK_ROWS * j + i, 1), :]
                for k in range(CAPACITY)
                for i in range(CHUNK_ROWS)
            ],
            axis=1,
        )

    row = take(rows_s)
    count = row.shape[1]
    cols = pltpu.roll(cols_s[...], lax.rem(LANES - CHUNK_ROWS * j, LANES), axis=1)
    offset = jnp.where((row >= low) & (row < stop), row - base, -1)
    hot = iota((WINDOW, count), 0) == offset
    left = jnp.concatenate(
        [jnp.where(hot, take(weights_s.at[c]), 0.0).astype(BF16) for c in range(channels)],
        axis=0,
    )
    for g in range(TILE_COLS // span):
        target = iota((LANES, span), 1) + g * span
        right = jnp.concatenate(
            [
                (target == cols[:, quarter * k + i : quarter * k + i + 1]).astype(F32).astype(BF16)
                for k in range(CAPACITY)
                for i in range(CHUNK_ROWS)
            ],
            axis=0,
        )
        layer = dot(left, right)
        for c in range(channels):
            raw_ref[c, pl.ds(base, WINDOW), g * span : (g + 1) * span] += layer[
                c * WINDOW : (c + 1) * WINDOW
            ]


def fixed_row(j, chunks):
    row = TILE_ROWS // chunks * j - LEAD
    return min(max(row, REACH), TILE_ROWS - REACH - WINDOW)


def inner_chunks(chunks):
    tall = TILE_ROWS // chunks
    inner = [
        j
        for j in range(chunks)
        if tall * (j - 1) >= REACH and tall * (j + 2) <= TILE_ROWS - REACH
    ]
    return inner[0], inner[-1] + 1


def outer_kernel(
    cols_n, message_ref, zeros_ref, raw_ref, rows_s, cols_s, weights_s, corner_ref, wide_s, first_s, last_s, next_s, done_s
):
    senders, rows_all, points = message_ref.shape
    rows_each = rows_all // CAPACITY
    channels = rows_each - 2
    quarter = points // 4
    chunks = quarter // CHUNK_ROWS
    wide_s[...] = message_ref[...].astype(F32)

    def wide(v):
        return widened([wide_s[:, k * rows_each + v, :] for k in range(CAPACITY)], quarter)

    cells = (wide(channels) + HALF) * (2 * HALF) + (wide(channels + 1) + HALF)
    cols_s[...] = cells.astype(jnp.int32) & (TILE_COLS - 1)
    rows = jnp.transpose(cells).astype(jnp.int32) >> (TILE_COLS.bit_length() - 1)
    rows_s[...] = rows
    for c in range(channels):
        weights_s[c] = jnp.transpose(wide(c))
    low, high = rows[:quarter], rows[:quarter]
    for k in range(1, CAPACITY):
        low = jnp.minimum(low, rows[quarter * k : quarter * (k + 1)])
        high = jnp.maximum(high, rows[quarter * k : quarter * (k + 1)])
    low = jnp.min(low, axis=1, keepdims=True)
    high = jnp.max(high, axis=1, keepdims=True)
    begin, end = inner_chunks(chunks)
    for j in range(chunks):
        lows = [low[CHUNK_ROWS * j + i, 0] for i in range(CHUNK_ROWS)]
        highs = [high[CHUNK_ROWS * j + i, 0] for i in range(CHUNK_ROWS)]
        first = (functools.reduce(jnp.minimum, lows) >> 3) << 3
        done = fixed_row(j, chunks) if begin <= j < end else first
        done_s[j] = done
        first_s[j] = first
        last_s[j] = functools.reduce(jnp.maximum, highs)
        next_s[j] = jnp.where(first < done, first, done + WINDOW)

    def add(j, low, stop):
        base = pl.multiple_of(jnp.minimum(low, TILE_ROWS - WINDOW), 8)
        add_window(raw_ref, rows_s, cols_s, weights_s, j, low, stop, base)

    def common(i, carry):
        j = jnp.where(i < begin, i, i + end - begin)
        low = first_s[j]
        add(j, low, low + WINDOW)
        return carry

    lax.fori_loop(0, chunks - (end - begin), common, 0, unroll=True)

    def rest(j, carry):
        done = done_s[j]

        def more(low):
            stop = jnp.where(low < done, jnp.minimum(low + WINDOW, done), low + WINDOW)
            add(j, low, stop)
            return jnp.where(stop == done, done + WINDOW, stop)

        lax.while_loop(lambda low: low <= last_s[j], more, next_s[j])
        return carry

    lax.fori_loop(0, chunks, rest, 0)
    my_col = lax.axis_index("col")
    near = pl.ds(pl.multiple_of((1 - my_col) * (TILE_COLS - LANES), LANES), LANES)
    for i, start in enumerate((0, TILE_ROWS - REACH)):
        packed = jnp.zeros((REACH, LANES), F32)
        lane = iota(packed.shape, 1)
        for c in range(channels):
            block = raw_ref[c, start : start + REACH, near]
            block = pltpu.roll(block, REACH * c + REACH * (1 - my_col), axis=1)
            mine = (lane >= REACH * c) & (lane < REACH * (c + 1))
            packed = jnp.where(mine, block, packed)
        corner_ref[i] = packed


def outer(message, zeros, cols_n):
    senders, rows_all, points = message.shape
    channels = rows_all // CAPACITY - 2
    vmem = pl.BlockSpec(memory_space=pltpu.VMEM)
    turns = points // 4 // CHUNK_ROWS
    return pl.pallas_call(
        functools.partial(outer_kernel, cols_n),
        name="outer",
        out_shape=(
            jax.ShapeDtypeStruct((channels, TILE_ROWS, TILE_COLS), F32),
            jax.ShapeDtypeStruct((LANES, LANES), jnp.int32),
            jax.ShapeDtypeStruct((LANES, LANES), jnp.int32),
            jax.ShapeDtypeStruct((channels, LANES, LANES), F32),
            jax.ShapeDtypeStruct((2, REACH, LANES), F32),
        ),
        in_specs=[vmem] * 2,
        input_output_aliases={1: 0},
        out_specs=(vmem,) * 5,
        scratch_shapes=[pltpu.VMEM(message.shape, F32)]
        + [pltpu.SMEM((turns,), jnp.int32)] * 4,
        compiler_params=pltpu.CompilerParams(vmem_limit_bytes=16 << 20),
    )(message, zeros)


def along_cols(block, beyond, count, my_col, cols_n, band, store):
    for n in range(count):
        own = block(n)
        before = block(n - 1) if n else jnp.where(my_col > 0, beyond, 0.0)
        after = block(n + 1) if n + 1 < count else jnp.where(my_col + 1 < cols_n, beyond, 0.0)
        edge = jnp.where(iota(own.shape, 1) < LANES // 2, after, before)
        x_high, x_low = split(jnp.concatenate([own, edge], axis=1))
        both = dot(x_high, band)
        store(n, both[:, :LANES] + both[:, LANES:] + dot(x_low, band[:, :LANES]))


def inner_kernel(
    rows_n, cols_n, row_bands, col_bands, raw_ref, rows_s, cols_s, weights_s, corner_ref,
    out_ref, tall, above, below, corners, acc, send_sem, recv_sem
):
    channels, height, width = raw_ref.shape
    my_row, my_col = lax.axis_index("row"), lax.axis_index("col")
    other = lax.rem(my_col + 1, cols_n)
    prev = lax.rem(my_row + rows_n - 1, rows_n)
    following = lax.rem(my_row + 1, rows_n)

    def at(row, col):
        return {"row": row, "col": col}

    barrier = pltpu.get_barrier_semaphore()
    peers = [at(prev, my_col), at(following, my_col), at(prev, other), at(following, other), at(my_row, other)]
    for peer in peers:
        pl.semaphore_signal(barrier, inc=1, device_id=peer, device_id_type=MESH)
    acc[...] = raw_ref[...]
    chunks = LANES // 4 // CHUNK_ROWS
    begin, end = inner_chunks(chunks)

    def add(j, base):
        add_window(acc, rows_s, cols_s, weights_s, j, base, base + WINDOW, base)

    def chunk(j, carry):
        add(j, pl.multiple_of(TILE_ROWS // chunks * j - LEAD, 8))
        return carry

    for j in (begin, end - 1):
        add(j, fixed_row(j, chunks))
    pl.semaphore_wait(barrier, len(peers))
    near = pl.ds(pl.multiple_of((1 - my_col) * (width - LANES), LANES), LANES)
    beyond = pl.ds(width, LANES)
    top, bottom = pl.ds(0, REACH), pl.ds(height - REACH, REACH)

    def remote(i, source, target, peer):
        return pltpu.make_async_remote_copy(
            src_ref=source, dst_ref=target, send_sem=send_sem.at[i], recv_sem=recv_sem.at[i],
            device_id=peer, device_id_type=MESH,
        )

    halo = [
        remote(0, raw_ref.at[:, bottom, :], above, peers[1]),
        remote(1, raw_ref.at[:, top, :], below, peers[0]),
        remote(2, corner_ref.at[1], corners.at[0], peers[3]),
        remote(3, corner_ref.at[0], corners.at[1], peers[2]),
    ]
    for copy in halo:
        copy.start()
    add(begin + 1, fixed_row(begin + 1, chunks))
    lax.fori_loop(begin + 2, end - 1, chunk, 0, unroll=UNROLL)

    step = 2 * LANES

    def own_rows(c, carry):
        bands = row_bands[c]
        for g in range(width // step):
            cols = slice(g * step, (g + 1) * step)
            x_high, x_low = split(acc[c, :, cols])
            both = dot(bands, x_high)
            tall[c, :, cols] = both[:height] + both[height:] + dot(bands[:height], x_low)
        return carry

    def partner(c):
        return remote(4 + c, tall.at[c, :, near], tall.at[c, :, beyond], peers[4])

    def next_rows(c, carry):
        own_rows(c, carry)
        partner(c - 1).start()
        return carry

    own_rows(0, 0)
    lax.fori_loop(1, channels, next_rows, 0, unroll=True)
    partner(channels - 1).start()

    def inner_cols(c, carry):
        partner(c).wait_recv()
        rows = slice(REACH, height - REACH)

        def block(n):
            return tall[c, rows, n * LANES : (n + 1) * LANES]

        def store(n, value):
            out_ref[c, rows, n * LANES : (n + 1) * LANES] = value

        count = width // LANES
        along_cols(block, block(count), count, my_col, cols_n, col_bands[c], store)
        return carry

    lax.fori_loop(0, channels - 1, inner_cols, 0, unroll=True)
    partner(channels - 1).wait_recv()
    for copy in halo:
        copy.wait_recv()
    for copy in halo + [partner(c) for c in range(channels)]:
        copy.wait_send()


def inner(row_bands, col_bands, raw, rows, cols, weights, corner, rows_n, cols_n):
    channels, height, width = raw.shape
    vmem = pl.BlockSpec(memory_space=pltpu.VMEM)
    return pl.pallas_call(
        functools.partial(inner_kernel, rows_n, cols_n),
        name="inner",
        out_shape=(
            jax.ShapeDtypeStruct((channels - 1, height, width), F32),
            jax.ShapeDtypeStruct((channels, height, width + LANES), F32),
            jax.ShapeDtypeStruct((channels, REACH, width), F32),
            jax.ShapeDtypeStruct((channels, REACH, width), F32),
            jax.ShapeDtypeStruct(corner.shape, F32),
        ),
        in_specs=[vmem] * 7,
        out_specs=(vmem,) * 5,
        scratch_shapes=[
            pltpu.VMEM(raw.shape, F32),
            pltpu.SemaphoreType.DMA((4 + channels,)),
            pltpu.SemaphoreType.DMA((4 + channels,)),
        ],
        compiler_params=pltpu.CompilerParams(
            collective_id=1, has_side_effects=True, vmem_limit_bytes=24 << 20
        ),
    )(row_bands, col_bands, raw, rows, cols, weights, corner)


def finish_kernel(
    cols_n, col_bands, halo_taps, done_ref, tall, above, below, corners, out_ref,
    last, edge, inner_sem, edge_sem
):
    channels, height, width = out_ref.shape
    my_col = lax.axis_index("col")
    count = width // LANES
    rows = pl.ds(REACH, height - 2 * REACH)
    copies = [
        pltpu.make_async_copy(done_ref.at[c, rows], out_ref.at[c, rows], inner_sem.at[c])
        for c in range(channels - 1)
    ]
    for copy in copies:
        copy.start()
    c = channels - 1

    def last_block(n):
        return tall[c, REACH : height - REACH, n * LANES : (n + 1) * LANES]

    def last_store(n, value):
        last[:, n * LANES : (n + 1) * LANES] = value

    along_cols(last_block, last_block(count), count, my_col, cols_n, col_bands[c], last_store)
    copies.append(pltpu.make_async_copy(last, out_ref.at[c, rows], inner_sem.at[c]))
    copies[-1].start()
    for c in range(channels):
        sides = []
        turn = lax.rem(my_col * (LANES - REACH) + LANES - REACH * c, LANES)
        for i, (halo, start) in enumerate(((above, 0), (below, height - REACH))):
            beyond = pltpu.roll(corners[i], turn, axis=1)
            x_high, x_low = split(jnp.concatenate([halo[c], beyond], axis=1))
            sides.append(
                tall[c, start : start + REACH, :]
                + dot(halo_taps[c, i], jnp.concatenate([x_high, x_high, x_low], axis=0))
            )
        rows = jnp.concatenate(sides, axis=0)

        def block(n):
            return rows[:, n * LANES : (n + 1) * LANES]

        def store(n, value):
            edge[c, :, n * LANES : (n + 1) * LANES] = value

        along_cols(block, block(count), count, my_col, cols_n, col_bands[c], store)
        for i, start in enumerate((0, height - REACH)):
            copies.append(
                pltpu.make_async_copy(
                    edge.at[c, pl.ds(i * REACH, REACH)],
                    out_ref.at[c, pl.ds(start, REACH)],
                    edge_sem.at[i, c],
                )
            )
            copies[-1].start()
    for copy in copies:
        copy.wait()


def finish(col_bands, halo_taps, done, tall, above, below, corners, cols_n):
    channels, height, wide = tall.shape
    width = wide - LANES
    vmem = pl.BlockSpec(memory_space=pltpu.VMEM)
    return pl.pallas_call(
        functools.partial(finish_kernel, cols_n),
        name="finish",
        out_shape=jax.ShapeDtypeStruct((channels, height, width), F32),
        in_specs=[vmem] * 7,
        out_specs=pl.BlockSpec(memory_space=pltpu.MemorySpace.HBM),
        scratch_shapes=[
            pltpu.VMEM((height - 2 * REACH, width), F32),
            pltpu.VMEM((channels, 2 * REACH, width), F32),
            pltpu.SemaphoreType.DMA((channels,)),
            pltpu.SemaphoreType.DMA((2, channels)),
        ],
        compiler_params=pltpu.CompilerParams(vmem_limit_bytes=12 << 20),
    )(col_bands, halo_taps, done, tall, above, below, corners)


def shards(cell_index, weights, block_tile, spread):
    rows_n, cols_n = lax.axis_size("row"), lax.axis_size("col")
    message, zeros, row_bands, col_bands, halo_taps = exchange(
        cell_index, weights, block_tile, spread, rows_n, cols_n
    )
    points = outer(message, zeros, cols_n)
    done = inner(row_bands, col_bands, *points, rows_n, cols_n)
    return finish(col_bands, halo_taps, *done, cols_n)


def solution(mesh):
    return jax.shard_map(
        shards,
        mesh=mesh,
        in_specs=(
            P(("groups", "row", "col"), None),
            P(("groups", "row", "col"), None),
            P(("groups", "row", "col")),
            P(),
        ),
        out_specs=P(None, ("groups", "row"), "col"),
        check_vma=False,
    )
```
